128 devices in a mesh: grp: 4 (over y), tile: 32 (over x, z, core).
Axes of the slice: x: 4, y: 4, z: 4, core: 2. Of those that a mesh axis runs over, the one named last changes fastest.
Arguments:
- base_rhs: float32 [1024, 16384], P('grp', 'tile'), may hold values from -6 to 6
- depth: float32 [1024, 16384], P('grp', 'tile'), may hold values from 0.25 to 2
- ssh_prev: float32 [1024, 16384], P('grp', 'tile'), may hold values from -6 to 6
- currents: float32 [2, 1024, 16384], P(None, 'grp', 'tile'), may hold values from -3 to 3
- land_blocks: int32 [128, 2048], P('grp', 'tile'), may hold values 0 or 1
- ice_thick: float32 [2, 256, 16384], P(None, 'grp', 'tile'), may hold values from 0.25 to 4
- ice_blocks: int32 [2, 32, 2048], P(None, 'grp', 'tile'), may hold values 0 or 1
- ice_vel: float32 [2, 2, 256, 16384], P(None, None, 'grp', 'tile'), may hold values from -3 to 3
- ice_stress: float32 [3, 2, 256, 16384], P(None, None, 'grp', 'tile'), may hold values from -5 to 5
- wind: float32 [2, 2, 256, 16384], P(None, None, 'grp', 'tile'), may hold values from -6 to 6
Outputs:
- ssh: float32 [1024, 16384], P('grp', 'tile')
- ice_vel_out: float32 [2, 2, 256, 16384], P(None, None, 'grp', 'tile')
- ice_stress_out: float32 [3, 2, 256, 16384], P(None, None, 'grp', 'tile')
The draws below stay inside these ranges and needn't reach their ends.
All inputs are finite; a program needn't handle non-finite values. No bound on the sum of `land_blocks` or of `ice_blocks` on one device may be relied on, other than what follows from the above.
Results may differ from the reference program's by a relative error of at most 0.0001.
Values sent between devices are 32-bit elements; how exact they have to be, the bound alone decides.
A program may use at most 64 MiB of HBM per device.

```python
import math
import jax
import jax.numpy as jnp

BS = 8
NSUB = 8
ITERS = 3
NX = 1024
NY = 16384
NXI = 256


def set_ends(values, own_key, least, largest):
    index_at = [jax.random.randint(jax.random.fold_in(own_key, axis), (), 0, length) for axis, length in enumerate(values.shape)]
    widest = values.shape.index(max(values.shape))
    beside = index_at[:widest] + [(index_at[widest] + 1) % values.shape[widest]] + index_at[widest + 1:]
    return values.at[tuple(index_at)].set(least).at[tuple(beside)].set(largest)


def level_of(key, extent, split, smallest, high):
    loudness = 1.0
    for position, shards_of in split:
        heights = jax.random.uniform(jax.random.fold_in(jax.random.fold_in(key, 6), position), (shards_of,), jnp.float32, smallest / len(split), high / len(split))
        loudness = loudness * jnp.repeat(jnp.exp(heights), extent[position] // shards_of).reshape((-1,) + (1,) * (len(extent) - 1 - position))
    return loudness


def bell_draw(rng, dims, scale, reach, pieces=(), held_as=jnp.bfloat16):
    level = level_of(rng, dims, pieces, -0.22, 0.18) if pieces else 1.0
    entries = jax.random.normal(rng, dims, jnp.float32) * scale * level
    return jnp.minimum(jnp.maximum(entries, -reach), reach).astype(held_as)


def setup_inputs(seed: int = 0) -> dict:
    key_list = jax.random.split(jax.random.key(seed), 11)
    base_rhs = bell_draw(key_list[0], (NX, NY), 1.0, 6.0, ((0, 4), (1, 32)), jnp.float32)
    depth = jnp.clip(jnp.exp(math.log(2.0) - 2.0794415 * jax.random.uniform(key_list[1], (NX, NY), jnp.float32) ** level_of(key_list[1], (NX, NY), ((0, 4), (1, 32)), -0.2, 0.2)), 0.25, 2.0)
    ssh_prev = bell_draw(key_list[2], (NX, NY), 1.0, 6.0, ((0, 4), (1, 32)), jnp.float32)
    currents = bell_draw(key_list[3], (2, NX, NY), 0.5, 3.0, ((1, 4), (2, 32)), jnp.float32)
    land_blocks = set_ends((jax.random.randint(key_list[4], (NX // BS, NY // BS), 0, 4) < 3).astype(jnp.int32), jax.random.fold_in(key_list[4], 1), 0, 1)
    ice_thick = jnp.clip(jnp.exp(math.log(4.0) - 2.7725887 * jax.random.uniform(key_list[5], (2, NXI, NY), jnp.float32) ** level_of(key_list[5], (2, NXI, NY), ((1, 4), (2, 32)), -0.2, 0.2)), 0.25, 4.0)
    ice_blocks = set_ends((jax.random.randint(key_list[6], (2, NXI // BS, NY // BS), 0, 4) < 3).astype(jnp.int32), jax.random.fold_in(key_list[6], 1), 0, 1)
    ice_vel = bell_draw(key_list[7], (2, 2, NXI, NY), 0.5, 3.0, ((2, 4), (3, 32)), jnp.float32)
    ice_stress = bell_draw(key_list[8], (3, 2, NXI, NY), 1.0, 5.0, ((2, 4), (3, 32)), jnp.float32)
    wind = bell_draw(key_list[9], (2, 2, NXI, NY), 1.0, 6.0, ((2, 4), (3, 32)), jnp.float32)
    return dict(base_rhs=base_rhs, depth=depth, ssh_prev=ssh_prev, currents=currents, land_blocks=land_blocks, ice_thick=ice_thick, ice_blocks=ice_blocks, ice_vel=ice_vel, ice_stress=ice_stress, wind=wind)


DAMP = 0.05
RELAX = 0.2
STRENGTH = 0.5
DRAG = 1.0
STEP = 0.5

def strain_rates(u_pad, v_pad):
    du_dx = u_pad[..., 1:, :-1] - u_pad[..., :-1, :-1]
    du_dy = u_pad[..., :-1, 1:] - u_pad[..., :-1, :-1]
    dv_dx = v_pad[..., 1:, :-1] - v_pad[..., :-1, :-1]
    dv_dy = v_pad[..., :-1, 1:] - v_pad[..., :-1, :-1]
    return (du_dx + dv_dy, du_dx - dv_dy, du_dy + dv_dx)

def relax_stress(previous, strength, div_rate, tens_rate, shear_rate):
    deformation = jnp.sqrt(div_rate * div_rate + tens_rate * tens_rate + shear_rate * shear_rate + 1.0)
    relax_scale = 1.0 / (1.0 + RELAX)
    div_part = (previous[0] + RELAX * strength * (div_rate / deformation - 1.0)) * relax_scale
    tens_part = (previous[1] + RELAX * strength * tens_rate / deformation) * relax_scale
    shear_part = (previous[2] + RELAX * strength * shear_rate / deformation) * relax_scale
    return jnp.stack([div_part, tens_part, shear_part])

def along_rows(field):
    return field[..., 1:, 1:] - field[..., :-1, 1:]

def along_cols(field):
    return field[..., 1:, 1:] - field[..., 1:, :-1]

def stress_force(stress_pad):
    force_x = 0.5 * along_rows(stress_pad[0] + stress_pad[1]) + along_cols(stress_pad[2])
    force_y = 0.5 * along_cols(stress_pad[0] - stress_pad[1]) + along_rows(stress_pad[2])
    return jnp.stack([force_x, force_y])

def momentum(velocity, force, ice_mass, ice_cover, wind, ocean_flow):
    return ice_cover * (ice_mass * velocity + STEP * (force + wind + DRAG * ocean_flow)) / (ice_mass + STEP * DRAG)

def face_weights(depth_pad):
    centre = depth_pad[1:-1, 1:-1]
    return (centre * depth_pad[2:, 1:-1], centre * depth_pad[:-2, 1:-1], centre * depth_pad[1:-1, 2:], centre * depth_pad[1:-1, :-2])

def apply_operator(field_pad, weights):
    field = field_pad[1:-1, 1:-1]
    north_weight, south_weight, east_weight, west_weight = weights
    return DAMP * field + north_weight * (field - field_pad[2:, 1:-1]) + south_weight * (field - field_pad[:-2, 1:-1]) + east_weight * (field - field_pad[1:-1, 2:]) + west_weight * (field - field_pad[1:-1, :-2])

def expand(blocks):
    return jnp.repeat(jnp.repeat(blocks, BS, axis=-2), BS, axis=-1).astype(jnp.float32)

def reference(base_rhs, depth, ssh_prev, currents, land_blocks, ice_thick, ice_blocks, ice_vel, ice_stress, wind):
    wet_cells = expand(land_blocks)
    ice_cover = expand(ice_blocks)
    strength = STRENGTH * ice_thick * ice_cover
    ice_mass = ice_thick * ice_cover + 1.0
    ocean_flow = jnp.stack([currents[:, :NXI], currents[:, NX - NXI:]], axis=1)
    velocity = ice_vel
    stress = ice_stress
    for subcycle in range(NSUB):
        vel_pad = jnp.pad(velocity, ((0, 0), (0, 0), (1, 1), (1, 1)))
        strain = strain_rates(vel_pad[0], vel_pad[1])
        div_rate = strain[0][:, 1:, 1:]
        tens_rate = strain[1][:, 1:, 1:]
        shear_rate = strain[2][:, 1:, 1:]
        stress = relax_stress(stress, strength, div_rate, tens_rate, shear_rate)
        stress_pad = jnp.pad(stress, ((0, 0), (0, 0), (1, 0), (1, 0)))
        velocity = momentum(velocity, stress_force(stress_pad), ice_mass, ice_cover, wind, ocean_flow)
    ice_drag = DRAG * ice_cover * (velocity - ocean_flow)
    ocean_drag = jnp.zeros((2, NX, NY), jnp.float32)
    ocean_drag = ocean_drag.at[:, :NXI].set(ice_drag[:, 0]).at[:, NX - NXI:].set(ice_drag[:, 1])
    forcing_pad = jnp.pad(jnp.stack([ocean_drag[0], ocean_drag[1], depth * wet_cells]), ((0, 0), (1, 1), (1, 1)))
    spread = forcing_pad[0, 1:-1, 1:-1] - forcing_pad[0, :-2, 1:-1] + (forcing_pad[1, 1:-1, 1:-1] - forcing_pad[1, 1:-1, :-2])
    forcing = wet_cells * (base_rhs + spread)
    weights = face_weights(forcing_pad[2])
    diagonal = DAMP + weights[0] + weights[1] + weights[2] + weights[3]
    solution = ssh_prev
    residual = forcing - apply_operator(jnp.pad(solution, 1), weights)
    precond = residual / diagonal
    direction = precond
    precond_norm = jnp.sum(residual * precond)
    for iteration in range(ITERS):
        applied = apply_operator(jnp.pad(direction, 1), weights)
        step_size = precond_norm / jnp.sum(direction * applied)
        solution = solution + step_size * direction
        residual = residual - step_size * applied
        precond = residual / diagonal
        norm_next = jnp.sum(residual * precond)
        direction = precond + norm_next / precond_norm * direction
        precond_norm = norm_next
    return (solution, velocity, stress)
```

```python
import functools

import jax
import jax.numpy as jnp
from jax import lax
from jax.experimental import pallas as pl
from jax.experimental.pallas import tpu as pltpu
from jax.sharding import PartitionSpec as P

BS = 8
NSUB = 8
DAMP = 0.05
RELAX = 0.2
STRENGTH = 0.5
DRAG = 1.0
STEP = 0.5
G = 4
LT = 4
NT = LT + 1
IR = 64
OR = 256
IH = IR + 32
OH = OR + 32
F32 = jnp.float32
MESH = pl.DeviceIdType.MESH
DUMMY = 4096

R_CL, R_CR, R_IL, R_IR, R_OL, R_OR = 0, 1, 2, 3, 4, 5
R_IU, R_ID, R_F = 6, 8, 10
R_OU, R_OD, R_RS, R_RH, R_1, R_2 = 12, 13, 14, 18, 19, 20
R_BI, R_BO = 21, 30
N_R = 39
S_CL, S_CR, S_L, S_R, S_U, S_D, S_F, S_RS, S_1, S_2 = 0, 1, 2, 3, 4, 5, 6, 7, 9, 10
S_RH = 11
S_BI, S_BO = 12, 21
N_S = 30
L_BLK, L_ICE, L_FL, L_OC, L_OUT, L_OUTS = 0, 1, 2, 3, 4, 5
N_L = 6


def east(tiles, lane):
    turned = [pltpu.roll(x, 127, 1) for x in tiles]
    return [jnp.where(lane == 127, turned[(j + 1) % NT], turned[j]) for j in range(NT)]


def west(tiles, lane):
    turned = [pltpu.roll(x, 1, 1) for x in tiles]
    return [jnp.where(lane == 0, turned[(j - 1) % NT], turned[j]) for j in range(NT)]


def kernel(
    T,
    base, depth, ssh, cur, land, thick, iblk, ivel, istr, wind,
    o_ssh, o_vel, o_str,
    V, S, W, TH, FL, CV, C1, C2, EV, ES, EW, ETH, EO,
    LV, LS, LW, LTH, LC, LO,
    B, D, X, Z, Y0, Y1, Y2, H, WID, DG, WET, V1, V2,
    BI, BO, PKO, PKI, SPB, XB, RSP, RX, RH, RXH, L1, L2, OUT, DUM,
    rs, ss, ls,
):
    g = lax.axis_index("grp")
    t = lax.axis_index("tile")
    has_l, has_r, has_u, has_d = t > 0, t < T - 1, g > 0, g < G - 1
    lane = lax.broadcasted_iota(jnp.int32, (8, 128), 1)
    sub = lax.broadcasted_iota(jnp.int32, (8, 128), 0)
    zero = jnp.zeros((8, 128), F32)
    first_cap = g // 2
    owner_cap = jnp.where(g == 0, 0, 1)
    is_owner = jnp.logical_or(g == 0, g == G - 1)

    def wait_rows(sem, rows):
        pltpu.make_async_copy(DUM.at[pl.ds(0, rows)], DUM.at[pl.ds(0, rows)], sem).wait()

    def send(src, dst, s, r, dev):
        pltpu.make_async_remote_copy(
            src_ref=src, dst_ref=dst, send_sem=ss.at[s], recv_sem=rs.at[r],
            device_id=dev, device_id_type=MESH,
        ).start()

    def local(src, dst, s):
        pltpu.make_async_copy(src, dst, ls.at[s]).start()

    def cols(j):
        return pl.ds(128 * j, 128)

    nbrs = []
    for dy in (-1, 0, 1):
        for dx in (-1, 0, 1):
            if dy == 0 and dx == 0:
                continue
            cond = None
            for need, there in ((dy < 0, has_u), (dy > 0, has_d), (dx < 0, has_l), (dx > 0, has_r)):
                if need:
                    cond = there if cond is None else jnp.logical_and(cond, there)
            nbrs.append((dy, dx, cond))

    local(iblk, BI.at[1, 1], L_BLK)
    local(land, BO.at[1, 1], L_BLK)
    for j in range(LT):
        local(ivel.at[:, :, :, cols(j)], V.at[:, :, j, pl.ds(16, IR), :], L_ICE)
        local(istr.at[:, :, :, cols(j)], S.at[:, :, j, pl.ds(16, IR), :], L_ICE)
        local(wind.at[:, :, :, cols(j)], W.at[:, :, j, pl.ds(16, IR), :], L_ICE)
        local(thick.at[:, :, cols(j)], TH.at[:, j, pl.ds(16, IR), :], L_ICE)
        local(base.at[:, cols(j)], B.at[j, pl.ds(16, OR), :], L_OC)
        local(depth.at[:, cols(j)], D.at[j, pl.ds(16, OR), :], L_OC)
        local(ssh.at[:, cols(j)], X.at[j, pl.ds(16, OR), :], L_OC)

    barrier = pltpu.get_barrier_semaphore()
    core = lax.rem(t, 2)
    for dy, dx, cond in nbrs:
        @pl.when(cond)
        def _(dy=dy, dx=dx):
            pl.semaphore_signal(barrier, inc=1, device_id=(g + dy, t + dx), device_id_type=MESH)
    peers1 = []
    for dg in range(G):
        for dc in range(2):
            if dg or dc:
                peers1.append((lax.rem(g + dg, G), t - core + lax.rem(core + dc, 2)))
    M2 = T // 2
    mine2 = t // 2
    peers2 = [(g, 2 * lax.rem(mine2 + k, M2) + core) for k in range(1, M2)]
    for dev in peers1 + peers2:
        pl.semaphore_signal(barrier, inc=1, device_id=dev, device_id_type=MESH)
    high = 1 + jnp.minimum(g, 1) + jnp.minimum(G - 1 - g, 1)
    wide = 1 + jnp.minimum(t, 1) + jnp.minimum(T - 1 - t, 1)
    pl.semaphore_wait(barrier, high * wide - 1 + len(peers1) + len(peers2))

    left, right, up, down = (g, t - 1), (g, t + 1), (g - 1, t), (g + 1, t)

    @pl.when(jnp.logical_and(is_owner, has_l))
    def _():
        send(cur.at[:, :, cols(0)], LC.at[1], S_CL, R_CR, left)

    @pl.when(jnp.logical_and(is_owner, has_r))
    def _():
        send(cur.at[:, :, cols(LT - 1)], LC.at[0], S_CR, R_CL, right)

    def flow_rows(d):
        lo, hi = max(IR * d - 8, 0), min(IR * d + IR + 8, OR)
        return lo, hi - lo, 16 + lo - IR * d

    dests = {0: (1, 2, 3), G - 1: (2, 1, 0)}

    def send_flow(c, d):
        lo, n, at = flow_rows(d)
        for j in range(LT):
            send(cur.at[:, pl.ds(lo, n), cols(j)], FL.at[:, c, j, pl.ds(at, n), :],
                 S_F, R_F + c, (d, t))

    def halo_ice(dev, c, src, dst, s, r):
        for j in range(LT):
            send(ivel.at[:, c, pl.ds(src, 8), cols(j)], V.at[:, c, j, pl.ds(dst, 8), :], s, r, dev)
            send(istr.at[:, c, pl.ds(src, 8), cols(j)], S.at[:, c, j, pl.ds(dst, 8), :], s, r, dev)
            send(wind.at[:, c, pl.ds(src, 8), cols(j)], W.at[:, c, j, pl.ds(dst, 8), :], s, r, dev)
            send(thick.at[c, pl.ds(src, 8), cols(j)], TH.at[c, j, pl.ds(dst, 8), :], s, r, dev)

    for own, c in ((0, 0), (G - 1, 1)):
        @pl.when(g == own)
        def _(own=own, c=c):
            send_flow(c, dests[own][0])
            lo, n, at = flow_rows(own)
            for j in range(LT):
                local(cur.at[:, pl.ds(lo, n), cols(j)], FL.at[:, c, j, pl.ds(at, n), :], L_FL)

    for turn in range(2):
        for dev, cond, src, dst, s, r in (
            (up, has_u, 0, IR + 16, S_U, R_ID),
            (down, has_d, IR - 8, 8, S_D, R_IU),
        ):
            @pl.when(cond)
            def _(dev=dev, src=src, dst=dst, s=s, r=r):
                if turn == 0:
                    at = 0 if s == S_U else OR - 8
                    to = OR + 16 if s == S_U else 8
                    ro = R_OD if s == S_U else R_OU
                    for j in range(LT):
                        send(base.at[pl.ds(at, 8), cols(j)], B.at[j, pl.ds(to, 8), :], s, ro, dev)
                        send(depth.at[pl.ds(at, 8), cols(j)], D.at[j, pl.ds(to, 8), :], s, ro, dev)
                        send(ssh.at[pl.ds(at, 8), cols(j)], X.at[j, pl.ds(to, 8), :], s, ro, dev)
                there = dev[0] // 2
                c = there if turn == 0 else 1 - there
                halo_ice(dev, c, src, dst, s, r + c)
        if turn == 0:
            for own, c in ((0, 0), (G - 1, 1)):
                @pl.when(g == own)
                def _(own=own, c=c):
                    for d in dests[own][1:]:
                        send_flow(c, d)

    for dy, dx, cond in nbrs:
        k = 3 * (1 - dy) + (1 - dx)
        @pl.when(cond)
        def _(dy=dy, dx=dx, k=k):
            dev = (g + dy, t + dx)
            send(iblk, BI.at[1 - dy, 1 - dx], S_BI + k, R_BI + k, dev)
            rows = pl.ds(0, OR // BS) if dy == 0 else pl.ds(0 if dy < 0 else OR // BS - 8, 8)
            send(land.at[rows], BO.at[1 - dy, 1 - dx, rows], S_BO + k, R_BO + k, dev)

    for dev, cond, side, at, s, ri, ro in (
        (left, has_l, 1, 0, S_L, R_IR, R_OR),
        (right, has_r, 0, LT - 1, S_R, R_IL, R_OL),
    ):
        @pl.when(cond)
        def _(dev=dev, side=side, at=at, s=s, ri=ri, ro=ro):
            send(ivel.at[:, :, :, cols(at)], LV.at[side], s, ri, dev)
            send(istr.at[:, :, :, cols(at)], LS.at[side], s, ri, dev)
            send(wind.at[:, :, :, cols(at)], LW.at[side], s, ri, dev)
            send(thick.at[:, :, cols(at)], LTH.at[side], s, ri, dev)
            send(base.at[:, cols(at)], LO.at[0, side], s, ro, dev)
            send(depth.at[:, cols(at)], LO.at[1, side], s, ro, dev)
            send(ssh.at[:, cols(at)], LO.at[2, side], s, ro, dev)

    def fill(ref, idx):
        ref[idx] = jnp.zeros(ref.at[idx].shape, ref.dtype)

    for cond, row, orow, by in ((g == 0, 8, 8, 0), (g == G - 1, IR + 16, OR + 16, 2)):
        @pl.when(cond)
        def _(row=row, orow=orow, by=by):
            for c in range(2):
                for j in range(NT):
                    for k in range(3):
                        S[k, c, j, pl.ds(row, 8), :] = zero
                    for k in range(2):
                        V[k, c, j, pl.ds(row, 8), :] = zero
                        W[k, c, j, pl.ds(row, 8), :] = zero
                        FL[k, c, j, pl.ds(row, 8), :] = zero
                    TH[c, j, pl.ds(row, 8), :] = zero
            for j in range(NT):
                B[j, pl.ds(orow, 8), :] = zero
                D[j, pl.ds(orow, 8), :] = zero
                X[j, pl.ds(orow, 8), :] = zero
            for x in range(3):
                for c in range(2):
                    BI[by, x, c] = jnp.zeros((8, 64), jnp.int32)
                BO[by, x] = jnp.zeros((32, 64), jnp.int32)

    for cond, side, bx in ((t == 0, 0, 0), (t == T - 1, 1, 2)):
        @pl.when(cond)
        def _(side=side, bx=bx):
            def body(i, carry):
                r = pl.ds(pl.multiple_of(8 * i, 8), 8)
                for c in range(2):
                    for k in range(3):
                        LS[side, k, c, r, :] = zero
                    for k in range(2):
                        LV[side, k, c, r, :] = zero
                        LW[side, k, c, r, :] = zero
                    LTH[side, c, r, :] = zero
                return carry
            lax.fori_loop(0, IR // 8, body, 0)

            def body2(i, carry):
                r = pl.ds(pl.multiple_of(8 * i, 8), 8)
                for k in range(2):
                    LC[side, k, r, :] = zero
                for k in range(3):
                    LO[k, side, r, :] = zero
                return carry
            lax.fori_loop(0, OR // 8, body2, 0)
            for y in range(3):
                for c in range(2):
                    BI[y, bx, c] = jnp.zeros((8, 64), jnp.int32)
                BO[y, bx] = jnp.zeros((32, 64), jnp.int32)

    for own, c in ((0, 0), (G - 1, 1)):
        @pl.when(g == own)
        def _(own=own, c=c):
            @pl.when(has_l)
            def _():
                wait_rows(rs.at[R_CL], 2 * OR)

            @pl.when(has_r)
            def _():
                wait_rows(rs.at[R_CR], 2 * OR)

            def merged(k, q):
                r = pl.ds(8 * q, 8)
                return jnp.where(lane < 64, LC[1, k, r, :], LC[0, k, r, :])

            for k in range(2):
                for s in range(10):
                    q = 8 * own - 1 + s
                    if 0 <= q < OR // 8:
                        FL[k, c, LT, pl.ds(8 + 8 * s, 8), :] = merged(k, q)
            for at, d in enumerate(dests[own]):
                packs = [zero] * 5
                for k in range(2):
                    for s in range(10):
                        q = 8 * d - 1 + s
                        if 0 <= q < OR // 8:
                            m = 10 * k + s
                            slot = m % 4
                            moved = pltpu.roll(merged(k, q), (32 * slot + 16) % 128, 1)
                            packs[m // 4] = jnp.where(lane // 32 == slot, moved, packs[m // 4])
                for v in range(5):
                    PKO[at, v] = packs[v]
                send(PKO.at[at], PKI.at[c], S_F, R_F + c, (d, t))

    wait_rows(ls.at[L_ICE], 8 * 2 * IR * LT)

    @pl.when(has_l)
    def _():
        wait_rows(rs.at[R_IL], 8 * 2 * IR)

    @pl.when(has_r)
    def _():
        wait_rows(rs.at[R_IR], 8 * 2 * IR)

    for c in range(2):
        def merge_ice(i, carry, c=c):
            r = pl.ds(pl.multiple_of(8 * i, 8), 8)
            w = pl.ds(pl.multiple_of(8 * i + 16, 8), 8)
            for k in range(2):
                V[k, c, LT, w, :] = jnp.where(lane < 64, LV[1, k, c, r, :], LV[0, k, c, r, :])
                W[k, c, LT, w, :] = jnp.where(lane < 64, LW[1, k, c, r, :], LW[0, k, c, r, :])
            for k in range(3):
                S[k, c, LT, w, :] = jnp.where(lane < 64, LS[1, k, c, r, :], LS[0, k, c, r, :])
            TH[c, LT, w, :] = jnp.where(lane < 64, LTH[1, c, r, :], LTH[0, c, r, :])
            return carry
        lax.fori_loop(0, IR // 8, merge_ice, 0)

    for e, dev, cond, src, dst, s, r in (
        (0, up, has_u, 16, IR + 16, S_U, R_ID),
        (1, down, has_d, IR + 8, 8, S_D, R_IU),
    ):
        @pl.when(cond)
        def _(e=e, dev=dev, src=src, dst=dst, s=s, r=r):
            a, b = pl.ds(src, 8), pl.ds(dst, 8)
            for c in range(2):
                for k in range(3):
                    ES[e, k, c] = S[k, c, LT, a, :]
                for k in range(2):
                    EV[e, k, c] = V[k, c, LT, a, :]
                    EW[e, k, c] = W[k, c, LT, a, :]
                ETH[e, c] = TH[c, LT, a, :]
            for turn in range(2):
                there = dev[0] // 2
                c = there if turn == 0 else 1 - there
                send(EV.at[e, :, c], V.at[:, c, LT, b, :], s, r + c, dev)
                send(ES.at[e, :, c], S.at[:, c, LT, b, :], s, r + c, dev)
                send(EW.at[e, :, c], W.at[:, c, LT, b, :], s, r + c, dev)
                send(ETH.at[e, c], TH.at[c, LT, b, :], s, r + c, dev)

    wait_rows(ls.at[L_OC], 3 * OR * LT)

    @pl.when(has_l)
    def _():
        wait_rows(rs.at[R_OL], 3 * OR)

    @pl.when(has_r)
    def _():
        wait_rows(rs.at[R_OR], 3 * OR)

    def merge_ocean(i, carry):
        r = pl.ds(pl.multiple_of(8 * i, 8), 8)
        w = pl.ds(pl.multiple_of(8 * i + 16, 8), 8)
        for k, ref in enumerate((B, D, X)):
            ref[LT, w, :] = jnp.where(lane < 64, LO[k, 1, r, :], LO[k, 0, r, :])
        return carry
    lax.fori_loop(0, OR // 8, merge_ocean, 0)
    for e, dev, cond, src, dst, s, r in (
        (0, up, has_u, 16, OR + 16, S_U, R_OD),
        (1, down, has_d, OR + 8, 8, S_D, R_OU),
    ):
        @pl.when(cond)
        def _(e=e, dev=dev, src=src, dst=dst, s=s, r=r):
            for k, ref in enumerate((B, D, X)):
                EO[e, k] = ref[LT, pl.ds(src, 8), :]
            for k, ref in enumerate((B, D, X)):
                send(EO.at[e, k], ref.at[LT, pl.ds(dst, 8), :], s, r, dev)

    pltpu.make_async_copy(iblk, BI.at[1, 1], ls.at[L_BLK]).wait()
    pltpu.make_async_copy(land, BO.at[1, 1], ls.at[L_BLK]).wait()
    for dy, dx, cond in nbrs:
        k = 3 * (1 + dy) + (1 + dx)
        @pl.when(cond)
        def _(dy=dy, dx=dx, k=k):
            dev = (g + dy, t + dx)
            pltpu.make_async_remote_copy(
                src_ref=iblk, dst_ref=BI.at[1 + dy, 1 + dx], send_sem=ss.at[S_BI + k],
                recv_sem=rs.at[R_BI + k], device_id=dev, device_id_type=MESH).wait_recv()
            rows = pl.ds(0, OR // BS) if dy == 0 else pl.ds(OR // BS - 8 if dy < 0 else 0, 8)
            pltpu.make_async_remote_copy(
                src_ref=land.at[rows], dst_ref=BO.at[1 + dy, 1 + dx, rows], send_sem=ss.at[S_BO + k],
                recv_sem=rs.at[R_BO + k], device_id=dev, device_id_type=MESH).wait_recv()

    def selection(width, first, start):
        block = lax.broadcasted_iota(jnp.int32, (64, width), 0)
        at = lax.broadcasted_iota(jnp.int32, (64, width), 1)
        hit = block == at // BS + first
        if start is not None:
            hit = jnp.logical_and(hit, (at < 64) if start == 0 else (at >= 64))
        return hit.astype(F32)

    sel_c = selection(128 * LT, 0, None)
    sel_r = selection(128, 0, 0)
    sel_l = selection(128, 48, 1)

    def spread_rows(refs):
        lft, mid, rgt = (ref.astype(F32) for ref in refs)
        wide = jnp.dot(mid, sel_c, preferred_element_type=F32)
        last = jnp.dot(rgt, sel_r, preferred_element_type=F32) + jnp.dot(
            lft, sel_l, preferred_element_type=F32)
        return wide, last

    def paint(ref, row, parts, b):
        wide, last = parts
        for j in range(LT):
            ref[j, pl.ds(row, 8), :] = jnp.broadcast_to(wide[b:b + 1, 128 * j:128 * j + 128], (8, 128))
        ref[LT, pl.ds(row, 8), :] = jnp.broadcast_to(last[b:b + 1, :], (8, 128))

    for c in range(2):
        cov = CV.at[c]
        paint(cov, 8, spread_rows([BI[0, x, c] for x in range(3)]), 7)
        mid = spread_rows([BI[1, x, c] for x in range(3)])
        for b in range(8):
            paint(cov, 16 + 8 * b, mid, b)
        paint(cov, IR + 16, spread_rows([BI[2, x, c] for x in range(3)]), 0)
    paint(WET, 8, spread_rows([BO[0, x, 24:32] for x in range(3)]), 7)
    for q in range(4):
        mid = spread_rows([BO[1, x, 8 * q:8 * q + 8] for x in range(3)])
        for b in range(8):
            paint(WET, 16 + 64 * q + 8 * b, mid, b)
    paint(WET, OR + 16, spread_rows([BO[2, x, 0:8] for x in range(3)]), 0)

    def cap(c):
        @pl.when(has_u)
        def _():
            wait_rows(rs.at[R_IU + c], 8 * 8 * NT)

        @pl.when(has_d)
        def _():
            wait_rows(rs.at[R_ID + c], 8 * 8 * NT)

        mine = jnp.logical_and(is_owner, c == owner_cap)
        at_end = jnp.logical_or(jnp.logical_and(c == 0, g == G - 1), jnp.logical_and(c == 1, g == 0))

        @pl.when(mine)
        def _():
            wait_rows(ls.at[L_FL], 2 * (IR + 8) * LT)

        @pl.when(jnp.logical_not(mine))
        def _():
            @pl.when(at_end)
            def _():
                wait_rows(rs.at[R_F + c], 2 * (IR + 8) * LT + 40)

            @pl.when(jnp.logical_not(at_end))
            def _():
                wait_rows(rs.at[R_F + c], 2 * (IR + 16) * LT + 40)

            for k in range(2):
                for s in range(10):
                    m = 10 * k + s
                    FL[k, c, LT, pl.ds(8 + 8 * s, 8), :] = pltpu.roll(
                        PKI[c, m // 4], (128 - (32 * (m % 4) + 16)) % 128, 1)

        def prepare(i, carry):
            r = pl.ds(pl.multiple_of(8 * i + 8, 8), 8)
            for j in range(NT):
                cov = CV[c, j, r, :]
                thc = TH[c, j, r, :] * cov
                scale = cov / (thc + (1.0 + STEP * DRAG))
                C1[c, j, r, :] = scale * (thc + 1.0)
                C2[c, j, r, :] = scale * STEP
                TH[c, j, r, :] = thc * (RELAX * STRENGTH / (1.0 + RELAX))
                for k in range(2):
                    W[k, c, j, r, :] = W[k, c, j, r, :] + FL[k, c, j, r, :] * DRAG
            return carry
        lax.fori_loop(0, IR // 8 + 2, prepare, 0)

        keep = 1.0 / (1.0 + RELAX)

        def group(r):
            rr = pl.ds(r, 8)
            u = [V[0, c, j, rr, :] for j in range(NT)]
            v = [V[1, c, j, rr, :] for j in range(NT)]
            ue, ve = east(u, lane), east(v, lane)
            s0, s1, s2 = [], [], []
            for j in range(NT):
                dux = V[0, c, j, pl.ds(r + 1, 8), :] - u[j]
                dvx = V[1, c, j, pl.ds(r + 1, 8), :] - v[j]
                duy, dvy = ue[j] - u[j], ve[j] - v[j]
                ed, et, es = dux + dvy, dux - dvy, duy + dvx
                inv = lax.rsqrt(ed * ed + et * et + es * es + 1.0)
                a = TH[c, j, rr, :]
                ai = a * inv
                s0.append(S[0, c, j, rr, :] * keep + (ed * ai - a))
                s1.append(S[1, c, j, rr, :] * keep + et * ai)
                s2.append(S[2, c, j, rr, :] * keep + es * ai)
                S[0, c, j, rr, :] = s0[j]
                S[1, c, j, rr, :] = s1[j]
                S[2, c, j, rr, :] = s2[j]
            dif = [s0[j] - s1[j] for j in range(NT)]
            dw, sw = west(dif, lane), west(s2, lane)
            above = pl.ds(r - 1, 8)
            for j in range(NT):
                tot_up = S[0, c, j, above, :] + S[1, c, j, above, :]
                f0 = 0.5 * ((s0[j] + s1[j]) - tot_up) + (s2[j] - sw[j])
                f1 = 0.5 * (dif[j] - dw[j]) + (s2[j] - S[2, c, j, above, :])
                c1, c2 = C1[c, j, rr, :], C2[c, j, rr, :]
                V[0, c, j, rr, :] = c1 * u[j] + c2 * (f0 + W[0, c, j, rr, :])
                V[1, c, j, rr, :] = c1 * v[j] + c2 * (f1 + W[1, c, j, rr, :])

        def subcycle(n, carry):
            for i in range(IR // 8 + 2):
                group(8 + 8 * i)
            return carry
        lax.fori_loop(0, NSUB, subcycle, 0)

        for j in range(LT):
            local(V.at[:, c, j, pl.ds(16, IR), :], o_vel.at[:, c, :, cols(j)], L_OUT)
            local(S.at[:, c, j, pl.ds(16, IR), :], o_str.at[:, c, :, cols(j)], L_OUT)

        prev = [zero] * NT
        pack = zero
        for i in range(IR // 8):
            rr = pl.ds(16 + 8 * i, 8)
            p0, p1 = [], []
            for j in range(NT):
                cov = CV[c, j, rr, :] * DRAG
                p0.append(cov * (V[0, c, j, rr, :] - FL[0, c, j, rr, :]))
                p1.append(cov * (V[1, c, j, rr, :] - FL[1, c, j, rr, :]))
            pw = west(p1, lane)
            for j in range(NT):
                turned = pltpu.roll(p0[j], 1, 0)
                above = jnp.where(sub == 0, prev[j], turned)
                prev[j] = turned
                sp = (p0[j] - above) + (p1[j] - pw[j])
                if j < LT:
                    SPB[c, j, pl.ds(8 * i, 8), :] = sp
                else:
                    pack = jnp.where(lane // 16 == i, pltpu.roll(sp, 16 * i + 8, 1), pack)
        XB[c, 0] = pack
        extra = zero
        for j in range(NT):
            extra = jnp.where(sub == j, -jnp.broadcast_to(prev[j][0:1, :], (8, 128)), extra)
        XB[c, 1] = extra

        @pl.when(mine)
        def _():
            for j in range(LT):
                for i in range(IR // 8):
                    RSP[g, j, pl.ds(8 * i, 8), :] = SPB[c, j, pl.ds(8 * i, 8), :]
            RX[g, 0] = XB[c, 0]
            RX[g, 1] = XB[c, 1]

        @pl.when(jnp.logical_not(mine))
        def _():
            dev = (c * (G - 1), t)
            send(SPB.at[c], RSP.at[g], S_RS + c, R_RS + g, dev)
            send(XB.at[c], RX.at[g], S_RS + c, R_RS + g, dev)

        @pl.when(at_end)
        def _():
            at = jnp.where(c == 0, IR - 8, 0)
            dev = (1 + c, t)
            send(SPB.at[c, :, pl.ds(pl.multiple_of(at, 8), 8), :], RH, S_RH, R_RH, dev)
            send(XB.at[c], RXH, S_RH, R_RH, dev)

    def caps(turn, carry):
        cap(jnp.where(turn == 0, first_cap, 1 - first_cap))
        return carry

    def ocean_rows(body, carry, unroll=2):
        def step(i, cc):
            for m in range(unroll):
                cc = body(pl.multiple_of(8 * (unroll * i + m) + 16, 8), cc)
            return cc
        return lax.fori_loop(0, OR // 8 // unroll, step, carry)

    def shifted_sum(ref, r):
        rr = pl.ds(r, 8)
        mid = [ref[j, rr, :] for j in range(NT)]
        e, w = east(mid, lane), west(mid, lane)
        return mid, [
            (ref[j, pl.ds(r + 1, 8), :] + ref[j, pl.ds(r - 1, 8), :]) + (e[j] + w[j])
            for j in range(NT)
        ]

    def ocean_prepare():
        @pl.when(has_u)
        def _():
            wait_rows(rs.at[R_OU], 24 * NT)

        @pl.when(has_d)
        def _():
            wait_rows(rs.at[R_OD], 24 * NT)

        def first(r, carry):
            rr = pl.ds(r, 8)
            for j in range(NT):
                gg = D[j, rr, :] * WET[j, rr, :]
                D[j, rr, :] = gg
                Y0[j, rr, :] = gg * X[j, rr, :]
            return carry

        def second(r, carry):
            rr = pl.ds(r, 8)
            gs, gn = shifted_sum(D, r)
            _, xn = shifted_sum(Y0, r)
            for j in range(NT):
                diag = gs[j] * gn[j] + DAMP
                inv = 1.0 / diag
                wid = WET[j, rr, :] * inv
                h = gs[j] * inv
                DG[j, rr, :] = diag
                WID[j, rr, :] = wid
                H[j, rr, :] = h
                Z[j, rr, :] = wid * B[j, rr, :] + h * xn[j] - X[j, rr, :]
            return carry
        for body in (first, second):
            body(8, 0)
            ocean_rows(body, 0)
            body(OR + 16, 0)

    def both(turn, carry):
        @pl.when(turn == 1)
        def _():
            ocean_prepare()
        return caps(turn, carry)
    lax.fori_loop(0, 2, both, 0)

    @pl.when(is_owner)
    def _():
        for d in range(G):
            @pl.when(g != d)
            def _(d=d):
                wait_rows(rs.at[R_RS + d], LT * IR + 16)
        for d in range(G):
            for i in range(IR // 8):
                rr = pl.ds(16 + IR * d + 8 * i, 8)
                for j in range(NT):
                    if j < LT:
                        sp = RSP[d, j, pl.ds(8 * i, 8), :]
                    else:
                        sp = pltpu.roll(RX[d, 0], 128 - (16 * i + 8), 1)
                    if i == 0 and d > 0:
                        more = jnp.broadcast_to(RX[d - 1, 1][j:j + 1, :], (8, 128))
                        sp = sp + jnp.where(sub == 0, more, 0.0)
                    Z[j, rr, :] = Z[j, rr, :] + WID[j, rr, :] * sp

    @pl.when(g == 0)
    def _():
        rr = pl.ds(OR + 16, 8)
        for j in range(NT):
            more = jnp.broadcast_to(RX[G - 1, 1][j:j + 1, :], (8, 128))
            Z[j, rr, :] = Z[j, rr, :] + WID[j, rr, :] * jnp.where(sub == 0, more, 0.0)

    @pl.when(jnp.logical_not(is_owner))
    def _():
        wait_rows(rs.at[R_RH], LT * 8 + 16)

        @pl.when(g == 1)
        def _():
            rr = pl.ds(16, 8)
            for j in range(NT):
                more = jnp.broadcast_to(RXH[1][j:j + 1, :], (8, 128))
                Z[j, rr, :] = Z[j, rr, :] + WID[j, rr, :] * jnp.where(sub == 0, more, 0.0)
        for at, row, i in ((1, 8, 7), (2, OR + 16, 0)):
            @pl.when(g == at)
            def _(row=row, i=i):
                rr = pl.ds(row, 8)
                for j in range(NT):
                    sp = RH[j] if j < LT else pltpu.roll(RXH[0], 128 - (16 * i + 8), 1)
                    Z[j, rr, :] = Z[j, rr, :] + WID[j, rr, :] * sp

    def krylov0(r, acc):
        rr = pl.ds(r, 8)
        for j in range(NT):
            z = Z[j, rr, :]
            Y0[j, rr, :] = D[j, rr, :] * z
            if j < LT and acc is not None:
                acc = acc + DG[j, rr, :] * z * z
        return acc

    def krylov(src, dst, vec, r, acc):
        rr = pl.ds(r, 8)
        y, n = shifted_sum(src, r)
        if acc is not None:
            odd, even = acc
        for j in range(NT):
            v = H[j, rr, :] * n[j]
            out = D[j, rr, :] * v
            vec[j, rr, :] = v
            dst[j, rr, :] = out
            if j < LT and acc is not None:
                odd = odd + y[j] * n[j]
                even = even + out * n[j]
        return None if acc is None else (odd, even)

    def last(r, acc):
        y, n = shifted_sum(Y2, r)
        for j in range(LT):
            acc = acc + y[j] * n[j]
        return acc

    krylov0(8, None)
    krylov0(OR + 16, None)
    moments = [ocean_rows(krylov0, zero)]
    for src, dst, vec in ((Y0, Y1, V1), (Y1, Y2, V2)):
        step = functools.partial(krylov, src, dst, vec)
        step(8, None)
        step(OR + 16, None)
        moments += list(ocean_rows(step, (zero, zero)))
    moments.append(ocean_rows(last, zero))

    tile = zero
    for k, m in enumerate(moments):
        tile = jnp.where(sub == k, jnp.sum(m, axis=0, keepdims=True), tile)
    slot1 = 2 * g + core
    L1[slot1] = tile
    for dev in peers1:
        send(L1.at[slot1], L1.at[slot1], S_1, R_1, dev)
    wait_rows(rs.at[R_1], 8 * len(peers1))
    tile = L1[0]
    for k in range(1, 8):
        tile = tile + L1[k]
    L2[mine2] = tile
    for dev in peers2:
        send(L2.at[mine2], L2.at[mine2], S_2, R_2, dev)
    wait_rows(rs.at[R_2], 8 * len(peers2))
    tile = L2[0]
    for k in range(1, M2):
        tile = tile + L2[k]
    total = jnp.sum(tile, axis=1, keepdims=True)
    mu = [total[k:k + 1, :] for k in range(6)]
    nu = [mu[k] - mu[k + 1] for k in range(5)]

    a0 = mu[0] / nu[0]
    z10, z11 = 1.0 - a0, a0
    rz1 = z11 * (z10 * mu[1] + z11 * mu[2])
    b0 = rz1 / mu[0]
    p10, p11 = z10 + b0, z11
    a1 = rz1 / (p11 * (p10 * nu[1] + p11 * nu[2]))
    z20, z21, z22 = z10 - a1 * p10, z11 - a1 * (p11 - p10), a1 * p11
    rz2 = z22 * (z20 * mu[2] + z21 * mu[3] + z22 * mu[4])
    b1 = rz2 / rz1
    p20, p21, p22 = z20 + b1 * p10, z21 + b1 * p11, z22
    a2 = rz2 / (p22 * (p20 * nu[2] + p21 * nu[3] + p22 * nu[4]))
    k0 = jnp.broadcast_to(a0 + a1 * p10 + a2 * p20, (8, 128))
    k1 = jnp.broadcast_to(a1 * p11 + a2 * p21, (8, 128))
    k2 = jnp.broadcast_to(a2 * p22, (8, 128))

    def finish(r, carry):
        rr = pl.ds(r, 8)
        for j in range(LT):
            OUT[j, pl.ds(pl.multiple_of(r - 16, 8), 8), :] = X[j, rr, :] + (
                k0 * Z[j, rr, :] + (k1 * V1[j, rr, :] + k2 * V2[j, rr, :]))
        return carry
    ocean_rows(finish, 0)
    for j in range(LT):
        local(OUT.at[j], o_ssh.at[:, cols(j)], L_OUTS)
    wait_rows(ls.at[L_OUTS], OR * LT)
    wait_rows(ls.at[L_OUT], 5 * 2 * IR * LT)

    for s, cond in ((S_CL, jnp.logical_and(is_owner, has_l)), (S_CR, jnp.logical_and(is_owner, has_r))):
        @pl.when(cond)
        def _(s=s):
            wait_rows(ss.at[s], 2 * OR)
    for s, cond in ((S_L, has_l), (S_R, has_r)):
        @pl.when(cond)
        def _(s=s):
            wait_rows(ss.at[s], 8 * 2 * IR + 3 * OR)
    for s, cond in ((S_U, has_u), (S_D, has_d)):
        @pl.when(cond)
        def _(s=s):
            wait_rows(ss.at[s], (8 * 2 + 3) * 8 * NT)

    @pl.when(is_owner)
    def _():
        wait_rows(ss.at[S_F], 2 * LT * (2 * (IR + 16) + IR + 8) + 3 * 40)
    for c in range(2):
        mine = jnp.logical_and(is_owner, c == owner_cap)

        @pl.when(jnp.logical_not(mine))
        def _(c=c):
            wait_rows(ss.at[S_RS + c], LT * IR + 16)

    @pl.when(is_owner)
    def _():
        wait_rows(ss.at[S_RH], LT * 8 + 16)
    wait_rows(ss.at[S_1], 8 * len(peers1))
    wait_rows(ss.at[S_2], 8 * len(peers2))
    for dy, dx, cond in nbrs:
        k = 3 * (1 - dy) + (1 - dx)
        @pl.when(cond)
        def _(dy=dy, dx=dx, k=k):
            dev = (g + dy, t + dx)
            pltpu.make_async_remote_copy(
                src_ref=iblk, dst_ref=BI.at[1 - dy, 1 - dx], send_sem=ss.at[S_BI + k],
                recv_sem=rs.at[R_BI + k], device_id=dev, device_id_type=MESH).wait_send()
            rows = pl.ds(0, OR // BS) if dy == 0 else pl.ds(0 if dy < 0 else OR // BS - 8, 8)
            pltpu.make_async_remote_copy(
                src_ref=land.at[rows], dst_ref=BO.at[1 - dy, 1 - dx, rows], send_sem=ss.at[S_BO + k],
                recv_sem=rs.at[R_BO + k], device_id=dev, device_id_type=MESH).wait_send()


def shards(T, *args):
    ice = (2, NT, IH, 128)
    ocean = (NT, OH, 128)
    vm = lambda *s: pltpu.VMEM(s, F32)
    scratch = [
        vm(2, *ice), vm(3, *ice), vm(2, *ice), vm(*ice), vm(2, *ice), vm(*ice), vm(*ice), vm(*ice),
        vm(2, 2, 2, 8, 128), vm(2, 3, 2, 8, 128), vm(2, 2, 2, 8, 128), vm(2, 2, 8, 128), vm(2, 3, 8, 128),
        vm(2, 2, 2, IR, 128), vm(2, 3, 2, IR, 128), vm(2, 2, 2, IR, 128), vm(2, 2, IR, 128),
        vm(2, 2, OR, 128), vm(3, 2, OR, 128),
        *[vm(*ocean) for _ in range(13)],
        pltpu.VMEM((3, 3, 2, 8, 64), jnp.int32), pltpu.VMEM((3, 3, 32, 64), jnp.int32),
        vm(3, 5, 8, 128), vm(2, 5, 8, 128), vm(2, LT, IR, 128), vm(2, 2, 8, 128),
        vm(G, LT, IR, 128), vm(G, 2, 8, 128), vm(LT, 8, 128), vm(2, 8, 128),
        vm(8, 8, 128), vm(T // 2, 8, 128), vm(LT, OR, 128), vm(DUMMY, 128),
        pltpu.SemaphoreType.DMA((N_R,)), pltpu.SemaphoreType.DMA((N_S,)), pltpu.SemaphoreType.DMA((N_L,)),
    ]
    hbm = pl.BlockSpec(memory_space=pltpu.HBM)
    return pl.pallas_call(
        functools.partial(kernel, T),
        out_shape=(
            jax.ShapeDtypeStruct((OR, 128 * LT), F32),
            jax.ShapeDtypeStruct((2, 2, IR, 128 * LT), F32),
            jax.ShapeDtypeStruct((3, 2, IR, 128 * LT), F32),
        ),
        in_specs=[hbm] * 10,
        out_specs=(hbm, hbm, hbm),
        scratch_shapes=scratch,
        compiler_params=pltpu.CompilerParams(
            collective_id=0, has_side_effects=True, vmem_limit_bytes=60 * 1024 * 1024),
    )(*args)


def solution(mesh):
    return jax.shard_map(
        functools.partial(shards, mesh.shape["tile"]),
        mesh=mesh,
        in_specs=(
            P("grp", "tile"),
            P("grp", "tile"),
            P("grp", "tile"),
            P(None, "grp", "tile"),
            P("grp", "tile"),
            P(None, "grp", "tile"),
            P(None, "grp", "tile"),
            P(None, None, "grp", "tile"),
            P(None, None, "grp", "tile"),
            P(None, None, "grp", "tile"),
        ),
        out_specs=(P("grp", "tile"), P(None, None, "grp", "tile"), P(None, None, "grp", "tile")),
        check_vma=False,
    )
```

```python
import functools

import jax
import jax.numpy as jnp
from jax import lax
from jax.experimental import pallas as pl
from jax.experimental.pallas import tpu as pltpu
from jax.sharding import PartitionSpec as P

BS = 8
NSUB = 8
DAMP = 0.05
RELAX = 0.2
STRENGTH = 0.5
DRAG = 1.0
STEP = 0.5
G = 4
LT = 4
NT = LT + 1
IR = 64
OR = 256
IH = IR + 32
OH = OR + 32
F32 = jnp.float32
MESH = pl.DeviceIdType.MESH
DUMMY = 4096

R_PL, R_PR, R_IL, R_IR, R_OL, R_OR = 41, 43, 4, 5, 6, 7
R_IU, R_ID, R_F = 8, 10, 12
R_OU, R_OD, R_RS, R_RH, R_1, R_2 = 14, 15, 16, 20, 21, 22
R_BI, R_BO = 23, 32
N_R = 45
S_FL, S_FR, S_L, S_R, S_U, S_D, S_F, S_RS, S_1, S_2 = 0, 1, 2, 3, 4, 5, 6, 7, 9, 10
S_RH = 11
S_BI, S_BO = 12, 21
N_S = 30
L_BLK, L_ICE, L_FL, L_OC, L_OUT, L_OUTS, L_ED = 0, 1, 2, 3, 4, 5, 6
N_L = 7


def east(tiles, lane):
    turned = [pltpu.roll(x, 127, 1) for x in tiles]
    return [jnp.where(lane == 127, turned[(j + 1) % NT], turned[j]) for j in range(NT)]


def west(tiles, lane):
    turned = [pltpu.roll(x, 1, 1) for x in tiles]
    return [jnp.where(lane == 0, turned[(j - 1) % NT], turned[j]) for j in range(NT)]


class Phases:
    def __init__(self):
        self.open = None

    def __call__(self, name):
        if self.open is not None:
            self.open.__exit__(None, None, None)
        self.open = None
        if name:
            self.open = jax.named_scope(name)
            self.open.__enter__()


def kernel(
    T,
    base, depth, ssh, cur, land, thick, iblk, ivel, istr, wind,
    o_ssh, o_vel, o_str,
    V, S, W, TH, FL, CV, C1, C2,
    PI, LI, PC, LC, PF, LF, PH, LH, PHO, LHO, CE,
    B, D, X, Z, Y0, Y1, Y2, H, WID, DG, WET, V1, V2,
    BI, BO, SPB, XB, RSP, RX, RH, RXH, L1, L2, OUT, DUM,
    rs, ss, ls,
):
    g = lax.axis_index("grp")
    t = lax.axis_index("tile")
    has_l, has_r, has_u, has_d = t > 0, t < T - 1, g > 0, g < G - 1
    lane = lax.broadcasted_iota(jnp.int32, (8, 128), 1)
    sub = lax.broadcasted_iota(jnp.int32, (8, 128), 0)
    zero = jnp.zeros((8, 128), F32)
    first_cap = g // 2
    owner_cap = jnp.where(g == 0, 0, 1)
    is_owner = jnp.logical_or(g == 0, g == G - 1)

    def wait_rows(sem, rows):
        pltpu.make_async_copy(DUM.at[pl.ds(0, rows)], DUM.at[pl.ds(0, rows)], sem).wait()

    def send(src, dst, s, r, dev):
        pltpu.make_async_remote_copy(
            src_ref=src, dst_ref=dst, send_sem=ss.at[s], recv_sem=rs.at[r],
            device_id=dev, device_id_type=MESH,
        ).start()

    def local(src, dst, s):
        pltpu.make_async_copy(src, dst, ls.at[s]).start()

    def cols(j):
        return pl.ds(128 * j, 128)

    nbrs = []
    for dy in (-1, 0, 1):
        for dx in (-1, 0, 1):
            if dy == 0 and dx == 0:
                continue
            cond = None
            for need, there in ((dy < 0, has_u), (dy > 0, has_d), (dx < 0, has_l), (dx > 0, has_r)):
                if need:
                    cond = there if cond is None else jnp.logical_and(cond, there)
            nbrs.append((dy, dx, cond))

    phase = Phases()
    phase("loads")
    local(iblk, BI.at[1, 1], L_BLK)
    local(land, BO.at[1, 1], L_BLK)
    for j in range(LT):
        local(ivel.at[:, :, :, cols(j)], V.at[:, :, j, pl.ds(16, IR), :], L_ICE)
        local(istr.at[:, :, :, cols(j)], S.at[:, :, j, pl.ds(16, IR), :], L_ICE)
        local(wind.at[:, :, :, cols(j)], W.at[:, :, j, pl.ds(16, IR), :], L_ICE)
        local(thick.at[:, :, cols(j)], TH.at[:, j, pl.ds(16, IR), :], L_ICE)
        local(base.at[:, cols(j)], B.at[j, pl.ds(16, OR), :], L_OC)
        local(depth.at[:, cols(j)], D.at[j, pl.ds(16, OR), :], L_OC)
        local(ssh.at[:, cols(j)], X.at[j, pl.ds(16, OR), :], L_OC)

    @pl.when(is_owner)
    def _():
        local(cur.at[:, :, cols(0)], CE.at[0], L_ED)
        local(cur.at[:, :, cols(LT - 1)], CE.at[1], L_ED)

    phase("signal")
    barrier = pltpu.get_barrier_semaphore()
    core = lax.rem(t, 2)
    M2 = T // 2
    mine2 = t // 2
    peers1 = []
    for dg in range(G):
        for dc in range(2):
            if dg or dc:
                peers1.append((lax.rem(g + dg, G), t - core + lax.rem(core + dc, 2)))
    peers2 = [(g, 2 * lax.rem(mine2 + k, M2) + core) for k in range(1, M2)]
    for dg in range(G):
        for dx, cond in ((-1, has_l), (0, None), (1, has_r)):
            dev = (lax.rem(g + dg, G), t + dx)
            if cond is not None:
                @pl.when(cond)
                def _(dev=dev):
                    pl.semaphore_signal(barrier, inc=1, device_id=dev, device_id_type=MESH)
            elif dg:
                pl.semaphore_signal(barrier, inc=1, device_id=dev, device_id_type=MESH)
    for dev in peers2:
        pl.semaphore_signal(barrier, inc=1, device_id=dev, device_id_type=MESH)

    phase("zeros")
    for cond, row, orow, by in ((g == 0, 8, 8, 0), (g == G - 1, IR + 16, OR + 16, 2)):
        @pl.when(cond)
        def _(row=row, orow=orow, by=by):
            for c in range(2):
                for j in range(NT):
                    for k in range(3):
                        S[k, c, j, pl.ds(row, 8), :] = zero
                    for k in range(2):
                        V[k, c, j, pl.ds(row, 8), :] = zero
                        W[k, c, j, pl.ds(row, 8), :] = zero
                        FL[k, c, j, pl.ds(row, 8), :] = zero
                    TH[c, j, pl.ds(row, 8), :] = zero
            for j in range(NT):
                B[j, pl.ds(orow, 8), :] = zero
                D[j, pl.ds(orow, 8), :] = zero
                X[j, pl.ds(orow, 8), :] = zero
            for x in range(3):
                for c in range(2):
                    BI[by, x, c] = jnp.zeros((8, 64), jnp.int32)
                BO[by, x] = jnp.zeros((32, 64), jnp.int32)

    for cond, side, bx in ((t == 0, 0, 0), (t == T - 1, 1, 2)):
        @pl.when(cond)
        def _(side=side, bx=bx):
            for c in range(2):
                for k in range(8):
                    LI[side, c, k] = zero
                for v in range(3):
                    LF[side, c, v] = zero
            for k in range(3):
                for v in range(4):
                    LC[side, k, v] = zero
            for y in range(3):
                for c in range(2):
                    BI[y, bx, c] = jnp.zeros((8, 64), jnp.int32)
                BO[y, bx] = jnp.zeros((32, 64), jnp.int32)

    phase("pack")
    slot_of = lane // 16

    def put(pack, e, at, x):
        moved = pltpu.roll(x, 16 * at, 1) if at else x
        return jnp.where(slot_of == (at - e) % 8, moved, pack)

    def take(from_right, from_left, at):
        both = jnp.where(slot_of == at, from_right, from_left)
        return pltpu.roll(both, 128 - 16 * at, 1) if at else both

    wait_rows(ls.at[L_ICE], 8 * 2 * IR * LT)

    def ice_get(k, c, j, r):
        if k < 2:
            return V[k, c, j, pl.ds(r, 8), :]
        if k < 5:
            return S[k - 2, c, j, pl.ds(r, 8), :]
        return W[k - 5, c, j, pl.ds(r, 8), :] if k < 7 else TH[c, j, pl.ds(r, 8), :]

    def ice_set(k, c, j, r, x):
        if k < 2:
            V[k, c, j, pl.ds(r, 8), :] = x
        elif k < 5:
            S[k - 2, c, j, pl.ds(r, 8), :] = x
        elif k < 7:
            W[k - 5, c, j, pl.ds(r, 8), :] = x
        else:
            TH[c, j, pl.ds(r, 8), :] = x

    for e, j in ((0, 0), (1, LT - 1)):
        for c in range(2):
            for k in range(8):
                pack = zero
                for i in range(IR // 8):
                    pack = put(pack, e, i, ice_get(k, c, j, 16 + 8 * i))
                PI[e, c, k] = pack

    for own in (0, G - 1):
        @pl.when(g == own)
        def _(own=own):
            wait_rows(ls.at[L_ED], 2 * 2 * OR)
            for e in range(2):
                for d in range(G):
                    packs = [zero] * 3
                    for k in range(2):
                        for s in range(10):
                            q = 8 * d - 1 + s
                            if 0 <= q < OR // 8:
                                m = 10 * k + s
                                packs[m // 8] = put(packs[m // 8], e, m % 8, CE[e, k, pl.ds(8 * q, 8), :])
                    for v in range(3):
                        PF[e, d, v] = packs[v]

    wait_rows(ls.at[L_OC], 3 * OR * LT)
    for e, j in ((0, 0), (1, LT - 1)):
        for k, ref in enumerate((B, D, X)):
            for v in range(4):
                pack = zero
                for i in range(8):
                    pack = put(pack, e, i, ref[j, pl.ds(16 + 64 * v + 8 * i, 8), :])
                PC[e, k, v] = pack

    phase("barrier")
    wide = 1 + jnp.minimum(t, 1) + jnp.minimum(T - 1 - t, 1)
    pl.semaphore_wait(barrier, G * wide - 1 + len(peers2))

    phase("sends")
    left, right, up, down = (g, t - 1), (g, t + 1), (g - 1, t), (g + 1, t)
    for dy, dx, cond in nbrs:
        k = 3 * (1 - dy) + (1 - dx)
        @pl.when(cond)
        def _(dy=dy, dx=dx, k=k):
            dev = (g + dy, t + dx)
            send(iblk, BI.at[1 - dy, 1 - dx], S_BI + k, R_BI + k, dev)
            rows = pl.ds(0, OR // BS) if dy == 0 else pl.ds(0 if dy < 0 else OR // BS - 8, 8)
            send(land.at[rows], BO.at[1 - dy, 1 - dx, rows], S_BO + k, R_BO + k, dev)

    for e, dev, cond, s, ri, ro in ((0, left, has_l, S_L, R_IR, R_OR), (1, right, has_r, S_R, R_IL, R_OL)):
        @pl.when(cond)
        def _(e=e, dev=dev, s=s, ri=ri, ro=ro):
            send(PI.at[e], LI.at[1 - e], s, ri, dev)
            send(PC.at[e], LC.at[1 - e], s, ro, dev)

    def flow_rows(d):
        lo, hi = max(IR * d - 8, 0), min(IR * d + IR + 8, OR)
        return lo, hi - lo, 16 + lo - IR * d

    dests = {0: (1, 2, 3), G - 1: (2, 1, 0)}

    def send_flow(c, d):
        lo, n, at = flow_rows(d)
        for j in range(LT):
            send(cur.at[:, pl.ds(lo, n), cols(j)], FL.at[:, c, j, pl.ds(at, n), :],
                 S_F, R_F + c, (d, t))

    def halo_ice(dev, c, src, dst, s, r):
        for j in range(LT):
            send(ivel.at[:, c, pl.ds(src, 8), cols(j)], V.at[:, c, j, pl.ds(dst, 8), :], s, r, dev)
            send(istr.at[:, c, pl.ds(src, 8), cols(j)], S.at[:, c, j, pl.ds(dst, 8), :], s, r, dev)
            send(wind.at[:, c, pl.ds(src, 8), cols(j)], W.at[:, c, j, pl.ds(dst, 8), :], s, r, dev)
            send(thick.at[c, pl.ds(src, 8), cols(j)], TH.at[c, j, pl.ds(dst, 8), :], s, r, dev)

    def halo_turn(turn):
        for dev, cond, src, dst, s, r in (
            (up, has_u, 0, IR + 16, S_U, R_ID),
            (down, has_d, IR - 8, 8, S_D, R_IU),
        ):
            @pl.when(cond)
            def _(dev=dev, src=src, dst=dst, s=s, r=r):
                there = dev[0] // 2
                c = there if turn == 0 else 1 - there
                halo_ice(dev, c, src, dst, s, r + c)

    for own, c in ((0, 0), (G - 1, 1)):
        @pl.when(g == own)
        def _(own=own, c=c):
            for e, dx, cond, s, r in ((0, -1, has_l, S_FL, R_PR), (1, 1, has_r, S_FR, R_PL)):
                @pl.when(cond)
                def _(e=e, dx=dx, s=s, r=r):
                    for dg in range(G):
                        d = dg if own == 0 else G - 1 - dg
                        dev = (g + dg if own == 0 else g - dg, t + dx)
                        send(PF.at[e, d], LF.at[1 - e, c], s, r + c, dev)
            send_flow(c, dests[own][0])
            lo, n, at = flow_rows(own)
            for j in range(LT):
                local(cur.at[:, pl.ds(lo, n), cols(j)], FL.at[:, c, j, pl.ds(at, n), :], L_FL)
    halo_turn(0)

    phase("mergeice")
    @pl.when(has_l)
    def _():
        wait_rows(rs.at[R_IL], 2 * 8 * 8)

    @pl.when(has_r)
    def _():
        wait_rows(rs.at[R_IR], 2 * 8 * 8)

    quarter = lane // 32
    for c in range(2):
        ends = [[zero, zero], [zero, zero]]
        for k in range(8):
            for i in range(IR // 8):
                x = take(LI[1, c, k], LI[0, c, k], i)
                ice_set(k, c, LT, 16 + 8 * i, x)
                for e, at in ((0, 0), (1, IR // 8 - 1)):
                    if i == at:
                        moved = pltpu.roll(x, (32 * (k % 4) + 16) % 128, 1)
                        ends[e][k // 4] = jnp.where(quarter == k % 4, moved, ends[e][k // 4])
        for e in range(2):
            for v in range(2):
                PH[e, c, v] = ends[e][v]
    for e, dev, cond, s, r in ((0, up, has_u, S_U, R_ID), (1, down, has_d, S_D, R_IU)):
        @pl.when(cond)
        def _(e=e, dev=dev, s=s, r=r):
            for c in range(2):
                send(PH.at[e, c], LH.at[1 - e, c], s, r + c, dev)

    for own, c in ((0, 0), (G - 1, 1)):
        @pl.when(g == own)
        def _(own=own, c=c):
            for d in dests[own][1:]:
                send_flow(c, d)
    halo_turn(1)
    for dev, cond, at, to, s, r in (
        (up, has_u, 0, OR + 16, S_U, R_OD),
        (down, has_d, OR - 8, 8, S_D, R_OU),
    ):
        @pl.when(cond)
        def _(dev=dev, at=at, to=to, s=s, r=r):
            for j in range(LT):
                send(base.at[pl.ds(at, 8), cols(j)], B.at[j, pl.ds(to, 8), :], s, r, dev)
                send(depth.at[pl.ds(at, 8), cols(j)], D.at[j, pl.ds(to, 8), :], s, r, dev)
                send(ssh.at[pl.ds(at, 8), cols(j)], X.at[j, pl.ds(to, 8), :], s, r, dev)

    phase("mergeoc")
    @pl.when(has_l)
    def _():
        wait_rows(rs.at[R_OL], 3 * 4 * 8)

    @pl.when(has_r)
    def _():
        wait_rows(rs.at[R_OR], 3 * 4 * 8)

    ends = [zero, zero]
    for k, ref in enumerate((B, D, X)):
        for q in range(OR // 8):
            x = take(LC[1, k, q // 8], LC[0, k, q // 8], q % 8)
            ref[LT, pl.ds(16 + 8 * q, 8), :] = x
            for e, at in ((0, 0), (1, OR // 8 - 1)):
                if q == at:
                    moved = pltpu.roll(x, 32 * k + 16, 1)
                    ends[e] = jnp.where(quarter == k, moved, ends[e])
    for e, dev, cond, s, r in ((0, up, has_u, S_U, R_OD), (1, down, has_d, S_D, R_OU)):
        PHO[e] = ends[e]
        @pl.when(cond)
        def _(e=e, dev=dev, s=s, r=r):
            send(PHO.at[e], LHO.at[1 - e], s, r, dev)

    phase("masks")
    pltpu.make_async_copy(iblk, BI.at[1, 1], ls.at[L_BLK]).wait()
    pltpu.make_async_copy(land, BO.at[1, 1], ls.at[L_BLK]).wait()
    for dy, dx, cond in nbrs:
        k = 3 * (1 + dy) + (1 + dx)
        @pl.when(cond)
        def _(dy=dy, dx=dx, k=k):
            dev = (g + dy, t + dx)
            pltpu.make_async_remote_copy(
                src_ref=iblk, dst_ref=BI.at[1 + dy, 1 + dx], send_sem=ss.at[S_BI + k],
                recv_sem=rs.at[R_BI + k], device_id=dev, device_id_type=MESH).wait_recv()
            rows = pl.ds(0, OR // BS) if dy == 0 else pl.ds(OR // BS - 8 if dy < 0 else 0, 8)
            pltpu.make_async_remote_copy(
                src_ref=land.at[rows], dst_ref=BO.at[1 + dy, 1 + dx, rows], send_sem=ss.at[S_BO + k],
                recv_sem=rs.at[R_BO + k], device_id=dev, device_id_type=MESH).wait_recv()

    def selection(width, first, start):
        block = lax.broadcasted_iota(jnp.int32, (64, width), 0)
        at = lax.broadcasted_iota(jnp.int32, (64, width), 1)
        hit = block == at // BS + first
        if start is not None:
            hit = jnp.logical_and(hit, (at < 64) if start == 0 else (at >= 64))
        return hit.astype(F32)

    sel_c = selection(128 * LT, 0, None)
    sel_r = selection(128, 0, 0)
    sel_l = selection(128, 48, 1)

    def spread_rows(refs):
        lft, mid, rgt = (ref.astype(F32) for ref in refs)
        wide = jnp.dot(mid, sel_c, preferred_element_type=F32)
        last = jnp.dot(rgt, sel_r, preferred_element_type=F32) + jnp.dot(
            lft, sel_l, preferred_element_type=F32)
        return wide, last

    def paint(ref, row, parts, b):
        wide, last = parts
        for j in range(LT):
            ref[j, pl.ds(row, 8), :] = jnp.broadcast_to(wide[b:b + 1, 128 * j:128 * j + 128], (8, 128))
        ref[LT, pl.ds(row, 8), :] = jnp.broadcast_to(last[b:b + 1, :], (8, 128))

    for c in range(2):
        cov = CV.at[c]
        paint(cov, 8, spread_rows([BI[0, x, c] for x in range(3)]), 7)
        mid = spread_rows([BI[1, x, c] for x in range(3)])
        for b in range(8):
            paint(cov, 16 + 8 * b, mid, b)
        paint(cov, IR + 16, spread_rows([BI[2, x, c] for x in range(3)]), 0)
    paint(WET, 8, spread_rows([BO[0, x, 24:32] for x in range(3)]), 7)
    for q in range(4):
        mid = spread_rows([BO[1, x, 8 * q:8 * q + 8] for x in range(3)])
        for b in range(8):
            paint(WET, 16 + 64 * q + 8 * b, mid, b)
    paint(WET, OR + 16, spread_rows([BO[2, x, 0:8] for x in range(3)]), 0)

    phase("")
    def cap(c):
        phase = Phases()
        phase("capwait")

        for e, cond, r, row in ((0, has_u, R_IU, 8), (1, has_d, R_ID, IR + 16)):
            @pl.when(cond)
            def _(e=e, r=r, row=row):
                wait_rows(rs.at[r + c], 8 * 8 * LT + 16)
                for k in range(8):
                    x = pltpu.roll(LH[e, c, k // 4], (128 - 32 * (k % 4) - 16) % 128, 1)
                    ice_set(k, c, LT, row, x)

        @pl.when(has_l)
        def _():
            wait_rows(rs.at[R_PL + c], 24)

        @pl.when(has_r)
        def _():
            wait_rows(rs.at[R_PR + c], 24)

        for k in range(2):
            for s in range(10):
                m = 10 * k + s
                FL[k, c, LT, pl.ds(8 + 8 * s, 8), :] = take(LF[1, c, m // 8], LF[0, c, m // 8], m % 8)

        mine = jnp.logical_and(is_owner, c == owner_cap)
        at_end = jnp.logical_or(jnp.logical_and(c == 0, g == G - 1), jnp.logical_and(c == 1, g == 0))

        @pl.when(mine)
        def _():
            wait_rows(ls.at[L_FL], 2 * (IR + 8) * LT)

        @pl.when(jnp.logical_not(mine))
        def _():
            @pl.when(at_end)
            def _():
                wait_rows(rs.at[R_F + c], 2 * (IR + 8) * LT)

            @pl.when(jnp.logical_not(at_end))
            def _():
                wait_rows(rs.at[R_F + c], 2 * (IR + 16) * LT)

        phase("prepare")
        def prepare(i, carry):
            r = pl.ds(pl.multiple_of(8 * i + 8, 8), 8)
            for j in range(NT):
                cov = CV[c, j, r, :]
                thc = TH[c, j, r, :] * cov
                scale = cov / (thc + (1.0 + STEP * DRAG))
                C1[c, j, r, :] = scale * (thc + 1.0)
                C2[c, j, r, :] = scale * STEP
                TH[c, j, r, :] = thc * (RELAX * STRENGTH / (1.0 + RELAX))
                for k in range(2):
                    W[k, c, j, r, :] = W[k, c, j, r, :] + FL[k, c, j, r, :] * DRAG
            return carry
        lax.fori_loop(0, IR // 8 + 2, prepare, 0)

        phase("subcycles")
        keep = 1.0 / (1.0 + RELAX)

        def group(r):
            rr = pl.ds(r, 8)
            u = [V[0, c, j, rr, :] for j in range(NT)]
            v = [V[1, c, j, rr, :] for j in range(NT)]
            ue, ve = east(u, lane), east(v, lane)
            s0, s1, s2 = [], [], []
            for j in range(NT):
                dux = V[0, c, j, pl.ds(r + 1, 8), :] - u[j]
                dvx = V[1, c, j, pl.ds(r + 1, 8), :] - v[j]
                duy, dvy = ue[j] - u[j], ve[j] - v[j]
                ed, et, es = dux + dvy, dux - dvy, duy + dvx
                inv = lax.rsqrt(ed * ed + et * et + es * es + 1.0)
                a = TH[c, j, rr, :]
                ai = a * inv
                s0.append(S[0, c, j, rr, :] * keep + (ed * ai - a))
                s1.append(S[1, c, j, rr, :] * keep + et * ai)
                s2.append(S[2, c, j, rr, :] * keep + es * ai)
                S[0, c, j, rr, :] = s0[j]
                S[1, c, j, rr, :] = s1[j]
                S[2, c, j, rr, :] = s2[j]
            dif = [s0[j] - s1[j] for j in range(NT)]
            dw, sw = west(dif, lane), west(s2, lane)
            above = pl.ds(r - 1, 8)
            for j in range(NT):
                tot_up = S[0, c, j, above, :] + S[1, c, j, above, :]
                f0 = 0.5 * ((s0[j] + s1[j]) - tot_up) + (s2[j] - sw[j])
                f1 = 0.5 * (dif[j] - dw[j]) + (s2[j] - S[2, c, j, above, :])
                c1, c2 = C1[c, j, rr, :], C2[c, j, rr, :]
                V[0, c, j, rr, :] = c1 * u[j] + c2 * (f0 + W[0, c, j, rr, :])
                V[1, c, j, rr, :] = c1 * v[j] + c2 * (f1 + W[1, c, j, rr, :])

        def subcycle(n, carry):
            for i in range(IR // 8 + 2):
                group(8 + 8 * i)
            return carry
        lax.fori_loop(0, NSUB, subcycle, 0)

        phase("diverge")
        for j in range(LT):
            local(V.at[:, c, j, pl.ds(16, IR), :], o_vel.at[:, c, :, cols(j)], L_OUT)
            local(S.at[:, c, j, pl.ds(16, IR), :], o_str.at[:, c, :, cols(j)], L_OUT)

        prev = [zero] * NT
        pack = zero
        for i in range(IR // 8):
            rr = pl.ds(16 + 8 * i, 8)
            p0, p1 = [], []
            for j in range(NT):
                cov = CV[c, j, rr, :] * DRAG
                p0.append(cov * (V[0, c, j, rr, :] - FL[0, c, j, rr, :]))
                p1.append(cov * (V[1, c, j, rr, :] - FL[1, c, j, rr, :]))
            pw = west(p1, lane)
            for j in range(NT):
                turned = pltpu.roll(p0[j], 1, 0)
                above = jnp.where(sub == 0, prev[j], turned)
                prev[j] = turned
                sp = (p0[j] - above) + (p1[j] - pw[j])
                if j < LT:
                    SPB[c, j, pl.ds(8 * i, 8), :] = sp
                else:
                    pack = jnp.where(lane // 16 == i, pltpu.roll(sp, 16 * i + 8, 1), pack)
        XB[c, 0] = pack
        extra = zero
        for j in range(NT):
            extra = jnp.where(sub == j, -jnp.broadcast_to(prev[j][0:1, :], (8, 128)), extra)
        XB[c, 1] = extra

        @pl.when(mine)
        def _():
            for j in range(LT):
                for i in range(IR // 8):
                    RSP[g, j, pl.ds(8 * i, 8), :] = SPB[c, j, pl.ds(8 * i, 8), :]
            RX[g, 0] = XB[c, 0]
            RX[g, 1] = XB[c, 1]

        @pl.when(jnp.logical_not(mine))
        def _():
            dev = (c * (G - 1), t)
            send(SPB.at[c], RSP.at[g], S_RS + c, R_RS + g, dev)
            send(XB.at[c], RX.at[g], S_RS + c, R_RS + g, dev)

        @pl.when(at_end)
        def _():
            at = jnp.where(c == 0, IR - 8, 0)
            dev = (1 + c, t)
            send(SPB.at[c, :, pl.ds(pl.multiple_of(at, 8), 8), :], RH, S_RH, R_RH, dev)
            send(XB.at[c], RXH, S_RH, R_RH, dev)
        phase(None)

    def caps(turn, carry):
        cap(jnp.where(turn == 0, first_cap, 1 - first_cap))
        return carry

    def ocean_rows(body, carry, unroll=2):
        def step(i, cc):
            for m in range(unroll):
                cc = body(pl.multiple_of(8 * (unroll * i + m) + 16, 8), cc)
            return cc
        return lax.fori_loop(0, OR // 8 // unroll, step, carry)

    def shifted_sum(ref, r):
        rr = pl.ds(r, 8)
        mid = [ref[j, rr, :] for j in range(NT)]
        e, w = east(mid, lane), west(mid, lane)
        return mid, [
            (ref[j, pl.ds(r + 1, 8), :] + ref[j, pl.ds(r - 1, 8), :]) + (e[j] + w[j])
            for j in range(NT)
        ]

    def ocean_prepare():
        phase = Phases()
        phase("oceanwait")

        for e, cond, r, row in ((0, has_u, R_OU, 8), (1, has_d, R_OD, OR + 16)):
            @pl.when(cond)
            def _(e=e, r=r, row=row):
                wait_rows(rs.at[r], 24 * LT + 8)
                for k, ref in enumerate((B, D, X)):
                    ref[LT, pl.ds(row, 8), :] = pltpu.roll(LHO[e], 128 - 32 * k - 16, 1)

        phase("oceanprep")
        def first(r, carry):
            rr = pl.ds(r, 8)
            for j in range(NT):
                gg = D[j, rr, :] * WET[j, rr, :]
                D[j, rr, :] = gg
                Y0[j, rr, :] = gg * X[j, rr, :]
            return carry

        def second(r, carry):
            rr = pl.ds(r, 8)
            gs, gn = shifted_sum(D, r)
            _, xn = shifted_sum(Y0, r)
            for j in range(NT):
                diag = gs[j] * gn[j] + DAMP
                inv = 1.0 / diag
                wid = WET[j, rr, :] * inv
                h = gs[j] * inv
                DG[j, rr, :] = diag
                WID[j, rr, :] = wid
                H[j, rr, :] = h
                Z[j, rr, :] = wid * B[j, rr, :] + h * xn[j] - X[j, rr, :]
            return carry
        for body in (first, second):
            body(8, 0)
            ocean_rows(body, 0)
            body(OR + 16, 0)
        phase(None)

    lax.fori_loop(0, 2, caps, 0)
    ocean_prepare()

    phase("arrive")
    @pl.when(is_owner)
    def _():
        for d in range(G):
            @pl.when(g != d)
            def _(d=d):
                wait_rows(rs.at[R_RS + d], LT * IR + 16)
        for d in range(G):
            for i in range(IR // 8):
                rr = pl.ds(16 + IR * d + 8 * i, 8)
                for j in range(NT):
                    if j < LT:
                        sp = RSP[d, j, pl.ds(8 * i, 8), :]
                    else:
                        sp = pltpu.roll(RX[d, 0], 128 - (16 * i + 8), 1)
                    if i == 0 and d > 0:
                        more = jnp.broadcast_to(RX[d - 1, 1][j:j + 1, :], (8, 128))
                        sp = sp + jnp.where(sub == 0, more, 0.0)
                    Z[j, rr, :] = Z[j, rr, :] + WID[j, rr, :] * sp

    @pl.when(g == 0)
    def _():
        rr = pl.ds(OR + 16, 8)
        for j in range(NT):
            more = jnp.broadcast_to(RX[G - 1, 1][j:j + 1, :], (8, 128))
            Z[j, rr, :] = Z[j, rr, :] + WID[j, rr, :] * jnp.where(sub == 0, more, 0.0)

    @pl.when(jnp.logical_not(is_owner))
    def _():
        wait_rows(rs.at[R_RH], LT * 8 + 16)

        @pl.when(g == 1)
        def _():
            rr = pl.ds(16, 8)
            for j in range(NT):
                more = jnp.broadcast_to(RXH[1][j:j + 1, :], (8, 128))
                Z[j, rr, :] = Z[j, rr, :] + WID[j, rr, :] * jnp.where(sub == 0, more, 0.0)
        for at, row, i in ((1, 8, 7), (2, OR + 16, 0)):
            @pl.when(g == at)
            def _(row=row, i=i):
                rr = pl.ds(row, 8)
                for j in range(NT):
                    sp = RH[j] if j < LT else pltpu.roll(RXH[0], 128 - (16 * i + 8), 1)
                    Z[j, rr, :] = Z[j, rr, :] + WID[j, rr, :] * sp

    phase("krylov")
    def krylov0(r, acc):
        rr = pl.ds(r, 8)
        for j in range(NT):
            z = Z[j, rr, :]
            Y0[j, rr, :] = D[j, rr, :] * z
            if j < LT and acc is not None:
                acc = acc + DG[j, rr, :] * z * z
        return acc

    def krylov(src, dst, vec, r, acc):
        rr = pl.ds(r, 8)
        y, n = shifted_sum(src, r)
        if acc is not None:
            odd, even = acc
        for j in range(NT):
            v = H[j, rr, :] * n[j]
            out = D[j, rr, :] * v
            vec[j, rr, :] = v
            dst[j, rr, :] = out
            if j < LT and acc is not None:
                odd = odd + y[j] * n[j]
                even = even + out * n[j]
        return None if acc is None else (odd, even)

    def last(r, acc):
        y, n = shifted_sum(Y2, r)
        for j in range(LT):
            acc = acc + y[j] * n[j]
        return acc

    krylov0(8, None)
    krylov0(OR + 16, None)
    moments = [ocean_rows(krylov0, zero)]
    for src, dst, vec in ((Y0, Y1, V1), (Y1, Y2, V2)):
        step = functools.partial(krylov, src, dst, vec)
        step(8, None)
        step(OR + 16, None)
        moments += list(ocean_rows(step, (zero, zero)))
    moments.append(ocean_rows(last, zero))

    phase("red1")
    tile = zero
    for k, m in enumerate(moments):
        tile = jnp.where(sub == k, jnp.sum(m, axis=0, keepdims=True), tile)
    slot1 = 2 * g + core
    L1[slot1] = tile
    for dev in peers1:
        send(L1.at[slot1], L1.at[slot1], S_1, R_1, dev)
    wait_rows(rs.at[R_1], 8 * len(peers1))
    tile = L1[0]
    for k in range(1, 8):
        tile = tile + L1[k]
    phase("red2")
    L2[mine2] = tile
    for dev in peers2:
        send(L2.at[mine2], L2.at[mine2], S_2, R_2, dev)
    wait_rows(rs.at[R_2], 8 * len(peers2))
    tile = L2[0]
    for k in range(1, M2):
        tile = tile + L2[k]
    phase("coef")
    total = jnp.sum(tile, axis=1, keepdims=True)
    mu = [total[k:k + 1, :] for k in range(6)]
    nu = [mu[k] - mu[k + 1] for k in range(5)]

    a0 = mu[0] / nu[0]
    z10, z11 = 1.0 - a0, a0
    rz1 = z11 * (z10 * mu[1] + z11 * mu[2])
    b0 = rz1 / mu[0]
    p10, p11 = z10 + b0, z11
    a1 = rz1 / (p11 * (p10 * nu[1] + p11 * nu[2]))
    z20, z21, z22 = z10 - a1 * p10, z11 - a1 * (p11 - p10), a1 * p11
    rz2 = z22 * (z20 * mu[2] + z21 * mu[3] + z22 * mu[4])
    b1 = rz2 / rz1
    p20, p21, p22 = z20 + b1 * p10, z21 + b1 * p11, z22
    a2 = rz2 / (p22 * (p20 * nu[2] + p21 * nu[3] + p22 * nu[4]))
    k0 = jnp.broadcast_to(a0 + a1 * p10 + a2 * p20, (8, 128))
    k1 = jnp.broadcast_to(a1 * p11 + a2 * p21, (8, 128))
    k2 = jnp.broadcast_to(a2 * p22, (8, 128))

    phase("finish")
    def finish(r, carry):
        rr = pl.ds(r, 8)
        for j in range(LT):
            OUT[j, pl.ds(pl.multiple_of(r - 16, 8), 8), :] = X[j, rr, :] + (
                k0 * Z[j, rr, :] + (k1 * V1[j, rr, :] + k2 * V2[j, rr, :]))
        return carry
    ocean_rows(finish, 0)
    for j in range(LT):
        local(OUT.at[j], o_ssh.at[:, cols(j)], L_OUTS)
    phase("outwait")
    wait_rows(ls.at[L_OUTS], OR * LT)
    wait_rows(ls.at[L_OUT], 5 * 2 * IR * LT)

    phase("sentwait")
    for s, cond in ((S_FL, jnp.logical_and(is_owner, has_l)), (S_FR, jnp.logical_and(is_owner, has_r))):
        @pl.when(cond)
        def _(s=s):
            wait_rows(ss.at[s], G * 24)
    for s, cond in ((S_L, has_l), (S_R, has_r)):
        @pl.when(cond)
        def _(s=s):
            wait_rows(ss.at[s], 2 * 8 * 8 + 3 * 4 * 8)
    for s, cond in ((S_U, has_u), (S_D, has_d)):
        @pl.when(cond)
        def _(s=s):
            wait_rows(ss.at[s], (8 * 2 + 3) * 8 * LT + 2 * 16 + 8)

    @pl.when(is_owner)
    def _():
        wait_rows(ss.at[S_F], 2 * LT * (2 * (IR + 16) + IR + 8))
    for c in range(2):
        mine = jnp.logical_and(is_owner, c == owner_cap)

        @pl.when(jnp.logical_not(mine))
        def _(c=c):
            wait_rows(ss.at[S_RS + c], LT * IR + 16)

    @pl.when(is_owner)
    def _():
        wait_rows(ss.at[S_RH], LT * 8 + 16)
    wait_rows(ss.at[S_1], 8 * len(peers1))
    wait_rows(ss.at[S_2], 8 * len(peers2))
    for dy, dx, cond in nbrs:
        k = 3 * (1 - dy) + (1 - dx)
        @pl.when(cond)
        def _(dy=dy, dx=dx, k=k):
            dev = (g + dy, t + dx)
            pltpu.make_async_remote_copy(
                src_ref=iblk, dst_ref=BI.at[1 - dy, 1 - dx], send_sem=ss.at[S_BI + k],
                recv_sem=rs.at[R_BI + k], device_id=dev, device_id_type=MESH).wait_send()
            rows = pl.ds(0, OR // BS) if dy == 0 else pl.ds(0 if dy < 0 else OR // BS - 8, 8)
            pltpu.make_async_remote_copy(
                src_ref=land.at[rows], dst_ref=BO.at[1 - dy, 1 - dx, rows], send_sem=ss.at[S_BO + k],
                recv_sem=rs.at[R_BO + k], device_id=dev, device_id_type=MESH).wait_send()
    phase(None)


def shards(T, *args):
    ice = (2, NT, IH, 128)
    ocean = (NT, OH, 128)
    vm = lambda *s: pltpu.VMEM(s, F32)
    scratch = [
        vm(2, *ice), vm(3, *ice), vm(2, *ice), vm(*ice), vm(2, *ice), vm(*ice), vm(*ice), vm(*ice),
        vm(2, 2, 8, 8, 128), vm(2, 2, 8, 8, 128), vm(2, 3, 4, 8, 128), vm(2, 3, 4, 8, 128),
        vm(2, G, 3, 8, 128), vm(2, 2, 3, 8, 128), vm(2, 2, 2, 8, 128), vm(2, 2, 2, 8, 128),
        vm(2, 8, 128), vm(2, 8, 128), vm(2, 2, OR, 128),
        *[vm(*ocean) for _ in range(13)],
        pltpu.VMEM((3, 3, 2, 8, 64), jnp.int32), pltpu.VMEM((3, 3, 32, 64), jnp.int32),
        vm(2, LT, IR, 128), vm(2, 2, 8, 128),
        vm(G, LT, IR, 128), vm(G, 2, 8, 128), vm(LT, 8, 128), vm(2, 8, 128),
        vm(8, 8, 128), vm(T // 2, 8, 128), vm(LT, OR, 128), vm(DUMMY, 128),
        pltpu.SemaphoreType.DMA((N_R,)), pltpu.SemaphoreType.DMA((N_S,)), pltpu.SemaphoreType.DMA((N_L,)),
    ]
    hbm = pl.BlockSpec(memory_space=pltpu.HBM)
    return pl.pallas_call(
        functools.partial(kernel, T),
        out_shape=(
            jax.ShapeDtypeStruct((OR, 128 * LT), F32),
            jax.ShapeDtypeStruct((2, 2, IR, 128 * LT), F32),
            jax.ShapeDtypeStruct((3, 2, IR, 128 * LT), F32),
        ),
        in_specs=[hbm] * 10,
        out_specs=(hbm, hbm, hbm),
        scratch_shapes=scratch,
        compiler_params=pltpu.CompilerParams(
            collective_id=0, has_side_effects=True, vmem_limit_bytes=60 * 1024 * 1024),
    )(*args)


def solution(mesh):
    return jax.shard_map(
        functools.partial(shards, mesh.shape["tile"]),
        mesh=mesh,
        in_specs=(
            P("grp", "tile"),
            P("grp", "tile"),
            P("grp", "tile"),
            P(None, "grp", "tile"),
            P("grp", "tile"),
            P(None, "grp", "tile"),
            P(None, "grp", "tile"),
            P(None, None, "grp", "tile"),
            P(None, None, "grp", "tile"),
            P(None, None, "grp", "tile"),
        ),
        out_specs=(P("grp", "tile"), P(None, None, "grp", "tile"), P(None, None, "grp", "tile")),
        check_vma=False,
    )
```

```python
import functools

import jax
import jax.numpy as jnp
from jax import lax
from jax.experimental import pallas as pl
from jax.experimental.pallas import tpu as pltpu
from jax.sharding import PartitionSpec as P

BS = 8
NSUB = 8
DAMP = 0.05
RELAX = 0.2
STRENGTH = 0.5
DRAG = 1.0
STEP = 0.5
G = 4
LT = 4
NT = LT + 1
IR = 64
OR = 256
IH = IR + 40
OH = OR + 40
F32 = jnp.float32
MESH = pl.DeviceIdType.MESH
DUMMY = 4096

R_PL, R_PR, R_FU, R_FD, R_IL, R_IR, R_OL, R_OR = 41, 43, 45, 47, 4, 5, 6, 7
R_IU, R_ID, R_F = 8, 10, 12
R_OU, R_OD, R_RS, R_RH, R_1, R_2 = 14, 15, 16, 20, 21, 22
R_BI, R_BO = 23, 32
N_R = 49
S_FL, S_FR, S_L, S_R, S_U, S_D, S_F, S_RS, S_1, S_2 = 0, 1, 2, 3, 4, 5, 6, 7, 9, 10
S_RH, S_FW = 11, 30
S_BI, S_BO = 12, 21
N_S = 31
L_BLK, L_ICE, L_FL, L_OC, L_OUT, L_OUTS, L_ED = 0, 1, 2, 3, 4, 5, 6
N_L = 7


def east(tiles, lane):
    turned = [pltpu.roll(x, 127, 1) for x in tiles]
    return [jnp.where(lane == 127, turned[(j + 1) % NT], turned[j]) for j in range(NT)]


def west(tiles, lane):
    turned = [pltpu.roll(x, 1, 1) for x in tiles]
    return [jnp.where(lane == 0, turned[(j - 1) % NT], turned[j]) for j in range(NT)]


class Phases:
    def __init__(self):
        self.open = None

    def __call__(self, name):
        if self.open is not None:
            self.open.__exit__(None, None, None)
        self.open = None
        if name:
            self.open = jax.named_scope(name)
            self.open.__enter__()


def kernel(
    T,
    base, depth, ssh, cur, land, thick, iblk, ivel, istr, wind,
    V, S, OUT,
    W, TH, FL, CV, C1, C2,
    PI, LI, PC, LC, PF, LF, PH, LH, PHO, LHO, CE, FE,
    B, D, X, Z, Y0, Y1, Y2, H, WID, DG, WET, V1, V2,
    BI, BO, SPB, XB, RSP, RX, RH, RXH, L1, L2, MOM, DUM,
    rs, ss, ls,
):
    g = lax.axis_index("grp")
    t = lax.axis_index("tile")
    has_l, has_r, has_u, has_d = t > 0, t < T - 1, g > 0, g < G - 1
    lane = lax.broadcasted_iota(jnp.int32, (8, 128), 1)
    sub = lax.broadcasted_iota(jnp.int32, (8, 128), 0)
    zero = jnp.zeros((8, 128), F32)
    first_cap = g // 2
    owner_cap = jnp.where(g == 0, 0, 1)
    is_owner = jnp.logical_or(g == 0, g == G - 1)

    def wait_rows(sem, rows):
        pltpu.make_async_copy(DUM.at[pl.ds(0, rows)], DUM.at[pl.ds(0, rows)], sem).wait()

    def send(src, dst, s, r, dev):
        pltpu.make_async_remote_copy(
            src_ref=src, dst_ref=dst, send_sem=ss.at[s], recv_sem=rs.at[r],
            device_id=dev, device_id_type=MESH,
        ).start()

    def local(src, dst, s):
        pltpu.make_async_copy(src, dst, ls.at[s]).start()

    def cols(j):
        return pl.ds(128 * j, 128)

    nbrs = []
    for dy in (-1, 0, 1):
        for dx in (-1, 0, 1):
            if dy == 0 and dx == 0:
                continue
            cond = None
            for need, there in ((dy < 0, has_u), (dy > 0, has_d), (dx < 0, has_l), (dx > 0, has_r)):
                if need:
                    cond = there if cond is None else jnp.logical_and(cond, there)
            nbrs.append((dy, dx, cond))

    def top_summed(c, d):
        return (c == 0 and d in (1, 2)) or (c == 1 and d == 1)

    def bottom_summed(c, d):
        return (c == 1 and d in (1, 2)) or (c == 0 and d == 2)

    def top_is_summed(c):
        return jnp.logical_or(g == 1, jnp.logical_and(g == 2, c == 0))

    def bottom_is_summed(c):
        return jnp.logical_or(g == 2, jnp.logical_and(g == 1, c == 1))

    phase = Phases()
    phase("signal")
    barrier = pltpu.get_barrier_semaphore()
    core = lax.rem(t, 2)
    M2 = T // 2
    mine2 = t // 2
    peers1 = []
    for dg in range(G):
        for dc in range(2):
            if dg or dc:
                peers1.append((lax.rem(g + dg, G), t - core + lax.rem(core + dc, 2)))
    peers2 = [(g, 2 * lax.rem(mine2 + k, M2) + core) for k in range(1, M2)]
    for dg in range(G):
        for dx, cond in ((-1, has_l), (0, None), (1, has_r)):
            dev = (lax.rem(g + dg, G), t + dx)
            if cond is not None:
                @pl.when(cond)
                def _(dev=dev):
                    pl.semaphore_signal(barrier, inc=1, device_id=dev, device_id_type=MESH)
            elif dg:
                pl.semaphore_signal(barrier, inc=1, device_id=dev, device_id_type=MESH)
    for dev in peers2:
        pl.semaphore_signal(barrier, inc=1, device_id=dev, device_id_type=MESH)

    phase("loads")
    local(iblk, BI.at[1, 1], L_BLK)
    local(land, BO.at[1, 1], L_BLK)
    for j in range(LT):
        local(ivel.at[:, :, :, cols(j)], V.at[:, :, j, pl.ds(16, IR), :], L_ICE)
        local(istr.at[:, :, :, cols(j)], S.at[:, :, j, pl.ds(16, IR), :], L_ICE)
        local(wind.at[:, :, :, cols(j)], W.at[:, :, j, pl.ds(16, IR), :], L_ICE)
        local(thick.at[:, :, cols(j)], TH.at[:, j, pl.ds(16, IR), :], L_ICE)
        local(base.at[:, cols(j)], B.at[j, pl.ds(16, OR), :], L_OC)
        local(depth.at[:, cols(j)], D.at[j, pl.ds(16, OR), :], L_OC)
        local(ssh.at[:, cols(j)], X.at[j, pl.ds(16, OR), :], L_OC)

    @pl.when(is_owner)
    def _():
        local(cur.at[:, :, cols(0)], CE.at[0], L_ED)
        local(cur.at[:, :, cols(LT - 1)], CE.at[1], L_ED)

    phase("barrier")
    wide = 1 + jnp.minimum(t, 1) + jnp.minimum(T - 1 - t, 1)
    pl.semaphore_wait(barrier, G * wide - 1 + len(peers2))

    phase("sends")
    left, right, up, down = (g, t - 1), (g, t + 1), (g - 1, t), (g + 1, t)
    for dy, dx, cond in nbrs:
        k = 3 * (1 - dy) + (1 - dx)
        @pl.when(cond)
        def _(dy=dy, dx=dx, k=k):
            dev = (g + dy, t + dx)
            send(iblk, BI.at[1 - dy, 1 - dx], S_BI + k, R_BI + k, dev)
            rows = pl.ds(0, OR // BS) if dy == 0 else pl.ds(0 if dy < 0 else OR // BS - 8, 8)
            send(land.at[rows], BO.at[1 - dy, 1 - dx, rows], S_BO + k, R_BO + k, dev)

    def flow_rows(c, d):
        lo = IR * d if d == 0 or top_summed(c, d) else IR * d - 8
        hi = IR * d + IR if d == G - 1 or bottom_summed(c, d) else IR * d + IR + 8
        return lo, hi - lo, 16 + lo - IR * d

    dests = {0: (1, 3, 2), G - 1: (2, 0, 1)}

    def send_flow(c, d):
        lo, n, at = flow_rows(c, d)
        for j in range(LT):
            send(cur.at[:, pl.ds(lo, n), cols(j)], FL.at[:, c, j, pl.ds(at, n), :],
                 S_F, R_F + c, (d, t))

    def halo_ice(dev, c, src, dst, s, r):
        there = dev[0]
        if s == S_D:
            summed = jnp.logical_or(there == 1, jnp.logical_and(there == 2, c == 0))
        else:
            summed = jnp.logical_or(there == 2, jnp.logical_and(there == 1, c == 1))

        @pl.when(jnp.logical_not(summed))
        def _():
            for j in range(LT):
                send(wind.at[:, c, pl.ds(src, 8), cols(j)], W.at[:, c, j, pl.ds(dst, 8), :], s, r, dev)
        for j in range(LT):
            send(ivel.at[:, c, pl.ds(src, 8), cols(j)], V.at[:, c, j, pl.ds(dst, 8), :], s, r, dev)
            send(istr.at[:, c, pl.ds(src, 8), cols(j)], S.at[:, c, j, pl.ds(dst, 8), :], s, r, dev)
            send(thick.at[c, pl.ds(src, 8), cols(j)], TH.at[c, j, pl.ds(dst, 8), :], s, r, dev)

    def halo_turn(turn):
        for dev, cond, src, dst, s, r in (
            (up, has_u, 0, IR + 16, S_U, R_ID),
            (down, has_d, IR - 8, 8, S_D, R_IU),
        ):
            @pl.when(cond)
            def _(dev=dev, src=src, dst=dst, s=s, r=r):
                there = dev[0] // 2
                c = there if turn == 0 else 1 - there
                halo_ice(dev, c, src, dst, s, r + c)

    for own, c in ((0, 0), (G - 1, 1)):
        @pl.when(g == own)
        def _(own=own, c=c):
            send_flow(c, dests[own][0])
            send_flow(c, dests[own][1])
            lo, n, at = flow_rows(c, own)
            for j in range(LT):
                local(cur.at[:, pl.ds(lo, n), cols(j)], FL.at[:, c, j, pl.ds(at, n), :], L_FL)
    halo_turn(0)

    phase("zeros")
    for cond, row, orow, by in ((g == 0, 8, 8, 0), (g == G - 1, IR + 16, OR + 16, 2)):
        @pl.when(cond)
        def _(row=row, orow=orow, by=by):
            for c in range(2):
                for j in range(NT):
                    for k in range(3):
                        S[k, c, j, pl.ds(row, 8), :] = zero
                    for k in range(2):
                        V[k, c, j, pl.ds(row, 8), :] = zero
                        W[k, c, j, pl.ds(row, 8), :] = zero
                        FL[k, c, j, pl.ds(row, 8), :] = zero
                    TH[c, j, pl.ds(row, 8), :] = zero
            for j in range(NT):
                B[j, pl.ds(orow, 8), :] = zero
                D[j, pl.ds(orow, 8), :] = zero
                X[j, pl.ds(orow, 8), :] = zero
            for x in range(3):
                for c in range(2):
                    BI[by, x, c] = jnp.zeros((8, 64), jnp.int32)
                BO[by, x] = jnp.zeros((32, 64), jnp.int32)

    for d in (1, 2):
        @pl.when(g == d)
        def _(d=d):
            for c in range(2):
                for here, row in ((top_summed(c, d), 8), (bottom_summed(c, d), IR + 16)):
                    if here:
                        for k in range(2):
                            for j in range(LT):
                                FL[k, c, j, pl.ds(row, 8), :] = zero

    for cond, side, bx in ((t == 0, 0, 0), (t == T - 1, 1, 2)):
        @pl.when(cond)
        def _(side=side, bx=bx):
            for c in range(2):
                for k in range(8):
                    LI[side, c, k] = zero
                for v in range(3):
                    LF[side, c, v] = zero
            for k in range(3):
                for v in range(4):
                    LC[side, k, v] = zero
            for y in range(3):
                for c in range(2):
                    BI[y, bx, c] = jnp.zeros((8, 64), jnp.int32)
                BO[y, bx] = jnp.zeros((32, 64), jnp.int32)

    phase("pack")
    slot_of = lane // 16

    def put(pack, e, at, x):
        moved = pltpu.roll(x, 16 * at, 1) if at else x
        return jnp.where(slot_of == (at - e) % 8, moved, pack)

    def take(from_right, from_left, at):
        both = jnp.where(slot_of == at, from_right, from_left)
        return pltpu.roll(both, 128 - 16 * at, 1) if at else both

    wait_rows(ls.at[L_ICE], 8 * 2 * IR * LT)

    def ice_get(k, c, j, r):
        if k < 2:
            return V[k, c, j, pl.ds(r, 8), :]
        if k < 5:
            return S[k - 2, c, j, pl.ds(r, 8), :]
        return W[k - 5, c, j, pl.ds(r, 8), :] if k < 7 else TH[c, j, pl.ds(r, 8), :]

    def ice_set(k, c, j, r, x):
        if k < 2:
            V[k, c, j, pl.ds(r, 8), :] = x
        elif k < 5:
            S[k - 2, c, j, pl.ds(r, 8), :] = x
        elif k < 7:
            W[k - 5, c, j, pl.ds(r, 8), :] = x
        else:
            TH[c, j, pl.ds(r, 8), :] = x

    for e, j in ((0, 0), (1, LT - 1)):
        for c in range(2):
            for k in range(8):
                pack = zero
                for i in range(IR // 8):
                    pack = put(pack, e, i, ice_get(k, c, j, 16 + 8 * i))
                PI[e, c, k] = pack

    for own in (0, G - 1):
        @pl.when(g == own)
        def _(own=own):
            wait_rows(ls.at[L_ED], 2 * 2 * OR)
            for e in range(2):
                for d in range(G):
                    packs = [zero] * 3
                    for k in range(2):
                        for s in range(10):
                            q = 8 * d - 1 + s
                            if 0 <= q < OR // 8:
                                m = 10 * k + s
                                packs[m // 8] = put(packs[m // 8], e, m % 8, CE[e, k, pl.ds(8 * q, 8), :])
                    for v in range(3):
                        PF[e, d, v] = packs[v]

    wait_rows(ls.at[L_OC], 3 * OR * LT)
    for e, j in ((0, 0), (1, LT - 1)):
        for k, ref in enumerate((B, D, X)):
            for v in range(4):
                pack = zero
                for i in range(8):
                    pack = put(pack, e, i, ref[j, pl.ds(16 + 64 * v + 8 * i, 8), :])
                PC[e, k, v] = pack

    for e, dev, cond, s, ri, ro in ((0, left, has_l, S_L, R_IR, R_OR), (1, right, has_r, S_R, R_IL, R_OL)):
        @pl.when(cond)
        def _(e=e, dev=dev, s=s, ri=ri, ro=ro):
            send(PI.at[e], LI.at[1 - e], s, ri, dev)
            send(PC.at[e], LC.at[1 - e], s, ro, dev)

    for own, c in ((0, 0), (G - 1, 1)):
        @pl.when(g == own)
        def _(own=own, c=c):
            for e, dx, cond, s, r in ((0, -1, has_l, S_FL, R_PR), (1, 1, has_r, S_FR, R_PL)):
                @pl.when(cond)
                def _(e=e, dx=dx, s=s, r=r):
                    for dg in range(G):
                        d = dg if own == 0 else G - 1 - dg
                        dev = (g + dg if own == 0 else g - dg, t + dx)
                        send(PF.at[e, d], LF.at[1 - e, c], s, r + c, dev)

    phase("mergeice")
    @pl.when(has_l)
    def _():
        wait_rows(rs.at[R_IL], 2 * 8 * 8)

    @pl.when(has_r)
    def _():
        wait_rows(rs.at[R_IR], 2 * 8 * 8)

    quarter = lane // 32
    for c in range(2):
        ends = [[zero, zero], [zero, zero]]
        for k in range(8):
            for i in range(IR // 8):
                x = take(LI[1, c, k], LI[0, c, k], i)
                ice_set(k, c, LT, 16 + 8 * i, x)
                for e, at in ((0, 0), (1, IR // 8 - 1)):
                    if i == at:
                        moved = pltpu.roll(x, (32 * (k % 4) + 16) % 128, 1)
                        ends[e][k // 4] = jnp.where(quarter == k % 4, moved, ends[e][k // 4])
        for e in range(2):
            for v in range(2):
                PH[e, c, v] = ends[e][v]
    for e, dev, cond, s, r in ((0, up, has_u, S_U, R_ID), (1, down, has_d, S_D, R_IU)):
        @pl.when(cond)
        def _(e=e, dev=dev, s=s, r=r):
            for c in range(2):
                send(PH.at[e, c], LH.at[1 - e, c], s, r + c, dev)

    for own, c, row, to, dev, r in (
        (0, 0, IR + 8, 8, down, R_FU), (G - 1, 1, 16, IR + 16, up, R_FD + 1)):
        @pl.when(g == own)
        def _(c=c, row=row, to=to, dev=dev, r=r):
            wait_rows(ls.at[L_FL], 2 * (IR + 8) * LT)
            for k in range(2):
                for j in range(LT):
                    FE[k, j] = W[k, c, j, pl.ds(row, 8), :] + FL[k, c, j, pl.ds(row, 8), :] * DRAG
            for j in range(LT):
                send(FE.at[:, j], W.at[:, c, j, pl.ds(to, 8), :], S_FW, r, dev)

    for own, c in ((0, 0), (G - 1, 1)):
        @pl.when(g == own)
        def _(own=own, c=c):
            send_flow(c, dests[own][2])
    halo_turn(1)
    for dev, cond, at, to, s, r in (
        (up, has_u, 0, OR + 16, S_U, R_OD),
        (down, has_d, OR - 8, 8, S_D, R_OU),
    ):
        @pl.when(cond)
        def _(dev=dev, at=at, to=to, s=s, r=r):
            for j in range(LT):
                send(base.at[pl.ds(at, 8), cols(j)], B.at[j, pl.ds(to, 8), :], s, r, dev)
                send(depth.at[pl.ds(at, 8), cols(j)], D.at[j, pl.ds(to, 8), :], s, r, dev)
                send(ssh.at[pl.ds(at, 8), cols(j)], X.at[j, pl.ds(to, 8), :], s, r, dev)

    phase("mergeoc")
    @pl.when(has_l)
    def _():
        wait_rows(rs.at[R_OL], 3 * 4 * 8)

    @pl.when(has_r)
    def _():
        wait_rows(rs.at[R_OR], 3 * 4 * 8)

    ends = [zero, zero]
    for k, ref in enumerate((B, D, X)):
        for q in range(OR // 8):
            x = take(LC[1, k, q // 8], LC[0, k, q // 8], q % 8)
            ref[LT, pl.ds(16 + 8 * q, 8), :] = x
            for e, at in ((0, 0), (1, OR // 8 - 1)):
                if q == at:
                    moved = pltpu.roll(x, 32 * k + 16, 1)
                    ends[e] = jnp.where(quarter == k, moved, ends[e])
    for e, dev, cond, s, r in ((0, up, has_u, S_U, R_OD), (1, down, has_d, S_D, R_OU)):
        PHO[e] = ends[e]
        @pl.when(cond)
        def _(e=e, dev=dev, s=s, r=r):
            send(PHO.at[e], LHO.at[1 - e], s, r, dev)

    phase("masks")
    pltpu.make_async_copy(iblk, BI.at[1, 1], ls.at[L_BLK]).wait()
    pltpu.make_async_copy(land, BO.at[1, 1], ls.at[L_BLK]).wait()
    for dy, dx, cond in nbrs:
        k = 3 * (1 + dy) + (1 + dx)
        @pl.when(cond)
        def _(dy=dy, dx=dx, k=k):
            dev = (g + dy, t + dx)
            pltpu.make_async_remote_copy(
                src_ref=iblk, dst_ref=BI.at[1 + dy, 1 + dx], send_sem=ss.at[S_BI + k],
                recv_sem=rs.at[R_BI + k], device_id=dev, device_id_type=MESH).wait_recv()
            rows = pl.ds(0, OR // BS) if dy == 0 else pl.ds(OR // BS - 8 if dy < 0 else 0, 8)
            pltpu.make_async_remote_copy(
                src_ref=land.at[rows], dst_ref=BO.at[1 + dy, 1 + dx, rows], send_sem=ss.at[S_BO + k],
                recv_sem=rs.at[R_BO + k], device_id=dev, device_id_type=MESH).wait_recv()

    def selection(width, first, start):
        block = lax.broadcasted_iota(jnp.int32, (64, width), 0)
        at = lax.broadcasted_iota(jnp.int32, (64, width), 1)
        hit = block == at // BS + first
        if start is not None:
            hit = jnp.logical_and(hit, (at < 64) if start == 0 else (at >= 64))
        return hit.astype(F32)

    sel_c = selection(128 * LT, 0, None)
    sel_r = selection(128, 0, 0)
    sel_l = selection(128, 48, 1)

    def spread_rows(refs):
        lft, mid, rgt = (ref.astype(F32) for ref in refs)
        wide = jnp.dot(mid, sel_c, preferred_element_type=F32)
        last = jnp.dot(rgt, sel_r, preferred_element_type=F32) + jnp.dot(
            lft, sel_l, preferred_element_type=F32)
        return wide, last

    def paint(ref, row, parts, b):
        wide, last = parts
        for j in range(LT):
            ref[j, pl.ds(row, 8), :] = jnp.broadcast_to(wide[b:b + 1, 128 * j:128 * j + 128], (8, 128))
        ref[LT, pl.ds(row, 8), :] = jnp.broadcast_to(last[b:b + 1, :], (8, 128))

    for c in range(2):
        cov = CV.at[c]
        paint(cov, 8, spread_rows([BI[0, x, c] for x in range(3)]), 7)
        mid = spread_rows([BI[1, x, c] for x in range(3)])
        for b in range(8):
            paint(cov, 16 + 8 * b, mid, b)
        paint(cov, IR + 16, spread_rows([BI[2, x, c] for x in range(3)]), 0)
    paint(WET, 8, spread_rows([BO[0, x, 24:32] for x in range(3)]), 7)
    for q in range(4):
        mid = spread_rows([BO[1, x, 8 * q:8 * q + 8] for x in range(3)])
        for b in range(8):
            paint(WET, 16 + 64 * q + 8 * b, mid, b)
    paint(WET, OR + 16, spread_rows([BO[2, x, 0:8] for x in range(3)]), 0)

    phase("")
    def pass_on(c, row, to, dev, r):
        for j in range(LT):
            send(W.at[:, c, j, pl.ds(row, 8), :], W.at[:, c, j, pl.ds(to, 8), :], S_FW, r + c, dev)

    def cap(c):
        phase = Phases()
        phase("capwait")

        for e, cond, r, row, rf, summed in (
            (0, has_u, R_IU, 8, R_FU, top_is_summed(c)),
            (1, has_d, R_ID, IR + 16, R_FD, bottom_is_summed(c)),
        ):
            @pl.when(cond)
            def _(e=e, r=r, row=row, rf=rf, summed=summed):
                @pl.when(summed)
                def _():
                    wait_rows(rs.at[rf + c], 2 * 8 * LT)
                    wait_rows(rs.at[r + c], 6 * 8 * LT + 16)

                @pl.when(jnp.logical_not(summed))
                def _():
                    wait_rows(rs.at[r + c], 8 * 8 * LT + 16)
                for k in range(8):
                    x = pltpu.roll(LH[e, c, k // 4], (128 - 32 * (k % 4) - 16) % 128, 1)
                    ice_set(k, c, LT, row, x)

        @pl.when(has_l)
        def _():
            wait_rows(rs.at[R_PL + c], 24)

        @pl.when(has_r)
        def _():
            wait_rows(rs.at[R_PR + c], 24)

        for k in range(2):
            for s in range(10):
                m = 10 * k + s
                FL[k, c, LT, pl.ds(8 + 8 * s, 8), :] = take(LF[1, c, m // 8], LF[0, c, m // 8], m % 8)

        mine = jnp.logical_and(is_owner, c == owner_cap)
        at_end = jnp.logical_or(jnp.logical_and(c == 0, g == G - 1), jnp.logical_and(c == 1, g == 0))

        @pl.when(jnp.logical_not(mine))
        def _():
            both = jnp.logical_and(top_is_summed(c), bottom_is_summed(c))

            @pl.when(both)
            def _():
                wait_rows(rs.at[R_F + c], 2 * IR * LT)

            @pl.when(jnp.logical_not(both))
            def _():
                wait_rows(rs.at[R_F + c], 2 * (IR + 8) * LT)

        phase("prepare")
        def prepare(i, carry):
            r = pl.ds(pl.multiple_of(8 * i + 8, 8), 8)
            for j in range(NT):
                cov = CV[c, j, r, :]
                thc = TH[c, j, r, :] * cov
                scale = cov / (thc + (1.0 + STEP * DRAG))
                C1[c, j, r, :] = scale * (thc + 1.0)
                C2[c, j, r, :] = scale * STEP
                TH[c, j, r, :] = thc * (RELAX * STRENGTH / (1.0 + RELAX))
                for k in range(2):
                    W[k, c, j, r, :] = W[k, c, j, r, :] + FL[k, c, j, r, :] * DRAG
            return carry
        lax.fori_loop(0, IR // 8 + 2, prepare, 0)

        @pl.when(jnp.logical_and(c == 0, g == 1))
        def _():
            pass_on(0, IR + 8, 8, down, R_FU)

        @pl.when(jnp.logical_and(c == 0, g == G - 1))
        def _():
            pass_on(0, 16, IR + 16, up, R_FD)

        @pl.when(jnp.logical_and(c == 1, g == 0))
        def _():
            pass_on(1, IR + 8, 8, down, R_FU)

        @pl.when(jnp.logical_and(c == 1, g == 2))
        def _():
            pass_on(1, 16, IR + 16, up, R_FD)

        phase("subcycles")
        keep = 1.0 / (1.0 + RELAX)

        def group(r):
            rr = pl.ds(r, 8)
            u = [V[0, c, j, rr, :] for j in range(NT)]
            v = [V[1, c, j, rr, :] for j in range(NT)]
            ue, ve = east(u, lane), east(v, lane)
            s0, s1, s2 = [], [], []
            for j in range(NT):
                dux = V[0, c, j, pl.ds(r + 1, 8), :] - u[j]
                dvx = V[1, c, j, pl.ds(r + 1, 8), :] - v[j]
                duy, dvy = ue[j] - u[j], ve[j] - v[j]
                ed, et, es = dux + dvy, dux - dvy, duy + dvx
                inv = lax.rsqrt(ed * ed + et * et + es * es + 1.0)
                a = TH[c, j, rr, :]
                ai = a * inv
                s0.append(S[0, c, j, rr, :] * keep + (ed * ai - a))
                s1.append(S[1, c, j, rr, :] * keep + et * ai)
                s2.append(S[2, c, j, rr, :] * keep + es * ai)
                S[0, c, j, rr, :] = s0[j]
                S[1, c, j, rr, :] = s1[j]
                S[2, c, j, rr, :] = s2[j]
            dif = [s0[j] - s1[j] for j in range(NT)]
            dw, sw = west(dif, lane), west(s2, lane)
            above = pl.ds(r - 1, 8)
            for j in range(NT):
                tot_up = S[0, c, j, above, :] + S[1, c, j, above, :]
                f0 = 0.5 * ((s0[j] + s1[j]) - tot_up) + (s2[j] - sw[j])
                f1 = 0.5 * (dif[j] - dw[j]) + (s2[j] - S[2, c, j, above, :])
                c1, c2 = C1[c, j, rr, :], C2[c, j, rr, :]
                V[0, c, j, rr, :] = c1 * u[j] + c2 * (f0 + W[0, c, j, rr, :])
                V[1, c, j, rr, :] = c1 * v[j] + c2 * (f1 + W[1, c, j, rr, :])

        def subcycle(n, carry):
            for _ in range(2):
                for i in range(IR // 8 + 2):
                    group(8 + 8 * i)
            return carry
        lax.fori_loop(0, NSUB // 2, subcycle, 0)

        phase("diverge")
        prev = [zero] * NT
        pack = zero
        for i in range(IR // 8):
            rr = pl.ds(16 + 8 * i, 8)
            p0, p1 = [], []
            for j in range(NT):
                cov = CV[c, j, rr, :] * DRAG
                p0.append(cov * (V[0, c, j, rr, :] - FL[0, c, j, rr, :]))
                p1.append(cov * (V[1, c, j, rr, :] - FL[1, c, j, rr, :]))
            pw = west(p1, lane)
            for j in range(NT):
                turned = pltpu.roll(p0[j], 1, 0)
                above = jnp.where(sub == 0, prev[j], turned)
                prev[j] = turned
                sp = (p0[j] - above) + (p1[j] - pw[j])
                if j < LT:
                    SPB[c, j, pl.ds(8 * i, 8), :] = sp
                else:
                    pack = jnp.where(lane // 16 == i, pltpu.roll(sp, 16 * i + 8, 1), pack)
        XB[c, 0] = pack
        extra = zero
        for j in range(NT):
            extra = jnp.where(sub == j, -jnp.broadcast_to(prev[j][0:1, :], (8, 128)), extra)
        XB[c, 1] = extra

        @pl.when(mine)
        def _():
            for j in range(LT):
                for i in range(IR // 8):
                    RSP[g, j, pl.ds(8 * i, 8), :] = SPB[c, j, pl.ds(8 * i, 8), :]
            RX[g, 0] = XB[c, 0]
            RX[g, 1] = XB[c, 1]

        @pl.when(jnp.logical_not(mine))
        def _():
            dev = (c * (G - 1), t)
            send(SPB.at[c], RSP.at[g], S_RS + c, R_RS + g, dev)
            send(XB.at[c], RX.at[g], S_RS + c, R_RS + g, dev)

        @pl.when(at_end)
        def _():
            at = jnp.where(c == 0, IR - 8, 0)
            dev = (1 + c, t)
            send(SPB.at[c, :, pl.ds(pl.multiple_of(at, 8), 8), :], RH, S_RH, R_RH, dev)
            send(XB.at[c], RXH, S_RH, R_RH, dev)
        phase(None)

    def caps(turn, carry):
        cap(jnp.where(turn == 0, first_cap, 1 - first_cap))
        return carry

    def ocean_rows(body, carry, unroll=4):
        def step(i, cc):
            for m in range(unroll):
                cc = body(pl.multiple_of(8 * (unroll * i + m) + 16, 8), cc)
            return cc
        return lax.fori_loop(0, OR // 8 // unroll, step, carry)

    def shifted_sum(ref, r):
        rr = pl.ds(r, 8)
        mid = [ref[j, rr, :] for j in range(NT)]
        e, w = east(mid, lane), west(mid, lane)
        return mid, [
            (ref[j, pl.ds(r + 1, 8), :] + ref[j, pl.ds(r - 1, 8), :]) + (e[j] + w[j])
            for j in range(NT)
        ]

    def ocean_prepare():
        phase = Phases()
        phase("oceanwait")

        for e, cond, r, row in ((0, has_u, R_OU, 8), (1, has_d, R_OD, OR + 16)):
            @pl.when(cond)
            def _(e=e, r=r, row=row):
                wait_rows(rs.at[r], 24 * LT + 8)
                for k, ref in enumerate((B, D, X)):
                    ref[LT, pl.ds(row, 8), :] = pltpu.roll(LHO[e], 128 - 32 * k - 16, 1)

        phase("oceanprep")
        def first(r, carry):
            rr = pl.ds(r, 8)
            for j in range(NT):
                gg = D[j, rr, :] * WET[j, rr, :]
                D[j, rr, :] = gg
                Y0[j, rr, :] = gg * X[j, rr, :]
            return carry

        def second(r, carry):
            rr = pl.ds(r, 8)
            gs, gn = shifted_sum(D, r)
            _, xn = shifted_sum(Y0, r)
            for j in range(NT):
                diag = gs[j] * gn[j] + DAMP
                inv = 1.0 / diag
                wid = WET[j, rr, :] * inv
                h = gs[j] * inv
                DG[j, rr, :] = diag
                WID[j, rr, :] = wid
                H[j, rr, :] = h
                Z[j, rr, :] = wid * B[j, rr, :] + h * xn[j] - X[j, rr, :]
            return carry
        for body in (first, second):
            body(8, 0)
            ocean_rows(body, 0)
            body(OR + 16, 0)
        phase(None)

    lax.fori_loop(0, 2, caps, 0)
    ocean_prepare()

    phase("arrive")
    late_block = {0: 2, G - 1: 1}

    def add_block(d, more_from):
        for i in range(IR // 8):
            rr = pl.ds(16 + IR * d + 8 * i, 8)
            for j in range(NT):
                if j < LT:
                    sp = RSP[d, j, pl.ds(8 * i, 8), :]
                else:
                    sp = pltpu.roll(RX[d, 0], 128 - (16 * i + 8), 1)
                if i == 0 and more_from is not None:
                    sp = sp + below_block(more_from, j)
                Z[j, rr, :] = Z[j, rr, :] + WID[j, rr, :] * sp

    def below_block(d, j):
        return jnp.where(sub == 0, jnp.broadcast_to(RX[d, 1][j:j + 1, :], (8, 128)), 0.0)

    def add_below(d):
        rr = pl.ds(16 + IR * (d + 1), 8)
        for j in range(NT):
            Z[j, rr, :] = Z[j, rr, :] + WID[j, rr, :] * below_block(d, j)

    for own, last_in in late_block.items():
        @pl.when(g == own)
        def _(own=own, last_in=last_in):
            rest = [d for d in range(G) if d != last_in]
            for d in rest:
                if d != own:
                    wait_rows(rs.at[R_RS + d], LT * IR + 16)
            for d in rest:
                add_block(d, d - 1 if d - 1 in rest else None)
            if own == 0:
                add_below(G - 1)

    @pl.when(jnp.logical_not(is_owner))
    def _():
        wait_rows(rs.at[R_RH], LT * 8 + 16)

        @pl.when(g == 1)
        def _():
            rr = pl.ds(16, 8)
            for j in range(NT):
                more = jnp.broadcast_to(RXH[1][j:j + 1, :], (8, 128))
                Z[j, rr, :] = Z[j, rr, :] + WID[j, rr, :] * jnp.where(sub == 0, more, 0.0)
        for at, row, i in ((1, 8, 7), (2, OR + 16, 0)):
            @pl.when(g == at)
            def _(row=row, i=i):
                rr = pl.ds(row, 8)
                for j in range(NT):
                    sp = RH[j] if j < LT else pltpu.roll(RXH[0], 128 - (16 * i + 8), 1)
                    Z[j, rr, :] = Z[j, rr, :] + WID[j, rr, :] * sp

    phase("krylov")
    def krylov0(r, acc):
        rr = pl.ds(r, 8)
        for j in range(NT):
            z = Z[j, rr, :]
            Y0[j, rr, :] = D[j, rr, :] * z
            if j < LT and acc is not None:
                acc = (acc[0] + DG[j, rr, :] * z * z,)
        return acc

    def krylov(src, dst, vec, r, acc):
        rr = pl.ds(r, 8)
        y, n = shifted_sum(src, r)
        for j in range(NT):
            v = H[j, rr, :] * n[j]
            out = D[j, rr, :] * v
            vec[j, rr, :] = v
            dst[j, rr, :] = out
            if j < LT and acc is not None:
                acc = (acc[0] + y[j] * n[j], acc[1] + out * n[j])
        return acc

    def krylov3(r, acc):
        if acc is None:
            return None
        y, n = shifted_sum(Y2, r)
        for j in range(LT):
            acc = (acc[0] + y[j] * n[j],)
        return acc

    sweeps = (
        (krylov0, (0,)),
        (functools.partial(krylov, Y0, Y1, V1), (1, 2)),
        (functools.partial(krylov, Y1, Y2, V2), (3, 4)),
        (krylov3, (5,)),
    )
    start = jnp.where(g == 0, 13, jnp.where(g == G - 1, 5, 17))
    end = jnp.where(g == 0, 29, jnp.where(g == G - 1, 21, 17))

    def row_of(group):
        return pl.multiple_of(8 * group + 8, 8)

    for body, into in sweeps:
        body(8, None)
        body(OR + 16, None)
        body(row_of(start), None)
        body(row_of(end - 1), None)

        def four(i, acc, first, body=body):
            for m in range(4):
                acc = body(row_of(first + 4 * i + m), acc)
            return acc
        acc = (zero,) * len(into)
        acc = lax.fori_loop(0, (start - 1) // 4, functools.partial(four, first=1), acc)
        acc = lax.fori_loop(0, (33 - end) // 4, functools.partial(four, first=end), acc)
        for k, m in zip(into, acc):
            MOM[k] = m

    phase("late")
    for own, last_in in late_block.items():
        @pl.when(g == own)
        def _(own=own, last_in=last_in):
            wait_rows(rs.at[R_RS + last_in], LT * IR + 16)
            add_block(last_in, last_in - 1)
            add_below(last_in)

    phase("krylate")

    @pl.when(is_owner)
    def _():
        for body, into in sweeps:
            acc = (zero,) * len(into)
            for m in range(16):
                acc = body(row_of(start + m), acc)
            for k, m in zip(into, acc):
                MOM[k] = MOM[k] + m

    moments = [MOM[k] for k in range(6)]
    phase("red1")
    tile = zero
    for k, m in enumerate(moments):
        tile = jnp.where(sub == k, jnp.sum(m, axis=0, keepdims=True), tile)
    slot1 = 2 * g + core
    L1[slot1] = tile
    for dev in peers1:
        send(L1.at[slot1], L1.at[slot1], S_1, R_1, dev)
    wait_rows(rs.at[R_1], 8 * len(peers1))
    tile = L1[0]
    for k in range(1, 8):
        tile = tile + L1[k]
    phase("red2")
    L2[mine2] = tile
    for dev in peers2:
        send(L2.at[mine2], L2.at[mine2], S_2, R_2, dev)
    wait_rows(rs.at[R_2], 8 * len(peers2))
    tile = L2[0]
    for k in range(1, M2):
        tile = tile + L2[k]
    phase("coef")
    total = jnp.sum(tile, axis=1, keepdims=True)
    mu = [total[k:k + 1, :] for k in range(6)]
    nu = [mu[k] - mu[k + 1] for k in range(5)]

    a0 = mu[0] / nu[0]
    z10, z11 = 1.0 - a0, a0
    rz1 = z11 * (z10 * mu[1] + z11 * mu[2])
    b0 = rz1 / mu[0]
    p10, p11 = z10 + b0, z11
    a1 = rz1 / (p11 * (p10 * nu[1] + p11 * nu[2]))
    z20, z21, z22 = z10 - a1 * p10, z11 - a1 * (p11 - p10), a1 * p11
    rz2 = z22 * (z20 * mu[2] + z21 * mu[3] + z22 * mu[4])
    b1 = rz2 / rz1
    p20, p21, p22 = z20 + b1 * p10, z21 + b1 * p11, z22
    a2 = rz2 / (p22 * (p20 * nu[2] + p21 * nu[3] + p22 * nu[4]))
    k0 = jnp.broadcast_to(a0 + a1 * p10 + a2 * p20, (8, 128))
    k1 = jnp.broadcast_to(a1 * p11 + a2 * p21, (8, 128))
    k2 = jnp.broadcast_to(a2 * p22, (8, 128))

    phase("finish")
    def finish(r, carry):
        rr = pl.ds(r, 8)
        for j in range(LT):
            OUT[j, pl.ds(pl.multiple_of(r - 16, 8), 8), :] = X[j, rr, :] + (
                k0 * Z[j, rr, :] + (k1 * V1[j, rr, :] + k2 * V2[j, rr, :]))
        return carry
    ocean_rows(finish, 0)
    phase("sentwait")
    for s, cond in ((S_FL, jnp.logical_and(is_owner, has_l)), (S_FR, jnp.logical_and(is_owner, has_r))):
        @pl.when(cond)
        def _(s=s):
            wait_rows(ss.at[s], G * 24)
    for s, cond in ((S_L, has_l), (S_R, has_r)):
        @pl.when(cond)
        def _(s=s):
            wait_rows(ss.at[s], 2 * 8 * 8 + 3 * 4 * 8)
    for at in range(G):
        @pl.when(g == at)
        def _(at=at):
            full = (8 * 2 + 3) * 8 * LT + 2 * 16 + 8
            if at > 0:
                less = sum(bottom_summed(c, at - 1) for c in range(2))
                wait_rows(ss.at[S_U], full - less * 2 * 8 * LT)
            if at < G - 1:
                less = sum(top_summed(c, at + 1) for c in range(2))
                wait_rows(ss.at[S_D], full - less * 2 * 8 * LT)
            if at in (0, G - 1):
                c = 0 if at == 0 else 1
                wait_rows(ss.at[S_F], 2 * LT * sum(flow_rows(c, d)[1] for d in dests[at]))
            wait_rows(ss.at[S_FW], (2 if at in (0, G - 1) else 1) * 2 * 8 * LT)
    for c in range(2):
        mine = jnp.logical_and(is_owner, c == owner_cap)

        @pl.when(jnp.logical_not(mine))
        def _(c=c):
            wait_rows(ss.at[S_RS + c], LT * IR + 16)

    @pl.when(is_owner)
    def _():
        wait_rows(ss.at[S_RH], LT * 8 + 16)
    wait_rows(ss.at[S_1], 8 * len(peers1))
    wait_rows(ss.at[S_2], 8 * len(peers2))
    for dy, dx, cond in nbrs:
        k = 3 * (1 - dy) + (1 - dx)
        @pl.when(cond)
        def _(dy=dy, dx=dx, k=k):
            dev = (g + dy, t + dx)
            pltpu.make_async_remote_copy(
                src_ref=iblk, dst_ref=BI.at[1 - dy, 1 - dx], send_sem=ss.at[S_BI + k],
                recv_sem=rs.at[R_BI + k], device_id=dev, device_id_type=MESH).wait_send()
            rows = pl.ds(0, OR // BS) if dy == 0 else pl.ds(0 if dy < 0 else OR // BS - 8, 8)
            pltpu.make_async_remote_copy(
                src_ref=land.at[rows], dst_ref=BO.at[1 - dy, 1 - dx, rows], send_sem=ss.at[S_BO + k],
                recv_sem=rs.at[R_BO + k], device_id=dev, device_id_type=MESH).wait_send()
    phase(None)


def shards(T, *args):
    ice = (2, NT, IH, 128)
    ocean = (NT, OH, 128)
    vm = lambda *s: pltpu.VMEM(s, F32)
    scratch = [
        vm(2, *ice), vm(*ice), vm(2, *ice), vm(*ice), vm(*ice), vm(*ice),
        vm(2, 2, 8, 8, 128), vm(2, 2, 8, 8, 128), vm(2, 3, 4, 8, 128), vm(2, 3, 4, 8, 128),
        vm(2, G, 3, 8, 128), vm(2, 2, 3, 8, 128), vm(2, 2, 2, 8, 128), vm(2, 2, 2, 8, 128),
        vm(2, 8, 128), vm(2, 8, 128), vm(2, 2, OR, 128), vm(2, LT, 8, 128),
        *[vm(*ocean) for _ in range(13)],
        pltpu.VMEM((3, 3, 2, 8, 64), jnp.int32), pltpu.VMEM((3, 3, 32, 64), jnp.int32),
        vm(2, LT, IR, 128), vm(2, 2, 8, 128),
        vm(G, LT, IR, 128), vm(G, 2, 8, 128), vm(LT, 8, 128), vm(2, 8, 128),
        vm(8, 8, 128), vm(T // 2, 8, 128), vm(6, 8, 128), vm(DUMMY, 128),
        pltpu.SemaphoreType.DMA((N_R,)), pltpu.SemaphoreType.DMA((N_S,)), pltpu.SemaphoreType.DMA((N_L,)),
    ]
    hbm = pl.BlockSpec(memory_space=pltpu.HBM)
    vmem = pl.BlockSpec(memory_space=pltpu.VMEM)
    worked = pl.pallas_call(
        functools.partial(kernel, T),
        out_shape=(vm(2, *ice), vm(3, *ice), vm(LT, OR, 128)),
        in_specs=[hbm] * 10,
        out_specs=(vmem, vmem, vmem),
        scratch_shapes=scratch,
        compiler_params=pltpu.CompilerParams(
            collective_id=0, has_side_effects=True, vmem_limit_bytes=60 * 1024 * 1024),
    )(*args)
    return pl.pallas_call(
        deliver,
        out_shape=(
            jax.ShapeDtypeStruct((OR, 128 * LT), F32),
            jax.ShapeDtypeStruct((2, 2, IR, 128 * LT), F32),
            jax.ShapeDtypeStruct((3, 2, IR, 128 * LT), F32),
        ),
        in_specs=[vmem] * 3,
        out_specs=(hbm, hbm, hbm),
        scratch_shapes=[pltpu.SemaphoreType.DMA((3, LT))],
        compiler_params=pltpu.CompilerParams(vmem_limit_bytes=1024 * 1024),
    )(*worked)


def deliver(V, S, OUT, o_ssh, o_vel, o_str, sem):
    copies = []
    for j in range(LT):
        to = pl.ds(128 * j, 128)
        copies += [
            pltpu.make_async_copy(S.at[:, :, j, pl.ds(16, IR), :], o_str.at[:, :, :, to], sem.at[0, j]),
            pltpu.make_async_copy(V.at[:, :, j, pl.ds(16, IR), :], o_vel.at[:, :, :, to], sem.at[1, j]),
            pltpu.make_async_copy(OUT.at[j], o_ssh.at[:, to], sem.at[2, j]),
        ]
    for c in copies:
        c.start()
    for c in copies:
        c.wait()


def solution(mesh):
    return jax.shard_map(
        functools.partial(shards, mesh.shape["tile"]),
        mesh=mesh,
        in_specs=(
            P("grp", "tile"),
            P("grp", "tile"),
            P("grp", "tile"),
            P(None, "grp", "tile"),
            P("grp", "tile"),
            P(None, "grp", "tile"),
            P(None, "grp", "tile"),
            P(None, None, "grp", "tile"),
            P(None, None, "grp", "tile"),
            P(None, None, "grp", "tile"),
        ),
        out_specs=(P("grp", "tile"), P(None, None, "grp", "tile"), P(None, None, "grp", "tile")),
        check_vma=False,
    )
```

```python
import functools

import jax
import jax.numpy as jnp
from jax import lax
from jax.experimental import pallas as pl
from jax.experimental.pallas import tpu as pltpu
from jax.sharding import PartitionSpec as P

BS = 8
NSUB = 8
DAMP = 0.05
RELAX = 0.2
STRENGTH = 0.5
DRAG = 1.0
STEP = 0.5
G = 4
LT = 4
NT = LT + 1
IR = 64
OR = 256
IH = IR + 40
OH = OR + 40
F32 = jnp.float32
MESH = pl.DeviceIdType.MESH
DUMMY = 4096

R_PL, R_PR, R_FU, R_FD, R_IL, R_IR, R_OL, R_OR = 41, 43, 45, 47, 4, 5, 6, 7
R_IU, R_ID, R_F = 8, 10, 12
R_OU, R_OD, R_RS, R_RH, R_1, R_2 = 14, 15, 16, 20, 21, 22
R_BI, R_BO = 23, 32
N_R = 49
S_FL, S_FR, S_L, S_R, S_U, S_D, S_F, S_RS, S_1, S_2 = 0, 1, 2, 3, 4, 5, 6, 7, 9, 10
S_RH, S_FW = 11, 30
S_BI, S_BO = 12, 21
N_S = 31
L_BLK, L_ICE, L_FL, L_OC, L_OUT, L_OUTS, L_ED = 0, 1, 2, 3, 4, 5, 6
N_L = 7


def east(tiles, lane):
    turned = [pltpu.roll(x, 127, 1) for x in tiles]
    return [jnp.where(lane == 127, turned[(j + 1) % NT], turned[j]) for j in range(NT)]


def west(tiles, lane):
    turned = [pltpu.roll(x, 1, 1) for x in tiles]
    return [jnp.where(lane == 0, turned[(j - 1) % NT], turned[j]) for j in range(NT)]


class Phases:
    def __init__(self):
        self.open = None

    def __call__(self, name):
        if self.open is not None:
            self.open.__exit__(None, None, None)
        self.open = None
        if name:
            self.open = jax.named_scope(name)
            self.open.__enter__()


def kernel(
    T,
    base, depth, ssh, cur, land, thick, iblk, ivel, istr, wind,
    V, S, OUT,
    W, TH, FL, CV, C1, C2,
    PI, LI, PC, LC, PF, LF, PH, LH, PHO, LHO, CE, FE,
    B, D, X, Z, Y0, Y1, Y2, H, WID, DG, WET, V1, V2,
    BI, BO, PB, LB, SPB, XB, RSP, RX, RH, RXH, L1, L2, MOM, DUM,
    rs, ss, ls,
):
    g = lax.axis_index("grp")
    t = lax.axis_index("tile")
    has_l, has_r, has_u, has_d = t > 0, t < T - 1, g > 0, g < G - 1
    lane = lax.broadcasted_iota(jnp.int32, (8, 128), 1)
    sub = lax.broadcasted_iota(jnp.int32, (8, 128), 0)
    zero = jnp.zeros((8, 128), F32)
    first_cap = g // 2
    owner_cap = jnp.where(g == 0, 0, 1)
    is_owner = jnp.logical_or(g == 0, g == G - 1)

    def wait_rows(sem, rows):
        pltpu.make_async_copy(DUM.at[pl.ds(0, rows)], DUM.at[pl.ds(0, rows)], sem).wait()

    def send(src, dst, s, r, dev):
        pltpu.make_async_remote_copy(
            src_ref=src, dst_ref=dst, send_sem=ss.at[s], recv_sem=rs.at[r],
            device_id=dev, device_id_type=MESH,
        ).start()

    def local(src, dst, s):
        pltpu.make_async_copy(src, dst, ls.at[s]).start()

    def cols(j):
        return pl.ds(128 * j, 128)

    nbrs = []
    for dy in (-1, 0, 1):
        for dx in (-1, 0, 1):
            if dy == 0 and dx == 0:
                continue
            cond = None
            for need, there in ((dy < 0, has_u), (dy > 0, has_d), (dx < 0, has_l), (dx > 0, has_r)):
                if need:
                    cond = there if cond is None else jnp.logical_and(cond, there)
            nbrs.append((dy, dx, cond))

    def top_summed(c, d):
        return (c == 0 and d in (1, 2)) or (c == 1 and d == 1)

    def bottom_summed(c, d):
        return (c == 1 and d in (1, 2)) or (c == 0 and d == 2)

    def top_is_summed(c):
        return jnp.logical_or(g == 1, jnp.logical_and(g == 2, c == 0))

    def bottom_is_summed(c):
        return jnp.logical_or(g == 2, jnp.logical_and(g == 1, c == 1))

    phase = Phases()
    phase("signal")
    barrier = pltpu.get_barrier_semaphore()
    core = lax.rem(t, 2)
    M2 = T // 2
    mine2 = t // 2
    peers1 = []
    for dg in range(G):
        for dc in range(2):
            if dg or dc:
                peers1.append((lax.rem(g + dg, G), t - core + lax.rem(core + dc, 2)))
    peers2 = [(g, 2 * lax.rem(mine2 + k, M2) + core) for k in range(1, M2)]
    for dg in range(G):
        for dx, cond in ((-1, has_l), (0, None), (1, has_r)):
            dev = (lax.rem(g + dg, G), t + dx)
            if cond is not None:
                @pl.when(cond)
                def _(dev=dev):
                    pl.semaphore_signal(barrier, inc=1, device_id=dev, device_id_type=MESH)
            elif dg:
                pl.semaphore_signal(barrier, inc=1, device_id=dev, device_id_type=MESH)
    for dev in peers2:
        pl.semaphore_signal(barrier, inc=1, device_id=dev, device_id_type=MESH)

    phase("loads")
    local(iblk, BI.at[1], L_BLK)
    local(land, BO.at[1], L_BLK)
    for j in range(LT):
        local(ivel.at[:, :, :, cols(j)], V.at[:, :, j, pl.ds(16, IR), :], L_ICE)
        local(istr.at[:, :, :, cols(j)], S.at[:, :, j, pl.ds(16, IR), :], L_ICE)
        local(wind.at[:, :, :, cols(j)], W.at[:, :, j, pl.ds(16, IR), :], L_ICE)
        local(thick.at[:, :, cols(j)], TH.at[:, j, pl.ds(16, IR), :], L_ICE)
        local(base.at[:, cols(j)], B.at[j, pl.ds(16, OR), :], L_OC)
        local(depth.at[:, cols(j)], D.at[j, pl.ds(16, OR), :], L_OC)
        local(ssh.at[:, cols(j)], X.at[j, pl.ds(16, OR), :], L_OC)

    @pl.when(is_owner)
    def _():
        local(cur.at[:, :, cols(0)], CE.at[0], L_ED)
        local(cur.at[:, :, cols(LT - 1)], CE.at[1], L_ED)

    pltpu.make_async_copy(iblk, BI.at[1], ls.at[L_BLK]).wait()
    pltpu.make_async_copy(land, BO.at[1], ls.at[L_BLK]).wait()
    line = lax.broadcasted_iota(jnp.int32, (8, 64), 0)
    for e, i, o in ((0, 0, 0), (1, 7, 7)):
        ends = [BI[1, 0][i:i + 1], BI[1, 1][i:i + 1], BO[1, 24 * e:24 * e + 8][o:o + 1]]
        ends = [jnp.broadcast_to(x, (8, 64)) for x in ends]
        PB[e] = jnp.where(line == 0, ends[0], jnp.where(line == 1, ends[1], ends[2]))

    phase("barrier")
    wide = 1 + jnp.minimum(t, 1) + jnp.minimum(T - 1 - t, 1)
    pl.semaphore_wait(barrier, G * wide - 1 + len(peers2))

    phase("sends")
    left, right, up, down = (g, t - 1), (g, t + 1), (g - 1, t), (g + 1, t)
    for dy, dx, cond in nbrs:
        k = 3 * (1 - dy) + (1 - dx)
        @pl.when(cond)
        def _(dy=dy, dx=dx, k=k):
            dev = (g + dy, t + dx)
            if dy == 0:
                send(iblk, BI.at[1 - dx], S_BI + k, R_BI + k, dev)
                send(land, BO.at[1 - dx], S_BO + k, R_BO + k, dev)
            else:
                e = 0 if dy < 0 else 1
                send(PB.at[e], LB.at[1 - e, 1 - dx], S_BI + k, R_BI + k, dev)

    def flow_rows(c, d):
        lo = IR * d if d == 0 or top_summed(c, d) else IR * d - 8
        hi = IR * d + IR if d == G - 1 or bottom_summed(c, d) else IR * d + IR + 8
        return lo, hi - lo, 16 + lo - IR * d

    dests = {0: (1, 3, 2), G - 1: (2, 0, 1)}

    def send_flow(c, d):
        lo, n, at = flow_rows(c, d)
        for j in range(LT):
            send(cur.at[:, pl.ds(lo, n), cols(j)], FL.at[:, c, j, pl.ds(at, n), :],
                 S_F, R_F + c, (d, t))

    def halo_ice(dev, c, src, dst, s, r):
        there = dev[0]
        if s == S_D:
            summed = jnp.logical_or(there == 1, jnp.logical_and(there == 2, c == 0))
        else:
            summed = jnp.logical_or(there == 2, jnp.logical_and(there == 1, c == 1))

        @pl.when(jnp.logical_not(summed))
        def _():
            for j in range(LT):
                send(wind.at[:, c, pl.ds(src, 8), cols(j)], W.at[:, c, j, pl.ds(dst, 8), :], s, r, dev)
        for j in range(LT):
            send(ivel.at[:, c, pl.ds(src, 8), cols(j)], V.at[:, c, j, pl.ds(dst, 8), :], s, r, dev)
            send(istr.at[:, c, pl.ds(src, 8), cols(j)], S.at[:, c, j, pl.ds(dst, 8), :], s, r, dev)
            send(thick.at[c, pl.ds(src, 8), cols(j)], TH.at[c, j, pl.ds(dst, 8), :], s, r, dev)

    def halo_turn(turn):
        for dev, cond, src, dst, s, r in (
            (up, has_u, 0, IR + 16, S_U, R_ID),
            (down, has_d, IR - 8, 8, S_D, R_IU),
        ):
            @pl.when(cond)
            def _(dev=dev, src=src, dst=dst, s=s, r=r):
                there = dev[0] // 2
                c = there if turn == 0 else 1 - there
                halo_ice(dev, c, src, dst, s, r + c)

    for own, c in ((0, 0), (G - 1, 1)):
        @pl.when(g == own)
        def _(own=own, c=c):
            send_flow(c, dests[own][0])
            send_flow(c, dests[own][1])
            lo, n, at = flow_rows(c, own)
            for j in range(LT):
                local(cur.at[:, pl.ds(lo, n), cols(j)], FL.at[:, c, j, pl.ds(at, n), :], L_FL)
    halo_turn(0)

    phase("zeros")
    for cond, row, orow, by in ((g == 0, 8, 8, 0), (g == G - 1, IR + 16, OR + 16, 1)):
        @pl.when(cond)
        def _(row=row, orow=orow, by=by):
            for c in range(2):
                for j in range(NT):
                    for k in range(3):
                        S[k, c, j, pl.ds(row, 8), :] = zero
                    for k in range(2):
                        V[k, c, j, pl.ds(row, 8), :] = zero
                        W[k, c, j, pl.ds(row, 8), :] = zero
                        FL[k, c, j, pl.ds(row, 8), :] = zero
                    TH[c, j, pl.ds(row, 8), :] = zero
            for j in range(NT):
                B[j, pl.ds(orow, 8), :] = zero
                D[j, pl.ds(orow, 8), :] = zero
                X[j, pl.ds(orow, 8), :] = zero
            for x in range(3):
                LB[by, x] = jnp.zeros((8, 64), jnp.int32)

    for d in (1, 2):
        @pl.when(g == d)
        def _(d=d):
            for c in range(2):
                for here, row in ((top_summed(c, d), 8), (bottom_summed(c, d), IR + 16)):
                    if here:
                        for k in range(2):
                            for j in range(LT):
                                FL[k, c, j, pl.ds(row, 8), :] = zero

    for cond, side, bx in ((t == 0, 0, 0), (t == T - 1, 1, 2)):
        @pl.when(cond)
        def _(side=side, bx=bx):
            for c in range(2):
                for k in range(8):
                    LI[side, c, k] = zero
                for v in range(3):
                    LF[side, c, v] = zero
            for k in range(3):
                for v in range(4):
                    LC[side, k, v] = zero
            for y in range(2):
                LB[y, bx] = jnp.zeros((8, 64), jnp.int32)
                BI[bx, y] = jnp.zeros((8, 64), jnp.int32)
            BO[bx] = jnp.zeros((32, 64), jnp.int32)

    phase("pack")
    slot_of = lane // 16

    def put(pack, e, at, x):
        moved = pltpu.roll(x, 16 * at, 1) if at else x
        return jnp.where(slot_of == (at - e) % 8, moved, pack)

    def take(from_right, from_left, at):
        both = jnp.where(slot_of == at, from_right, from_left)
        return pltpu.roll(both, 128 - 16 * at, 1) if at else both

    wait_rows(ls.at[L_ICE], 8 * 2 * IR * LT)

    def ice_get(k, c, j, r):
        if k < 2:
            return V[k, c, j, pl.ds(r, 8), :]
        if k < 5:
            return S[k - 2, c, j, pl.ds(r, 8), :]
        return W[k - 5, c, j, pl.ds(r, 8), :] if k < 7 else TH[c, j, pl.ds(r, 8), :]

    def ice_set(k, c, j, r, x):
        if k < 2:
            V[k, c, j, pl.ds(r, 8), :] = x
        elif k < 5:
            S[k - 2, c, j, pl.ds(r, 8), :] = x
        elif k < 7:
            W[k - 5, c, j, pl.ds(r, 8), :] = x
        else:
            TH[c, j, pl.ds(r, 8), :] = x

    for e, j in ((0, 0), (1, LT - 1)):
        for c in range(2):
            for k in range(8):
                pack = zero
                for i in range(IR // 8):
                    pack = put(pack, e, i, ice_get(k, c, j, 16 + 8 * i))
                PI[e, c, k] = pack

    for own in (0, G - 1):
        @pl.when(g == own)
        def _(own=own):
            wait_rows(ls.at[L_ED], 2 * 2 * OR)
            for e in range(2):
                for d in range(G):
                    packs = [zero] * 3
                    for k in range(2):
                        for s in range(10):
                            q = 8 * d - 1 + s
                            if 0 <= q < OR // 8:
                                m = 10 * k + s
                                packs[m // 8] = put(packs[m // 8], e, m % 8, CE[e, k, pl.ds(8 * q, 8), :])
                    for v in range(3):
                        PF[e, d, v] = packs[v]

    wait_rows(ls.at[L_OC], 3 * OR * LT)
    for e, j in ((0, 0), (1, LT - 1)):
        for k, ref in enumerate((B, D, X)):
            for v in range(4):
                pack = zero
                for i in range(8):
                    pack = put(pack, e, i, ref[j, pl.ds(16 + 64 * v + 8 * i, 8), :])
                PC[e, k, v] = pack

    for e, dev, cond, s, ri, ro in ((0, left, has_l, S_L, R_IR, R_OR), (1, right, has_r, S_R, R_IL, R_OL)):
        @pl.when(cond)
        def _(e=e, dev=dev, s=s, ri=ri, ro=ro):
            send(PI.at[e], LI.at[1 - e], s, ri, dev)
            send(PC.at[e], LC.at[1 - e], s, ro, dev)

    for own, c in ((0, 0), (G - 1, 1)):
        @pl.when(g == own)
        def _(own=own, c=c):
            for e, dx, cond, s, r in ((0, -1, has_l, S_FL, R_PR), (1, 1, has_r, S_FR, R_PL)):
                @pl.when(cond)
                def _(e=e, dx=dx, s=s, r=r):
                    for dg in range(G):
                        d = dg if own == 0 else G - 1 - dg
                        dev = (g + dg if own == 0 else g - dg, t + dx)
                        send(PF.at[e, d], LF.at[1 - e, c], s, r + c, dev)

    phase("mergeice")
    @pl.when(has_l)
    def _():
        wait_rows(rs.at[R_IL], 2 * 8 * 8)

    @pl.when(has_r)
    def _():
        wait_rows(rs.at[R_IR], 2 * 8 * 8)

    quarter = lane // 32
    for c in range(2):
        ends = [[zero, zero], [zero, zero]]
        for k in range(8):
            for i in range(IR // 8):
                x = take(LI[1, c, k], LI[0, c, k], i)
                ice_set(k, c, LT, 16 + 8 * i, x)
                for e, at in ((0, 0), (1, IR // 8 - 1)):
                    if i == at:
                        moved = pltpu.roll(x, (32 * (k % 4) + 16) % 128, 1)
                        ends[e][k // 4] = jnp.where(quarter == k % 4, moved, ends[e][k // 4])
        for e in range(2):
            for v in range(2):
                PH[e, c, v] = ends[e][v]
    for e, dev, cond, s, r in ((0, up, has_u, S_U, R_ID), (1, down, has_d, S_D, R_IU)):
        @pl.when(cond)
        def _(e=e, dev=dev, s=s, r=r):
            for c in range(2):
                send(PH.at[e, c], LH.at[1 - e, c], s, r + c, dev)

    for own, c, row, to, dev, r in (
        (0, 0, IR + 8, 8, down, R_FU), (G - 1, 1, 16, IR + 16, up, R_FD + 1)):
        @pl.when(g == own)
        def _(c=c, row=row, to=to, dev=dev, r=r):
            wait_rows(ls.at[L_FL], 2 * (IR + 8) * LT)
            for k in range(2):
                for j in range(LT):
                    FE[k, j] = W[k, c, j, pl.ds(row, 8), :] + FL[k, c, j, pl.ds(row, 8), :] * DRAG
            for j in range(LT):
                send(FE.at[:, j], W.at[:, c, j, pl.ds(to, 8), :], S_FW, r, dev)

    for own, c in ((0, 0), (G - 1, 1)):
        @pl.when(g == own)
        def _(own=own, c=c):
            send_flow(c, dests[own][2])
    halo_turn(1)
    def ocean_ends():
        for dev, cond, at, to, s, r in (
            (up, has_u, 0, OR + 16, S_U, R_OD),
            (down, has_d, OR - 8, 8, S_D, R_OU),
        ):
            @pl.when(cond)
            def _(dev=dev, at=at, to=to, s=s, r=r):
                for j in range(LT):
                    send(base.at[pl.ds(at, 8), cols(j)], B.at[j, pl.ds(to, 8), :], s, r, dev)
                    send(depth.at[pl.ds(at, 8), cols(j)], D.at[j, pl.ds(to, 8), :], s, r, dev)
                    send(ssh.at[pl.ds(at, 8), cols(j)], X.at[j, pl.ds(to, 8), :], s, r, dev)

    phase("mergeoc")
    @pl.when(has_l)
    def _():
        wait_rows(rs.at[R_OL], 3 * 4 * 8)

    @pl.when(has_r)
    def _():
        wait_rows(rs.at[R_OR], 3 * 4 * 8)

    ends = [zero, zero]
    for k, ref in enumerate((B, D, X)):
        for q in range(OR // 8):
            x = take(LC[1, k, q // 8], LC[0, k, q // 8], q % 8)
            ref[LT, pl.ds(16 + 8 * q, 8), :] = x
            for e, at in ((0, 0), (1, OR // 8 - 1)):
                if q == at:
                    moved = pltpu.roll(x, 32 * k + 16, 1)
                    ends[e] = jnp.where(quarter == k, moved, ends[e])
    for e, dev, cond, s, r in ((0, up, has_u, S_U, R_OD), (1, down, has_d, S_D, R_OU)):
        PHO[e] = ends[e]
        @pl.when(cond)
        def _(e=e, dev=dev, s=s, r=r):
            send(PHO.at[e], LHO.at[1 - e], s, r, dev)

    phase("masks")
    def block_pairs(dy, x, e):
        if dy == 0:
            return [(iblk, BI.at[x], S_BI, R_BI), (land, BO.at[x], S_BO, R_BO)]
        return [(PB.at[e], LB.at[1 - e, x], S_BI, R_BI)]

    for dy, dx, cond in nbrs:
        k = 3 * (1 + dy) + (1 + dx)
        @pl.when(cond)
        def _(dy=dy, dx=dx, k=k):
            dev = (g + dy, t + dx)
            pairs = block_pairs(dy, 1 + dx, 1 if dy < 0 else 0)
            for src, dst, s, r in pairs:
                pltpu.make_async_remote_copy(
                    src_ref=src, dst_ref=dst, send_sem=ss.at[s + k], recv_sem=rs.at[r + k],
                    device_id=dev, device_id_type=MESH).wait_recv()

    def selection(width, first, start):
        block = lax.broadcasted_iota(jnp.int32, (64, width), 0)
        at = lax.broadcasted_iota(jnp.int32, (64, width), 1)
        hit = block == at // BS + first
        if start is not None:
            hit = jnp.logical_and(hit, (at < 64) if start == 0 else (at >= 64))
        return hit.astype(F32)

    sel_c = selection(128 * LT, 0, None)
    sel_r = selection(128, 0, 0)
    sel_l = selection(128, 48, 1)

    def spread_rows(refs):
        lft, mid, rgt = (ref.astype(F32) for ref in refs)
        wide = jnp.dot(mid, sel_c, preferred_element_type=F32)
        last = jnp.dot(rgt, sel_r, preferred_element_type=F32) + jnp.dot(
            lft, sel_l, preferred_element_type=F32)
        return wide, last

    def paint(ref, row, parts, b):
        wide, last = parts
        for j in range(LT):
            ref[j, pl.ds(row, 8), :] = jnp.broadcast_to(wide[b:b + 1, 128 * j:128 * j + 128], (8, 128))
        ref[LT, pl.ds(row, 8), :] = jnp.broadcast_to(last[b:b + 1, :], (8, 128))

    ends = [spread_rows([LB[y, x] for x in range(3)]) for y in range(2)]
    for c in range(2):
        cov = CV.at[c]
        paint(cov, 8, ends[0], c)
        mid = spread_rows([BI[x, c] for x in range(3)])
        for b in range(8):
            paint(cov, 16 + 8 * b, mid, b)
        paint(cov, IR + 16, ends[1], c)
    paint(WET, 8, ends[0], 2)
    for q in range(4):
        mid = spread_rows([BO[x, 8 * q:8 * q + 8] for x in range(3)])
        for b in range(8):
            paint(WET, 16 + 64 * q + 8 * b, mid, b)
    paint(WET, OR + 16, ends[1], 2)

    def pass_on(c, row, to, dev, r):
        for j in range(LT):
            send(W.at[:, c, j, pl.ds(row, 8), :], W.at[:, c, j, pl.ds(to, 8), :], S_FW, r + c, dev)

    def cap(c, turn):
        phase = Phases()
        phase("capwait")

        for e, cond, r, row, rf, summed in (
            (0, has_u, R_IU, 8, R_FU, top_is_summed(c)),
            (1, has_d, R_ID, IR + 16, R_FD, bottom_is_summed(c)),
        ):
            @pl.when(cond)
            def _(e=e, r=r, row=row, rf=rf, summed=summed):
                @pl.when(summed)
                def _():
                    wait_rows(rs.at[rf + c], 2 * 8 * LT)
                    wait_rows(rs.at[r + c], 6 * 8 * LT + 16)

                @pl.when(jnp.logical_not(summed))
                def _():
                    wait_rows(rs.at[r + c], 8 * 8 * LT + 16)
                for k in range(8):
                    x = pltpu.roll(LH[e, c, k // 4], (128 - 32 * (k % 4) - 16) % 128, 1)
                    ice_set(k, c, LT, row, x)

        @pl.when(has_l)
        def _():
            wait_rows(rs.at[R_PL + c], 24)

        @pl.when(has_r)
        def _():
            wait_rows(rs.at[R_PR + c], 24)

        for k in range(2):
            for s in range(10):
                m = 10 * k + s
                FL[k, c, LT, pl.ds(8 + 8 * s, 8), :] = take(LF[1, c, m // 8], LF[0, c, m // 8], m % 8)

        mine = jnp.logical_and(is_owner, c == owner_cap)
        at_end = jnp.logical_or(jnp.logical_and(c == 0, g == G - 1), jnp.logical_and(c == 1, g == 0))

        @pl.when(jnp.logical_not(mine))
        def _():
            both = jnp.logical_and(top_is_summed(c), bottom_is_summed(c))

            @pl.when(both)
            def _():
                wait_rows(rs.at[R_F + c], 2 * IR * LT)

            @pl.when(jnp.logical_not(both))
            def _():
                wait_rows(rs.at[R_F + c], 2 * (IR + 8) * LT)

        phase("prepare")
        def prepare(i, carry):
            r = pl.ds(pl.multiple_of(8 * i + 8, 8), 8)
            for j in range(NT):
                cov = CV[c, j, r, :]
                thc = TH[c, j, r, :] * cov
                scale = cov / (thc + (1.0 + STEP * DRAG))
                C1[c, j, r, :] = scale * (thc + 1.0)
                C2[c, j, r, :] = scale * STEP
                TH[c, j, r, :] = thc * (RELAX * STRENGTH / (1.0 + RELAX))
                for k in range(2):
                    W[k, c, j, r, :] = W[k, c, j, r, :] + FL[k, c, j, r, :] * DRAG
            return carry
        lax.fori_loop(0, IR // 8 + 2, prepare, 0)

        @pl.when(jnp.logical_and(c == 0, g == 1))
        def _():
            pass_on(0, IR + 8, 8, down, R_FU)

        @pl.when(jnp.logical_and(c == 0, g == G - 1))
        def _():
            pass_on(0, 16, IR + 16, up, R_FD)

        @pl.when(jnp.logical_and(c == 1, g == 0))
        def _():
            pass_on(1, IR + 8, 8, down, R_FU)

        @pl.when(jnp.logical_and(c == 1, g == 2))
        def _():
            pass_on(1, 16, IR + 16, up, R_FD)

        phase("subcycles")
        @pl.when(turn == 1)
        def _():
            ocean_ends()

        keep = 1.0 / (1.0 + RELAX)

        def group(r):
            rr = pl.ds(r, 8)
            u = [V[0, c, j, rr, :] for j in range(NT)]
            v = [V[1, c, j, rr, :] for j in range(NT)]
            ue, ve = east(u, lane), east(v, lane)
            s0, s1, s2 = [], [], []
            for j in range(NT):
                dux = V[0, c, j, pl.ds(r + 1, 8), :] - u[j]
                dvx = V[1, c, j, pl.ds(r + 1, 8), :] - v[j]
                duy, dvy = ue[j] - u[j], ve[j] - v[j]
                ed, et, es = dux + dvy, dux - dvy, duy + dvx
                inv = lax.rsqrt(ed * ed + et * et + es * es + 1.0)
                a = TH[c, j, rr, :]
                ai = a * inv
                s0.append(S[0, c, j, rr, :] * keep + (ed * ai - a))
                s1.append(S[1, c, j, rr, :] * keep + et * ai)
                s2.append(S[2, c, j, rr, :] * keep + es * ai)
                S[0, c, j, rr, :] = s0[j]
                S[1, c, j, rr, :] = s1[j]
                S[2, c, j, rr, :] = s2[j]

        def push(r):
            rr, above = pl.ds(r, 8), pl.ds(r - 1, 8)
            s0 = [S[0, c, j, rr, :] for j in range(NT)]
            s1 = [S[1, c, j, rr, :] for j in range(NT)]
            s2 = [S[2, c, j, rr, :] for j in range(NT)]
            dif = [s0[j] - s1[j] for j in range(NT)]
            dw, sw = west(dif, lane), west(s2, lane)
            for j in range(NT):
                tot_up = S[0, c, j, above, :] + S[1, c, j, above, :]
                f0 = 0.5 * ((s0[j] + s1[j]) - tot_up) + (s2[j] - sw[j])
                f1 = 0.5 * (dif[j] - dw[j]) + (s2[j] - S[2, c, j, above, :])
                c1, c2 = C1[c, j, rr, :], C2[c, j, rr, :]
                V[0, c, j, rr, :] = c1 * V[0, c, j, rr, :] + c2 * (f0 + W[0, c, j, rr, :])
                V[1, c, j, rr, :] = c1 * V[1, c, j, rr, :] + c2 * (f1 + W[1, c, j, rr, :])

        def subcycle(n, carry):
            for i in range(IR // 8 + 2):
                group(8 + 8 * i)
            for i in range(IR // 8 + 2):
                push(8 + 8 * i)
            return carry
        lax.fori_loop(0, NSUB, subcycle, 0)

        phase("diverge")
        prev = [zero] * NT
        pack = zero
        for i in range(IR // 8):
            rr = pl.ds(16 + 8 * i, 8)
            p0, p1 = [], []
            for j in range(NT):
                cov = CV[c, j, rr, :] * DRAG
                p0.append(cov * (V[0, c, j, rr, :] - FL[0, c, j, rr, :]))
                p1.append(cov * (V[1, c, j, rr, :] - FL[1, c, j, rr, :]))
            pw = west(p1, lane)
            for j in range(NT):
                turned = pltpu.roll(p0[j], 1, 0)
                above = jnp.where(sub == 0, prev[j], turned)
                prev[j] = turned
                sp = (p0[j] - above) + (p1[j] - pw[j])
                if j < LT:
                    SPB[c, j, pl.ds(8 * i, 8), :] = sp
                else:
                    pack = jnp.where(lane // 16 == i, pltpu.roll(sp, 16 * i + 8, 1), pack)
        XB[c, 0] = pack
        extra = zero
        for j in range(NT):
            extra = jnp.where(sub == j, -jnp.broadcast_to(prev[j][0:1, :], (8, 128)), extra)
        XB[c, 1] = extra

        @pl.when(mine)
        def _():
            for j in range(LT):
                for i in range(IR // 8):
                    RSP[g, j, pl.ds(8 * i, 8), :] = SPB[c, j, pl.ds(8 * i, 8), :]
            RX[g, 0] = XB[c, 0]
            RX[g, 1] = XB[c, 1]

        @pl.when(jnp.logical_not(mine))
        def _():
            dev = (c * (G - 1), t)
            send(SPB.at[c], RSP.at[g], S_RS + c, R_RS + g, dev)
            send(XB.at[c], RX.at[g], S_RS + c, R_RS + g, dev)

        @pl.when(at_end)
        def _():
            at = jnp.where(c == 0, IR - 8, 0)
            dev = (1 + c, t)
            send(SPB.at[c, :, pl.ds(pl.multiple_of(at, 8), 8), :], RH, S_RH, R_RH, dev)
            send(XB.at[c], RXH, S_RH, R_RH, dev)
        phase(None)

    def caps(turn, carry):
        cap(jnp.where(turn == 0, first_cap, 1 - first_cap), turn)
        return carry

    def ocean_rows(body, carry, unroll=4):
        def step(i, cc):
            for m in range(unroll):
                cc = body(pl.multiple_of(8 * (unroll * i + m) + 16, 8), cc)
            return cc
        return lax.fori_loop(0, OR // 8 // unroll, step, carry)

    def shifted_sum(ref, r):
        rr = pl.ds(r, 8)
        mid = [ref[j, rr, :] for j in range(NT)]
        e, w = east(mid, lane), west(mid, lane)
        return mid, [
            (ref[j, pl.ds(r + 1, 8), :] + ref[j, pl.ds(r - 1, 8), :]) + (e[j] + w[j])
            for j in range(NT)
        ]

    def ocean_prepare():
        phase = Phases()
        phase("oceanwait")

        for e, cond, r, row in ((0, has_u, R_OU, 8), (1, has_d, R_OD, OR + 16)):
            @pl.when(cond)
            def _(e=e, r=r, row=row):
                wait_rows(rs.at[r], 24 * LT + 8)
                for k, ref in enumerate((B, D, X)):
                    ref[LT, pl.ds(row, 8), :] = pltpu.roll(LHO[e], 128 - 32 * k - 16, 1)

        phase("oceanprep")
        def first(r, carry):
            rr = pl.ds(r, 8)
            for j in range(NT):
                gg = D[j, rr, :] * WET[j, rr, :]
                D[j, rr, :] = gg
                Y0[j, rr, :] = gg * X[j, rr, :]
            return carry

        def second(r, carry):
            rr = pl.ds(r, 8)
            gs, gn = shifted_sum(D, r)
            _, xn = shifted_sum(Y0, r)
            for j in range(NT):
                diag = gs[j] * gn[j] + DAMP
                inv = 1.0 / diag
                wid = WET[j, rr, :] * inv
                h = gs[j] * inv
                DG[j, rr, :] = diag
                WID[j, rr, :] = wid
                H[j, rr, :] = h
                Z[j, rr, :] = wid * B[j, rr, :] + h * xn[j] - X[j, rr, :]
            return carry
        for body in (first, second):
            body(8, 0)
            ocean_rows(body, 0)
            body(OR + 16, 0)
        phase(None)

    lax.fori_loop(0, 2, caps, 0)
    ocean_prepare()

    phase("arrive")
    late_block = {0: 2, G - 1: 1}

    def add_block(d, more_from):
        for i in range(IR // 8):
            rr = pl.ds(16 + IR * d + 8 * i, 8)
            for j in range(NT):
                if j < LT:
                    sp = RSP[d, j, pl.ds(8 * i, 8), :]
                else:
                    sp = pltpu.roll(RX[d, 0], 128 - (16 * i + 8), 1)
                if i == 0 and more_from is not None:
                    sp = sp + below_block(more_from, j)
                Z[j, rr, :] = Z[j, rr, :] + WID[j, rr, :] * sp

    def below_block(d, j):
        return jnp.where(sub == 0, jnp.broadcast_to(RX[d, 1][j:j + 1, :], (8, 128)), 0.0)

    def add_below(d):
        rr = pl.ds(16 + IR * (d + 1), 8)
        for j in range(NT):
            Z[j, rr, :] = Z[j, rr, :] + WID[j, rr, :] * below_block(d, j)

    for own, last_in in late_block.items():
        @pl.when(g == own)
        def _(own=own, last_in=last_in):
            rest = [d for d in range(G) if d != last_in]
            for d in rest:
                if d != own:
                    wait_rows(rs.at[R_RS + d], LT * IR + 16)
            for d in rest:
                add_block(d, d - 1 if d - 1 in rest else None)
            if own == 0:
                add_below(G - 1)

    @pl.when(jnp.logical_not(is_owner))
    def _():
        wait_rows(rs.at[R_RH], LT * 8 + 16)

        @pl.when(g == 1)
        def _():
            rr = pl.ds(16, 8)
            for j in range(NT):
                more = jnp.broadcast_to(RXH[1][j:j + 1, :], (8, 128))
                Z[j, rr, :] = Z[j, rr, :] + WID[j, rr, :] * jnp.where(sub == 0, more, 0.0)
        for at, row, i in ((1, 8, 7), (2, OR + 16, 0)):
            @pl.when(g == at)
            def _(row=row, i=i):
                rr = pl.ds(row, 8)
                for j in range(NT):
                    sp = RH[j] if j < LT else pltpu.roll(RXH[0], 128 - (16 * i + 8), 1)
                    Z[j, rr, :] = Z[j, rr, :] + WID[j, rr, :] * sp

    phase("krylov")
    def krylov0(r, acc):
        rr = pl.ds(r, 8)
        for j in range(NT):
            z = Z[j, rr, :]
            Y0[j, rr, :] = D[j, rr, :] * z
            if j < LT and acc is not None:
                acc = (acc[0] + DG[j, rr, :] * z * z,)
        return acc

    def krylov(src, dst, vec, r, acc):
        rr = pl.ds(r, 8)
        y, n = shifted_sum(src, r)
        for j in range(NT):
            v = H[j, rr, :] * n[j]
            out = D[j, rr, :] * v
            vec[j, rr, :] = v
            dst[j, rr, :] = out
            if j < LT and acc is not None:
                acc = (acc[0] + y[j] * n[j], acc[1] + out * n[j])
        return acc

    def krylov3(r, acc):
        if acc is None:
            return None
        y, n = shifted_sum(Y2, r)
        for j in range(LT):
            acc = (acc[0] + y[j] * n[j],)
        return acc

    sweeps = (
        (krylov0, (0,)),
        (functools.partial(krylov, Y0, Y1, V1), (1, 2)),
        (functools.partial(krylov, Y1, Y2, V2), (3, 4)),
        (krylov3, (5,)),
    )
    start = jnp.where(g == 0, 13, jnp.where(g == G - 1, 5, 17))
    end = jnp.where(g == 0, 29, jnp.where(g == G - 1, 21, 17))

    def row_of(group):
        return pl.multiple_of(8 * group + 8, 8)

    for body, into in sweeps:
        body(8, None)
        body(OR + 16, None)
        body(row_of(start), None)
        body(row_of(end - 1), None)

        def four(i, acc, first, body=body):
            for m in range(4):
                acc = body(row_of(first + 4 * i + m), acc)
            return acc
        acc = (zero,) * len(into)
        acc = lax.fori_loop(0, (start - 1) // 4, functools.partial(four, first=1), acc)
        acc = lax.fori_loop(0, (33 - end) // 4, functools.partial(four, first=end), acc)
        for k, m in zip(into, acc):
            MOM[k] = m

    phase("late")
    for own, last_in in late_block.items():
        @pl.when(g == own)
        def _(own=own, last_in=last_in):
            wait_rows(rs.at[R_RS + last_in], LT * IR + 16)
            add_block(last_in, last_in - 1)
            add_below(last_in)

    phase("krylate")

    @pl.when(is_owner)
    def _():
        for body, into in sweeps:
            acc = (zero,) * len(into)
            for m in range(16):
                acc = body(row_of(start + m), acc)
            for k, m in zip(into, acc):
                MOM[k] = MOM[k] + m

    moments = [MOM[k] for k in range(6)]
    phase("red1")
    tile = zero
    for k, m in enumerate(moments):
        tile = jnp.where(sub == k, jnp.sum(m, axis=0, keepdims=True), tile)
    slot1 = 2 * g + core
    L1[slot1] = tile
    for dev in peers1:
        send(L1.at[slot1], L1.at[slot1], S_1, R_1, dev)
    wait_rows(rs.at[R_1], 8 * len(peers1))
    tile = L1[0]
    for k in range(1, 8):
        tile = tile + L1[k]
    phase("red2")
    L2[mine2] = tile
    for dev in peers2:
        send(L2.at[mine2], L2.at[mine2], S_2, R_2, dev)
    wait_rows(rs.at[R_2], 8 * len(peers2))
    tile = L2[0]
    for k in range(1, M2):
        tile = tile + L2[k]
    phase("coef")
    total = jnp.sum(tile, axis=1, keepdims=True)
    mu = [total[k:k + 1, :] for k in range(6)]
    nu = [mu[k] - mu[k + 1] for k in range(5)]

    a0 = mu[0] / nu[0]
    z10, z11 = 1.0 - a0, a0
    rz1 = z11 * (z10 * mu[1] + z11 * mu[2])
    b0 = rz1 / mu[0]
    p10, p11 = z10 + b0, z11
    a1 = rz1 / (p11 * (p10 * nu[1] + p11 * nu[2]))
    z20, z21, z22 = z10 - a1 * p10, z11 - a1 * (p11 - p10), a1 * p11
    rz2 = z22 * (z20 * mu[2] + z21 * mu[3] + z22 * mu[4])
    b1 = rz2 / rz1
    p20, p21, p22 = z20 + b1 * p10, z21 + b1 * p11, z22
    a2 = rz2 / (p22 * (p20 * nu[2] + p21 * nu[3] + p22 * nu[4]))
    k0 = jnp.broadcast_to(a0 + a1 * p10 + a2 * p20, (8, 128))
    k1 = jnp.broadcast_to(a1 * p11 + a2 * p21, (8, 128))
    k2 = jnp.broadcast_to(a2 * p22, (8, 128))

    phase("finish")
    def finish(r, carry):
        rr = pl.ds(r, 8)
        for j in range(LT):
            OUT[j, pl.ds(pl.multiple_of(r - 16, 8), 8), :] = X[j, rr, :] + (
                k0 * Z[j, rr, :] + (k1 * V1[j, rr, :] + k2 * V2[j, rr, :]))
        return carry
    ocean_rows(finish, 0)
    phase("sentwait")
    for s, cond in ((S_FL, jnp.logical_and(is_owner, has_l)), (S_FR, jnp.logical_and(is_owner, has_r))):
        @pl.when(cond)
        def _(s=s):
            wait_rows(ss.at[s], G * 24)
    for s, cond in ((S_L, has_l), (S_R, has_r)):
        @pl.when(cond)
        def _(s=s):
            wait_rows(ss.at[s], 2 * 8 * 8 + 3 * 4 * 8)
    for at in range(G):
        @pl.when(g == at)
        def _(at=at):
            full = (8 * 2 + 3) * 8 * LT + 2 * 16 + 8
            if at > 0:
                less = sum(bottom_summed(c, at - 1) for c in range(2))
                wait_rows(ss.at[S_U], full - less * 2 * 8 * LT)
            if at < G - 1:
                less = sum(top_summed(c, at + 1) for c in range(2))
                wait_rows(ss.at[S_D], full - less * 2 * 8 * LT)
            if at in (0, G - 1):
                c = 0 if at == 0 else 1
                wait_rows(ss.at[S_F], 2 * LT * sum(flow_rows(c, d)[1] for d in dests[at]))
            wait_rows(ss.at[S_FW], (2 if at in (0, G - 1) else 1) * 2 * 8 * LT)
    for c in range(2):
        mine = jnp.logical_and(is_owner, c == owner_cap)

        @pl.when(jnp.logical_not(mine))
        def _(c=c):
            wait_rows(ss.at[S_RS + c], LT * IR + 16)

    @pl.when(is_owner)
    def _():
        wait_rows(ss.at[S_RH], LT * 8 + 16)
    wait_rows(ss.at[S_1], 8 * len(peers1))
    wait_rows(ss.at[S_2], 8 * len(peers2))
    for dy, dx, cond in nbrs:
        k = 3 * (1 - dy) + (1 - dx)
        @pl.when(cond)
        def _(dy=dy, dx=dx, k=k):
            dev = (g + dy, t + dx)
            for src, dst, s, r in block_pairs(dy, 1 - dx, 0 if dy < 0 else 1):
                pltpu.make_async_remote_copy(
                    src_ref=src, dst_ref=dst, send_sem=ss.at[s + k], recv_sem=rs.at[r + k],
                    device_id=dev, device_id_type=MESH).wait_send()
    phase(None)


def shards(T, *args):
    ice = (2, NT, IH, 128)
    ocean = (NT, OH, 128)
    vm = lambda *s: pltpu.VMEM(s, F32)
    scratch = [
        vm(2, *ice), vm(*ice), vm(2, *ice), vm(*ice), vm(*ice), vm(*ice),
        vm(2, 2, 8, 8, 128), vm(2, 2, 8, 8, 128), vm(2, 3, 4, 8, 128), vm(2, 3, 4, 8, 128),
        vm(2, G, 3, 8, 128), vm(2, 2, 3, 8, 128), vm(2, 2, 2, 8, 128), vm(2, 2, 2, 8, 128),
        vm(2, 8, 128), vm(2, 8, 128), vm(2, 2, OR, 128), vm(2, LT, 8, 128),
        *[vm(*ocean) for _ in range(13)],
        pltpu.VMEM((3, 2, 8, 64), jnp.int32), pltpu.VMEM((3, 32, 64), jnp.int32),
        pltpu.VMEM((2, 8, 64), jnp.int32), pltpu.VMEM((2, 3, 8, 64), jnp.int32),
        vm(2, LT, IR, 128), vm(2, 2, 8, 128),
        vm(G, LT, IR, 128), vm(G, 2, 8, 128), vm(LT, 8, 128), vm(2, 8, 128),
        vm(8, 8, 128), vm(T // 2, 8, 128), vm(6, 8, 128), vm(DUMMY, 128),
        pltpu.SemaphoreType.DMA((N_R,)), pltpu.SemaphoreType.DMA((N_S,)), pltpu.SemaphoreType.DMA((N_L,)),
    ]
    hbm = pl.BlockSpec(memory_space=pltpu.HBM)
    vmem = pl.BlockSpec(memory_space=pltpu.VMEM)
    worked = pl.pallas_call(
        functools.partial(kernel, T),
        out_shape=(vm(2, *ice), vm(3, *ice), vm(LT, OR, 128)),
        in_specs=[hbm] * 10,
        out_specs=(vmem, vmem, vmem),
        scratch_shapes=scratch,
        compiler_params=pltpu.CompilerParams(
            collective_id=0, has_side_effects=True, vmem_limit_bytes=60 * 1024 * 1024),
    )(*args)
    return pl.pallas_call(
        deliver,
        out_shape=(
            jax.ShapeDtypeStruct((OR, 128 * LT), F32),
            jax.ShapeDtypeStruct((2, 2, IR, 128 * LT), F32),
            jax.ShapeDtypeStruct((3, 2, IR, 128 * LT), F32),
        ),
        in_specs=[vmem] * 3,
        out_specs=(hbm, hbm, hbm),
        scratch_shapes=[pltpu.SemaphoreType.DMA((3, LT))],
        compiler_params=pltpu.CompilerParams(vmem_limit_bytes=1024 * 1024),
    )(*worked)


def deliver(V, S, OUT, o_ssh, o_vel, o_str, sem):
    copies = []
    for j in range(LT):
        to = pl.ds(128 * j, 128)
        copies += [
            pltpu.make_async_copy(S.at[:, :, j, pl.ds(16, IR), :], o_str.at[:, :, :, to], sem.at[0, j]),
            pltpu.make_async_copy(V.at[:, :, j, pl.ds(16, IR), :], o_vel.at[:, :, :, to], sem.at[1, j]),
            pltpu.make_async_copy(OUT.at[j], o_ssh.at[:, to], sem.at[2, j]),
        ]
    for c in copies:
        c.start()
    for c in copies:
        c.wait()


def solution(mesh):
    return jax.shard_map(
        functools.partial(shards, mesh.shape["tile"]),
        mesh=mesh,
        in_specs=(
            P("grp", "tile"),
            P("grp", "tile"),
            P("grp", "tile"),
            P(None, "grp", "tile"),
            P("grp", "tile"),
            P(None, "grp", "tile"),
            P(None, "grp", "tile"),
            P(None, None, "grp", "tile"),
            P(None, None, "grp", "tile"),
            P(None, None, "grp", "tile"),
        ),
        out_specs=(P("grp", "tile"), P(None, None, "grp", "tile"), P(None, None, "grp", "tile")),
        check_vma=False,
    )
```

```python
import functools

import jax
import jax.numpy as jnp
from jax import lax
from jax.experimental import pallas as pl
from jax.experimental.pallas import tpu as pltpu
from jax.sharding import PartitionSpec as P

BS = 8
NSUB = 8
DAMP = 0.05
RELAX = 0.2
STRENGTH = 0.5
DRAG = 1.0
STEP = 0.5
G = 4
LT = 4
NT = LT + 1
IR = 64
OR = 256
IH = IR + 40
OH = OR + 40
F32 = jnp.float32
MESH = pl.DeviceIdType.MESH
DUMMY = 4096

R_PL, R_PR, R_FU, R_FD, R_IL, R_IR, R_OL, R_OR = 41, 43, 45, 47, 4, 5, 6, 7
R_IU, R_ID, R_F = 8, 10, 12
R_OU, R_OD, R_RS, R_RH, R_1, R_2 = 14, 15, 16, 20, 21, 22
R_BI, R_BO = 23, 32
N_R = 49
S_FL, S_FR, S_L, S_R, S_U, S_D, S_F, S_RS, S_1, S_2 = 0, 1, 2, 3, 4, 5, 6, 7, 9, 10
S_RH, S_FW = 11, 30
S_BI, S_BO = 12, 21
N_S = 31
L_BLK, L_ICE, L_FL, L_OC, L_OUT, L_OUTS, L_ED = 0, 1, 2, 3, 4, 5, 6
N_L = 7


def east(tiles, lane):
    turned = [pltpu.roll(x, 127, 1) for x in tiles]
    return [jnp.where(lane == 127, turned[(j + 1) % NT], turned[j]) for j in range(NT)]


def west(tiles, lane):
    turned = [pltpu.roll(x, 1, 1) for x in tiles]
    return [jnp.where(lane == 0, turned[(j - 1) % NT], turned[j]) for j in range(NT)]


class Phases:
    def __init__(self):
        self.open = None

    def __call__(self, name):
        if self.open is not None:
            self.open.__exit__(None, None, None)
        self.open = None
        if name:
            self.open = jax.named_scope(name)
            self.open.__enter__()


def kernel(
    T,
    base, depth, ssh, cur, land, thick, iblk, ivel, istr, wind,
    V, S, OUT,
    W, TH, FL, CV, C1, C2,
    PI, LI, PC, LC, PF, LF, PH, LH, PHO, LHO, CE, FE,
    B, D, X, Z, Y0, Y1, Y2, H, WID, DG, WET, V1, V2,
    BI, BO, PB, LB, SPB, XB, RSP, RX, RH, RXH, L1, L2, MOM, DUM,
    rs, ss, ls,
):
    g = lax.axis_index("grp")
    t = lax.axis_index("tile")
    has_l, has_r, has_u, has_d = t > 0, t < T - 1, g > 0, g < G - 1
    lane = lax.broadcasted_iota(jnp.int32, (8, 128), 1)
    sub = lax.broadcasted_iota(jnp.int32, (8, 128), 0)
    zero = jnp.zeros((8, 128), F32)
    first_cap = g // 2
    owner_cap = jnp.where(g == 0, 0, 1)
    is_owner = jnp.logical_or(g == 0, g == G - 1)

    def wait_rows(sem, rows):
        pltpu.make_async_copy(DUM.at[pl.ds(0, rows)], DUM.at[pl.ds(0, rows)], sem).wait()

    def send(src, dst, s, r, dev):
        pltpu.make_async_remote_copy(
            src_ref=src, dst_ref=dst, send_sem=ss.at[s], recv_sem=rs.at[r],
            device_id=dev, device_id_type=MESH,
        ).start()

    def local(src, dst, s):
        pltpu.make_async_copy(src, dst, ls.at[s]).start()

    def cols(j):
        return pl.ds(128 * j, 128)

    nbrs = []
    for dy in (-1, 0, 1):
        for dx in (-1, 0, 1):
            if dy == 0 and dx == 0:
                continue
            cond = None
            for need, there in ((dy < 0, has_u), (dy > 0, has_d), (dx < 0, has_l), (dx > 0, has_r)):
                if need:
                    cond = there if cond is None else jnp.logical_and(cond, there)
            nbrs.append((dy, dx, cond))

    def top_summed(c, d):
        return (c == 0 and d in (1, 2)) or (c == 1 and d == 1)

    def bottom_summed(c, d):
        return (c == 1 and d in (1, 2)) or (c == 0 and d == 2)

    def top_is_summed(c):
        return jnp.logical_or(g == 1, jnp.logical_and(g == 2, c == 0))

    def bottom_is_summed(c):
        return jnp.logical_or(g == 2, jnp.logical_and(g == 1, c == 1))

    phase = Phases()
    phase("signal")
    barrier = pltpu.get_barrier_semaphore()
    core = lax.rem(t, 2)
    M2 = T // 2
    mine2 = t // 2
    peers1 = []
    for dg in range(G):
        for dc in range(2):
            if dg or dc:
                peers1.append((lax.rem(g + dg, G), t - core + lax.rem(core + dc, 2)))
    peers2 = [(g, 2 * lax.rem(mine2 + k, M2) + core) for k in range(1, M2)]
    for dg in range(G):
        for dx, cond in ((-1, has_l), (0, None), (1, has_r)):
            dev = (lax.rem(g + dg, G), t + dx)
            if cond is not None:
                @pl.when(cond)
                def _(dev=dev):
                    pl.semaphore_signal(barrier, inc=1, device_id=dev, device_id_type=MESH)
            elif dg:
                pl.semaphore_signal(barrier, inc=1, device_id=dev, device_id_type=MESH)
    for dev in peers2:
        pl.semaphore_signal(barrier, inc=1, device_id=dev, device_id_type=MESH)

    phase("loads")
    local(iblk, BI.at[1], L_BLK)
    local(land, BO.at[1], L_BLK)
    for j in range(LT):
        local(ivel.at[:, :, :, cols(j)], V.at[:, :, j, pl.ds(16, IR), :], L_ICE)
        local(istr.at[:, :, :, cols(j)], S.at[:, :, j, pl.ds(16, IR), :], L_ICE)
        local(wind.at[:, :, :, cols(j)], W.at[:, :, j, pl.ds(16, IR), :], L_ICE)
        local(thick.at[:, :, cols(j)], TH.at[:, j, pl.ds(16, IR), :], L_ICE)
        local(base.at[:, cols(j)], B.at[j, pl.ds(16, OR), :], L_OC)
        local(depth.at[:, cols(j)], D.at[j, pl.ds(16, OR), :], L_OC)
        local(ssh.at[:, cols(j)], X.at[j, pl.ds(16, OR), :], L_OC)

    @pl.when(is_owner)
    def _():
        local(cur.at[:, :, cols(0)], CE.at[0], L_ED)
        local(cur.at[:, :, cols(LT - 1)], CE.at[1], L_ED)

    pltpu.make_async_copy(iblk, BI.at[1], ls.at[L_BLK]).wait()
    pltpu.make_async_copy(land, BO.at[1], ls.at[L_BLK]).wait()
    line = lax.broadcasted_iota(jnp.int32, (8, 64), 0)
    for e, i, o in ((0, 0, 0), (1, 7, 7)):
        ends = [BI[1, 0][i:i + 1], BI[1, 1][i:i + 1], BO[1, 24 * e:24 * e + 8][o:o + 1]]
        ends = [jnp.broadcast_to(x, (8, 64)) for x in ends]
        PB[e] = jnp.where(line == 0, ends[0], jnp.where(line == 1, ends[1], ends[2]))

    phase("barrier")
    wide = 1 + jnp.minimum(t, 1) + jnp.minimum(T - 1 - t, 1)
    pl.semaphore_wait(barrier, G * wide - 1 + len(peers2))

    phase("sends")
    left, right, up, down = (g, t - 1), (g, t + 1), (g - 1, t), (g + 1, t)
    for dy, dx, cond in nbrs:
        k = 3 * (1 - dy) + (1 - dx)
        @pl.when(cond)
        def _(dy=dy, dx=dx, k=k):
            dev = (g + dy, t + dx)
            if dy == 0:
                send(iblk, BI.at[1 - dx], S_BI + k, R_BI + k, dev)
                send(land, BO.at[1 - dx], S_BO + k, R_BO + k, dev)
            else:
                e = 0 if dy < 0 else 1
                send(PB.at[e], LB.at[1 - e, 1 - dx], S_BI + k, R_BI + k, dev)

    def flow_rows(c, d):
        lo = IR * d if d == 0 or top_summed(c, d) else IR * d - 8
        hi = IR * d + IR if d == G - 1 or bottom_summed(c, d) else IR * d + IR + 8
        return lo, hi - lo, 16 + lo - IR * d

    dests = {0: (1, 3, 2), G - 1: (2, 0, 1)}

    def send_flow(c, d):
        lo, n, at = flow_rows(c, d)
        for j in range(LT):
            send(cur.at[:, pl.ds(lo, n), cols(j)], FL.at[:, c, j, pl.ds(at, n), :],
                 S_F, R_F + c, (d, t))

    def halo_ice(dev, c, src, dst, s, r):
        there = dev[0]
        if s == S_D:
            summed = jnp.logical_or(there == 1, jnp.logical_and(there == 2, c == 0))
        else:
            summed = jnp.logical_or(there == 2, jnp.logical_and(there == 1, c == 1))

        @pl.when(jnp.logical_not(summed))
        def _():
            for j in range(LT):
                send(wind.at[:, c, pl.ds(src, 8), cols(j)], W.at[:, c, j, pl.ds(dst, 8), :], s, r, dev)
        for j in range(LT):
            send(ivel.at[:, c, pl.ds(src, 8), cols(j)], V.at[:, c, j, pl.ds(dst, 8), :], s, r, dev)
            send(istr.at[:, c, pl.ds(src, 8), cols(j)], S.at[:, c, j, pl.ds(dst, 8), :], s, r, dev)
            send(thick.at[c, pl.ds(src, 8), cols(j)], TH.at[c, j, pl.ds(dst, 8), :], s, r, dev)

    def halo_turn(turn):
        for dev, cond, src, dst, s, r in (
            (up, has_u, 0, IR + 16, S_U, R_ID),
            (down, has_d, IR - 8, 8, S_D, R_IU),
        ):
            @pl.when(cond)
            def _(dev=dev, src=src, dst=dst, s=s, r=r):
                there = dev[0] // 2
                c = there if turn == 0 else 1 - there
                halo_ice(dev, c, src, dst, s, r + c)

    for own, c in ((0, 0), (G - 1, 1)):
        @pl.when(g == own)
        def _(own=own, c=c):
            send_flow(c, dests[own][0])
            send_flow(c, dests[own][1])
            lo, n, at = flow_rows(c, own)
            for j in range(LT):
                local(cur.at[:, pl.ds(lo, n), cols(j)], FL.at[:, c, j, pl.ds(at, n), :], L_FL)
    halo_turn(0)

    phase("zeros")
    for cond, row, orow, by in ((g == 0, 8, 8, 0), (g == G - 1, IR + 16, OR + 16, 1)):
        @pl.when(cond)
        def _(row=row, orow=orow, by=by):
            for c in range(2):
                for j in range(NT):
                    for k in range(3):
                        S[k, c, j, pl.ds(row, 8), :] = zero
                    for k in range(2):
                        V[k, c, j, pl.ds(row, 8), :] = zero
                        W[k, c, j, pl.ds(row, 8), :] = zero
                        FL[k, c, j, pl.ds(row, 8), :] = zero
                    TH[c, j, pl.ds(row, 8), :] = zero
            for j in range(NT):
                B[j, pl.ds(orow, 8), :] = zero
                D[j, pl.ds(orow, 8), :] = zero
                X[j, pl.ds(orow, 8), :] = zero
            for x in range(3):
                LB[by, x] = jnp.zeros((8, 64), jnp.int32)

    for d in (1, 2):
        @pl.when(g == d)
        def _(d=d):
            for c in range(2):
                for here, row in ((top_summed(c, d), 8), (bottom_summed(c, d), IR + 16)):
                    if here:
                        for k in range(2):
                            for j in range(LT):
                                FL[k, c, j, pl.ds(row, 8), :] = zero

    for cond, side, bx in ((t == 0, 0, 0), (t == T - 1, 1, 2)):
        @pl.when(cond)
        def _(side=side, bx=bx):
            for c in range(2):
                for k in range(8):
                    LI[side, c, k] = zero
                for v in range(2):
                    LF[side, c, v] = zero
            for k in range(3):
                for v in range(4):
                    LC[side, k, v] = zero
            for y in range(2):
                LB[y, bx] = jnp.zeros((8, 64), jnp.int32)
                BI[bx, y] = jnp.zeros((8, 64), jnp.int32)
            BO[bx] = jnp.zeros((32, 64), jnp.int32)

    phase("pack")
    slot_of = lane // 16

    def put(pack, e, at, x):
        moved = pltpu.roll(x, 16 * at, 1) if at else x
        return jnp.where(slot_of == (at - e) % 8, moved, pack)

    def take(from_right, from_left, at):
        both = jnp.where(slot_of == at, from_right, from_left)
        return pltpu.roll(both, 128 - 16 * at, 1) if at else both

    thin_of, thin_before = lane // 12, lax.rem(lane + 12, 128) // 12

    def put_thin(pack, e, at, x):
        moved = pltpu.roll(x, 12 * at, 1) if at else x
        return jnp.where((thin_before if e else thin_of) == at, moved, pack)

    def take_thin(from_right, from_left, at):
        both = jnp.where(thin_of == at, from_right, from_left)
        return pltpu.roll(both, 128 - 12 * at, 1) if at else both

    wait_rows(ls.at[L_ICE], 8 * 2 * IR * LT)

    def ice_get(k, c, j, r):
        if k < 2:
            return V[k, c, j, pl.ds(r, 8), :]
        if k < 5:
            return S[k - 2, c, j, pl.ds(r, 8), :]
        return W[k - 5, c, j, pl.ds(r, 8), :] if k < 7 else TH[c, j, pl.ds(r, 8), :]

    def ice_set(k, c, j, r, x):
        if k < 2:
            V[k, c, j, pl.ds(r, 8), :] = x
        elif k < 5:
            S[k - 2, c, j, pl.ds(r, 8), :] = x
        elif k < 7:
            W[k - 5, c, j, pl.ds(r, 8), :] = x
        else:
            TH[c, j, pl.ds(r, 8), :] = x

    for e, j in ((0, 0), (1, LT - 1)):
        for c in range(2):
            for k in range(8):
                pack = zero
                for i in range(IR // 8):
                    pack = put(pack, e, i, ice_get(k, c, j, 16 + 8 * i))
                PI[e, c, k] = pack

    for own in (0, G - 1):
        @pl.when(g == own)
        def _(own=own):
            wait_rows(ls.at[L_ED], 2 * 2 * OR)
            for e in range(2):
                for d in range(G):
                    for k in range(2):
                        pack = zero
                        for s in range(10):
                            q = 8 * d - 1 + s
                            if 0 <= q < OR // 8:
                                pack = put_thin(pack, e, s, CE[e, k, pl.ds(8 * q, 8), :])
                        PF[e, d, k] = pack

    wait_rows(ls.at[L_OC], 3 * OR * LT)
    for e, j in ((0, 0), (1, LT - 1)):
        for k, ref in enumerate((B, D, X)):
            for v in range(4):
                pack = zero
                for i in range(8):
                    pack = put(pack, e, i, ref[j, pl.ds(16 + 64 * v + 8 * i, 8), :])
                PC[e, k, v] = pack

    for e, dev, cond, s, ri, ro in ((0, left, has_l, S_L, R_IR, R_OR), (1, right, has_r, S_R, R_IL, R_OL)):
        @pl.when(cond)
        def _(e=e, dev=dev, s=s, ri=ri, ro=ro):
            send(PI.at[e], LI.at[1 - e], s, ri, dev)
            send(PC.at[e], LC.at[1 - e], s, ro, dev)

    for own, c in ((0, 0), (G - 1, 1)):
        @pl.when(g == own)
        def _(own=own, c=c):
            for e, dx, cond, s, r in ((0, -1, has_l, S_FL, R_PR), (1, 1, has_r, S_FR, R_PL)):
                @pl.when(cond)
                def _(e=e, dx=dx, s=s, r=r):
                    for dg in range(G):
                        d = dg if own == 0 else G - 1 - dg
                        dev = (g + dg if own == 0 else g - dg, t + dx)
                        send(PF.at[e, d], LF.at[1 - e, c], s, r + c, dev)

    phase("mergeice")
    @pl.when(has_l)
    def _():
        wait_rows(rs.at[R_IL], 2 * 8 * 8)

    @pl.when(has_r)
    def _():
        wait_rows(rs.at[R_IR], 2 * 8 * 8)

    quarter = lane // 32
    for c in range(2):
        ends = [[zero, zero], [zero, zero]]
        for k in range(8):
            for i in range(IR // 8):
                x = take(LI[1, c, k], LI[0, c, k], i)
                ice_set(k, c, LT, 16 + 8 * i, x)
                for e, at in ((0, 0), (1, IR // 8 - 1)):
                    if i == at:
                        moved = pltpu.roll(x, (32 * (k % 4) + 16) % 128, 1)
                        ends[e][k // 4] = jnp.where(quarter == k % 4, moved, ends[e][k // 4])
        for e in range(2):
            for v in range(2):
                PH[e, c, v] = ends[e][v]
    for e, dev, cond, s, r in ((0, up, has_u, S_U, R_ID), (1, down, has_d, S_D, R_IU)):
        @pl.when(cond)
        def _(e=e, dev=dev, s=s, r=r):
            for c in range(2):
                send(PH.at[e, c], LH.at[1 - e, c], s, r + c, dev)

    for own, c, row, to, dev, r in (
        (0, 0, IR + 8, 8, down, R_FU), (G - 1, 1, 16, IR + 16, up, R_FD + 1)):
        @pl.when(g == own)
        def _(c=c, row=row, to=to, dev=dev, r=r):
            wait_rows(ls.at[L_FL], 2 * (IR + 8) * LT)
            for k in range(2):
                for j in range(LT):
                    FE[k, j] = W[k, c, j, pl.ds(row, 8), :] + FL[k, c, j, pl.ds(row, 8), :] * DRAG
            for j in range(LT):
                send(FE.at[:, j], W.at[:, c, j, pl.ds(to, 8), :], S_FW, r, dev)

    for own, c in ((0, 0), (G - 1, 1)):
        @pl.when(g == own)
        def _(own=own, c=c):
            send_flow(c, dests[own][2])
    halo_turn(1)
    def ocean_ends():
        for dev, cond, at, to, s, r in (
            (up, has_u, 0, OR + 16, S_U, R_OD),
            (down, has_d, OR - 8, 8, S_D, R_OU),
        ):
            @pl.when(cond)
            def _(dev=dev, at=at, to=to, s=s, r=r):
                for j in range(LT):
                    send(base.at[pl.ds(at, 8), cols(j)], B.at[j, pl.ds(to, 8), :], s, r, dev)
                    send(depth.at[pl.ds(at, 8), cols(j)], D.at[j, pl.ds(to, 8), :], s, r, dev)
                    send(ssh.at[pl.ds(at, 8), cols(j)], X.at[j, pl.ds(to, 8), :], s, r, dev)

    phase("mergeoc")
    @pl.when(has_l)
    def _():
        wait_rows(rs.at[R_OL], 3 * 4 * 8)

    @pl.when(has_r)
    def _():
        wait_rows(rs.at[R_OR], 3 * 4 * 8)

    ends = [zero, zero]
    for k, ref in enumerate((B, D, X)):
        for q in range(OR // 8):
            x = take(LC[1, k, q // 8], LC[0, k, q // 8], q % 8)
            ref[LT, pl.ds(16 + 8 * q, 8), :] = x
            for e, at in ((0, 0), (1, OR // 8 - 1)):
                if q == at:
                    moved = pltpu.roll(x, 32 * k + 16, 1)
                    ends[e] = jnp.where(quarter == k, moved, ends[e])
    for e, dev, cond, s, r in ((0, up, has_u, S_U, R_OD), (1, down, has_d, S_D, R_OU)):
        PHO[e] = ends[e]
        @pl.when(cond)
        def _(e=e, dev=dev, s=s, r=r):
            send(PHO.at[e], LHO.at[1 - e], s, r, dev)

    phase("masks")
    def block_pairs(dy, x, e):
        if dy == 0:
            return [(iblk, BI.at[x], S_BI, R_BI), (land, BO.at[x], S_BO, R_BO)]
        return [(PB.at[e], LB.at[1 - e, x], S_BI, R_BI)]

    for dy, dx, cond in nbrs:
        k = 3 * (1 + dy) + (1 + dx)
        @pl.when(cond)
        def _(dy=dy, dx=dx, k=k):
            dev = (g + dy, t + dx)
            pairs = block_pairs(dy, 1 + dx, 1 if dy < 0 else 0)
            for src, dst, s, r in pairs:
                pltpu.make_async_remote_copy(
                    src_ref=src, dst_ref=dst, send_sem=ss.at[s + k], recv_sem=rs.at[r + k],
                    device_id=dev, device_id_type=MESH).wait_recv()

    def selection(width, first, start):
        block = lax.broadcasted_iota(jnp.int32, (64, width), 0)
        at = lax.broadcasted_iota(jnp.int32, (64, width), 1)
        hit = block == at // BS + first
        if start is not None:
            hit = jnp.logical_and(hit, (at < 64) if start == 0 else (at >= 64))
        return hit.astype(F32)

    sel_c = selection(128 * LT, 0, None)
    sel_r = selection(128, 0, 0)
    sel_l = selection(128, 48, 1)

    def spread_rows(refs):
        lft, mid, rgt = (ref.astype(F32) for ref in refs)
        wide = jnp.dot(mid, sel_c, preferred_element_type=F32)
        last = jnp.dot(rgt, sel_r, preferred_element_type=F32) + jnp.dot(
            lft, sel_l, preferred_element_type=F32)
        return wide, last

    def paint(ref, row, parts, b):
        wide, last = parts
        for j in range(LT):
            ref[j, pl.ds(row, 8), :] = jnp.broadcast_to(wide[b:b + 1, 128 * j:128 * j + 128], (8, 128))
        ref[LT, pl.ds(row, 8), :] = jnp.broadcast_to(last[b:b + 1, :], (8, 128))

    ends = [spread_rows([LB[y, x] for x in range(3)]) for y in range(2)]
    for c in range(2):
        cov = CV.at[c]
        paint(cov, 8, ends[0], c)
        mid = spread_rows([BI[x, c] for x in range(3)])
        for b in range(8):
            paint(cov, 16 + 8 * b, mid, b)
        paint(cov, IR + 16, ends[1], c)
    paint(WET, 8, ends[0], 2)
    for q in range(4):
        mid = spread_rows([BO[x, 8 * q:8 * q + 8] for x in range(3)])
        for b in range(8):
            paint(WET, 16 + 64 * q + 8 * b, mid, b)
    paint(WET, OR + 16, ends[1], 2)

    def static(c, r):
        rr = pl.ds(r, 8)
        for j in range(NT):
            cov = CV[c, j, rr, :]
            thc = TH[c, j, rr, :] * cov
            scale = cov / (thc + (1.0 + STEP * DRAG))
            C1[c, j, rr, :] = scale * (thc + 1.0)
            C2[c, j, rr, :] = scale * STEP
            TH[c, j, rr, :] = thc * (RELAX * STRENGTH / (1.0 + RELAX))

    for c in range(2):
        def own_static(i, carry, c=c):
            static(c, pl.multiple_of(8 * i + 16, 8))
            return carry
        lax.fori_loop(0, IR // 8, own_static, 0)

    def pass_on(c, row, to, dev, r):
        for j in range(LT):
            send(W.at[:, c, j, pl.ds(row, 8), :], W.at[:, c, j, pl.ds(to, 8), :], S_FW, r + c, dev)

    def cap(c, turn):
        phase = Phases()
        phase("capwait")

        for e, cond, r, row, rf, summed in (
            (0, has_u, R_IU, 8, R_FU, top_is_summed(c)),
            (1, has_d, R_ID, IR + 16, R_FD, bottom_is_summed(c)),
        ):
            @pl.when(cond)
            def _(e=e, r=r, row=row, rf=rf, summed=summed):
                @pl.when(summed)
                def _():
                    wait_rows(rs.at[rf + c], 2 * 8 * LT)
                    wait_rows(rs.at[r + c], 6 * 8 * LT + 16)

                @pl.when(jnp.logical_not(summed))
                def _():
                    wait_rows(rs.at[r + c], 8 * 8 * LT + 16)
                for k in range(8):
                    x = pltpu.roll(LH[e, c, k // 4], (128 - 32 * (k % 4) - 16) % 128, 1)
                    ice_set(k, c, LT, row, x)

        @pl.when(has_l)
        def _():
            wait_rows(rs.at[R_PL + c], 16)

        @pl.when(has_r)
        def _():
            wait_rows(rs.at[R_PR + c], 16)

        for k in range(2):
            for s in range(10):
                FL[k, c, LT, pl.ds(8 + 8 * s, 8), :] = take_thin(LF[1, c, k], LF[0, c, k], s)

        mine = jnp.logical_and(is_owner, c == owner_cap)
        at_end = jnp.logical_or(jnp.logical_and(c == 0, g == G - 1), jnp.logical_and(c == 1, g == 0))

        @pl.when(jnp.logical_not(mine))
        def _():
            both = jnp.logical_and(top_is_summed(c), bottom_is_summed(c))

            @pl.when(both)
            def _():
                wait_rows(rs.at[R_F + c], 2 * IR * LT)

            @pl.when(jnp.logical_not(both))
            def _():
                wait_rows(rs.at[R_F + c], 2 * (IR + 8) * LT)

        phase("prepare")
        static(c, 8)
        static(c, IR + 16)

        def prepare(i, carry):
            r = pl.ds(pl.multiple_of(8 * i + 8, 8), 8)
            for j in range(NT):
                for k in range(2):
                    W[k, c, j, r, :] = W[k, c, j, r, :] + FL[k, c, j, r, :] * DRAG
            return carry
        lax.fori_loop(0, IR // 8 + 2, prepare, 0)

        @pl.when(jnp.logical_and(c == 0, g == 1))
        def _():
            pass_on(0, IR + 8, 8, down, R_FU)

        @pl.when(jnp.logical_and(c == 0, g == G - 1))
        def _():
            pass_on(0, 16, IR + 16, up, R_FD)

        @pl.when(jnp.logical_and(c == 1, g == 0))
        def _():
            pass_on(1, IR + 8, 8, down, R_FU)

        @pl.when(jnp.logical_and(c == 1, g == 2))
        def _():
            pass_on(1, 16, IR + 16, up, R_FD)

        phase("subcycles")
        @pl.when(turn == 1)
        def _():
            ocean_ends()

        keep = 1.0 / (1.0 + RELAX)

        def group(r):
            rr = pl.ds(r, 8)
            u = [V[0, c, j, rr, :] for j in range(NT)]
            v = [V[1, c, j, rr, :] for j in range(NT)]
            ue, ve = east(u, lane), east(v, lane)
            s0, s1, s2 = [], [], []
            for j in range(NT):
                dux = V[0, c, j, pl.ds(r + 1, 8), :] - u[j]
                dvx = V[1, c, j, pl.ds(r + 1, 8), :] - v[j]
                duy, dvy = ue[j] - u[j], ve[j] - v[j]
                ed, et, es = dux + dvy, dux - dvy, duy + dvx
                inv = lax.rsqrt(ed * ed + et * et + es * es + 1.0)
                a = TH[c, j, rr, :]
                ai = a * inv
                s0.append(S[0, c, j, rr, :] * keep + (ed * ai - a))
                s1.append(S[1, c, j, rr, :] * keep + et * ai)
                s2.append(S[2, c, j, rr, :] * keep + es * ai)
                S[0, c, j, rr, :] = s0[j]
                S[1, c, j, rr, :] = s1[j]
                S[2, c, j, rr, :] = s2[j]

        def push(r):
            rr, above = pl.ds(r, 8), pl.ds(r - 1, 8)
            s0 = [S[0, c, j, rr, :] for j in range(NT)]
            s1 = [S[1, c, j, rr, :] for j in range(NT)]
            s2 = [S[2, c, j, rr, :] for j in range(NT)]
            dif = [s0[j] - s1[j] for j in range(NT)]
            dw, sw = west(dif, lane), west(s2, lane)
            for j in range(NT):
                tot_up = S[0, c, j, above, :] + S[1, c, j, above, :]
                f0 = 0.5 * ((s0[j] + s1[j]) - tot_up) + (s2[j] - sw[j])
                f1 = 0.5 * (dif[j] - dw[j]) + (s2[j] - S[2, c, j, above, :])
                c1, c2 = C1[c, j, rr, :], C2[c, j, rr, :]
                V[0, c, j, rr, :] = c1 * V[0, c, j, rr, :] + c2 * (f0 + W[0, c, j, rr, :])
                V[1, c, j, rr, :] = c1 * V[1, c, j, rr, :] + c2 * (f1 + W[1, c, j, rr, :])

        def subcycle(n, carry):
            for i in range(IR // 8 + 2):
                group(8 + 8 * i)
            for i in range(IR // 8 + 2):
                push(8 + 8 * i)
            return carry
        lax.fori_loop(0, NSUB, subcycle, 0)

        phase("diverge")
        prev = [zero] * NT
        pack = zero
        for i in range(IR // 8):
            rr = pl.ds(16 + 8 * i, 8)
            p0, p1 = [], []
            for j in range(NT):
                cov = CV[c, j, rr, :] * DRAG
                p0.append(cov * (V[0, c, j, rr, :] - FL[0, c, j, rr, :]))
                p1.append(cov * (V[1, c, j, rr, :] - FL[1, c, j, rr, :]))
            pw = west(p1, lane)
            for j in range(NT):
                turned = pltpu.roll(p0[j], 1, 0)
                above = jnp.where(sub == 0, prev[j], turned)
                prev[j] = turned
                sp = (p0[j] - above) + (p1[j] - pw[j])
                if j < LT:
                    SPB[c, j, pl.ds(8 * i, 8), :] = sp
                else:
                    pack = jnp.where(lane // 16 == i, pltpu.roll(sp, 16 * i + 8, 1), pack)
        XB[c, 0] = pack
        extra = zero
        for j in range(NT):
            extra = jnp.where(sub == j, -jnp.broadcast_to(prev[j][0:1, :], (8, 128)), extra)
        XB[c, 1] = extra

        @pl.when(mine)
        def _():
            for j in range(LT):
                for i in range(IR // 8):
                    RSP[g, j, pl.ds(8 * i, 8), :] = SPB[c, j, pl.ds(8 * i, 8), :]
            RX[g, 0] = XB[c, 0]
            RX[g, 1] = XB[c, 1]

        @pl.when(jnp.logical_not(mine))
        def _():
            dev = (c * (G - 1), t)
            send(SPB.at[c], RSP.at[g], S_RS + c, R_RS + g, dev)
            send(XB.at[c], RX.at[g], S_RS + c, R_RS + g, dev)

        @pl.when(at_end)
        def _():
            at = jnp.where(c == 0, IR - 8, 0)
            dev = (1 + c, t)
            send(SPB.at[c, :, pl.ds(pl.multiple_of(at, 8), 8), :], RH, S_RH, R_RH, dev)
            send(XB.at[c], RXH, S_RH, R_RH, dev)
        phase(None)

    def caps(turn, carry):
        cap(jnp.where(turn == 0, first_cap, 1 - first_cap), turn)
        return carry

    def ocean_rows(body, carry, unroll=4):
        def step(i, cc):
            for m in range(unroll):
                cc = body(pl.multiple_of(8 * (unroll * i + m) + 16, 8), cc)
            return cc
        return lax.fori_loop(0, OR // 8 // unroll, step, carry)

    def shifted_sum(ref, r):
        rr = pl.ds(r, 8)
        mid = [ref[j, rr, :] for j in range(NT)]
        e, w = east(mid, lane), west(mid, lane)
        return mid, [
            (ref[j, pl.ds(r + 1, 8), :] + ref[j, pl.ds(r - 1, 8), :]) + (e[j] + w[j])
            for j in range(NT)
        ]

    def ocean_prepare():
        phase = Phases()
        phase("oceanwait")

        for e, cond, r, row in ((0, has_u, R_OU, 8), (1, has_d, R_OD, OR + 16)):
            @pl.when(cond)
            def _(e=e, r=r, row=row):
                wait_rows(rs.at[r], 24 * LT + 8)
                for k, ref in enumerate((B, D, X)):
                    ref[LT, pl.ds(row, 8), :] = pltpu.roll(LHO[e], 128 - 32 * k - 16, 1)

        phase("oceanprep")
        def first(r, carry):
            rr = pl.ds(r, 8)
            for j in range(NT):
                gg = D[j, rr, :] * WET[j, rr, :]
                D[j, rr, :] = gg
                Y0[j, rr, :] = gg * X[j, rr, :]
            return carry

        def second(r, carry):
            rr = pl.ds(r, 8)
            gs, gn = shifted_sum(D, r)
            _, xn = shifted_sum(Y0, r)
            for j in range(NT):
                diag = gs[j] * gn[j] + DAMP
                inv = 1.0 / diag
                wid = WET[j, rr, :] * inv
                h = gs[j] * inv
                DG[j, rr, :] = diag
                WID[j, rr, :] = wid
                H[j, rr, :] = h
                Z[j, rr, :] = wid * B[j, rr, :] + h * xn[j] - X[j, rr, :]
            return carry
        for body in (first, second):
            body(8, 0)
            ocean_rows(body, 0)
            body(OR + 16, 0)
        phase(None)

    lax.fori_loop(0, 2, caps, 0)
    ocean_prepare()

    phase("arrive")
    late_block = {0: 2, G - 1: 1}

    def add_block(d, more_from):
        for i in range(IR // 8):
            rr = pl.ds(16 + IR * d + 8 * i, 8)
            for j in range(NT):
                if j < LT:
                    sp = RSP[d, j, pl.ds(8 * i, 8), :]
                else:
                    sp = pltpu.roll(RX[d, 0], 128 - (16 * i + 8), 1)
                if i == 0 and more_from is not None:
                    sp = sp + below_block(more_from, j)
                Z[j, rr, :] = Z[j, rr, :] + WID[j, rr, :] * sp

    def below_block(d, j):
        return jnp.where(sub == 0, jnp.broadcast_to(RX[d, 1][j:j + 1, :], (8, 128)), 0.0)

    def add_below(d):
        rr = pl.ds(16 + IR * (d + 1), 8)
        for j in range(NT):
            Z[j, rr, :] = Z[j, rr, :] + WID[j, rr, :] * below_block(d, j)

    for own, last_in in late_block.items():
        @pl.when(g == own)
        def _(own=own, last_in=last_in):
            rest = [d for d in range(G) if d != last_in]
            for d in rest:
                if d != own:
                    wait_rows(rs.at[R_RS + d], LT * IR + 16)
            for d in rest:
                add_block(d, d - 1 if d - 1 in rest else None)
            if own == 0:
                add_below(G - 1)

    @pl.when(jnp.logical_not(is_owner))
    def _():
        wait_rows(rs.at[R_RH], LT * 8 + 16)

        @pl.when(g == 1)
        def _():
            rr = pl.ds(16, 8)
            for j in range(NT):
                more = jnp.broadcast_to(RXH[1][j:j + 1, :], (8, 128))
                Z[j, rr, :] = Z[j, rr, :] + WID[j, rr, :] * jnp.where(sub == 0, more, 0.0)
        for at, row, i in ((1, 8, 7), (2, OR + 16, 0)):
            @pl.when(g == at)
            def _(row=row, i=i):
                rr = pl.ds(row, 8)
                for j in range(NT):
                    sp = RH[j] if j < LT else pltpu.roll(RXH[0], 128 - (16 * i + 8), 1)
                    Z[j, rr, :] = Z[j, rr, :] + WID[j, rr, :] * sp

    phase("krylov")
    def krylov0(r, acc):
        rr = pl.ds(r, 8)
        for j in range(NT):
            z = Z[j, rr, :]
            Y0[j, rr, :] = D[j, rr, :] * z
            if j < LT and acc is not None:
                acc = (acc[0] + DG[j, rr, :] * z * z,)
        return acc

    def krylov(src, dst, vec, r, acc):
        rr = pl.ds(r, 8)
        y, n = shifted_sum(src, r)
        for j in range(NT):
            v = H[j, rr, :] * n[j]
            out = D[j, rr, :] * v
            vec[j, rr, :] = v
            dst[j, rr, :] = out
            if j < LT and acc is not None:
                acc = (acc[0] + y[j] * n[j], acc[1] + out * n[j])
        return acc

    def krylov3(r, acc):
        if acc is None:
            return None
        y, n = shifted_sum(Y2, r)
        for j in range(LT):
            acc = (acc[0] + y[j] * n[j],)
        return acc

    sweeps = (
        (krylov0, (0,)),
        (functools.partial(krylov, Y0, Y1, V1), (1, 2)),
        (functools.partial(krylov, Y1, Y2, V2), (3, 4)),
        (krylov3, (5,)),
    )
    start = jnp.where(g == 0, 13, jnp.where(g == G - 1, 5, 17))
    end = jnp.where(g == 0, 29, jnp.where(g == G - 1, 21, 17))

    def row_of(group):
        return pl.multiple_of(8 * group + 8, 8)

    for body, into in sweeps:
        body(8, None)
        body(OR + 16, None)
        body(row_of(start), None)
        body(row_of(end - 1), None)

        def some(i, acc, first, count, body=body):
            for m in range(count):
                acc = body(row_of(first + count * i + m), acc)
            return acc

        @pl.when(is_owner)
        def _(some=some, into=into):
            acc = (zero,) * len(into)
            acc = lax.fori_loop(0, (start - 1) // 4, functools.partial(some, first=1, count=4), acc)
            acc = lax.fori_loop(0, (33 - end) // 4, functools.partial(some, first=end, count=4), acc)
            for k, m in zip(into, acc):
                MOM[k] = m

        @pl.when(jnp.logical_not(is_owner))
        def _(some=some, into=into):
            acc = lax.fori_loop(
                0, 2, functools.partial(some, first=1, count=16), (zero,) * len(into))
            for k, m in zip(into, acc):
                MOM[k] = m

    phase("late")
    for own, last_in in late_block.items():
        @pl.when(g == own)
        def _(own=own, last_in=last_in):
            wait_rows(rs.at[R_RS + last_in], LT * IR + 16)
            add_block(last_in, last_in - 1)
            add_below(last_in)

    phase("krylate")

    @pl.when(is_owner)
    def _():
        for body, into in sweeps:
            acc = (zero,) * len(into)
            for m in range(16):
                acc = body(row_of(start + m), acc)
            for k, m in zip(into, acc):
                MOM[k] = MOM[k] + m

    moments = [MOM[k] for k in range(6)]
    phase("red1")
    tile = zero
    for k, m in enumerate(moments):
        tile = jnp.where(sub == k, jnp.sum(m, axis=0, keepdims=True), tile)
    slot1 = 2 * g + core
    L1[slot1] = tile
    for dev in peers1:
        send(L1.at[slot1], L1.at[slot1], S_1, R_1, dev)
    wait_rows(rs.at[R_1], 8 * len(peers1))
    tile = L1[0]
    for k in range(1, 8):
        tile = tile + L1[k]
    phase("red2")
    L2[mine2] = tile
    for dev in peers2:
        send(L2.at[mine2], L2.at[mine2], S_2, R_2, dev)
    wait_rows(rs.at[R_2], 8 * len(peers2))
    tile = L2[0]
    for k in range(1, M2):
        tile = tile + L2[k]
    phase("coef")
    total = jnp.sum(tile, axis=1, keepdims=True)
    mu = [total[k:k + 1, :] for k in range(6)]
    nu = [mu[k] - mu[k + 1] for k in range(5)]

    a0 = mu[0] / nu[0]
    z10, z11 = 1.0 - a0, a0
    rz1 = z11 * (z10 * mu[1] + z11 * mu[2])
    b0 = rz1 / mu[0]
    p10, p11 = z10 + b0, z11
    a1 = rz1 / (p11 * (p10 * nu[1] + p11 * nu[2]))
    z20, z21, z22 = z10 - a1 * p10, z11 - a1 * (p11 - p10), a1 * p11
    rz2 = z22 * (z20 * mu[2] + z21 * mu[3] + z22 * mu[4])
    b1 = rz2 / rz1
    p20, p21, p22 = z20 + b1 * p10, z21 + b1 * p11, z22
    a2 = rz2 / (p22 * (p20 * nu[2] + p21 * nu[3] + p22 * nu[4]))
    k0 = jnp.broadcast_to(a0 + a1 * p10 + a2 * p20, (8, 128))
    k1 = jnp.broadcast_to(a1 * p11 + a2 * p21, (8, 128))
    k2 = jnp.broadcast_to(a2 * p22, (8, 128))

    phase("finish")
    def finish(r, carry):
        rr = pl.ds(r, 8)
        for j in range(LT):
            OUT[j, pl.ds(pl.multiple_of(r - 16, 8), 8), :] = X[j, rr, :] + (
                k0 * Z[j, rr, :] + (k1 * V1[j, rr, :] + k2 * V2[j, rr, :]))
        return carry
    ocean_rows(finish, 0)
    phase("sentwait")
    for s, cond in ((S_FL, jnp.logical_and(is_owner, has_l)), (S_FR, jnp.logical_and(is_owner, has_r))):
        @pl.when(cond)
        def _(s=s):
            wait_rows(ss.at[s], G * 16)
    for s, cond in ((S_L, has_l), (S_R, has_r)):
        @pl.when(cond)
        def _(s=s):
            wait_rows(ss.at[s], 2 * 8 * 8 + 3 * 4 * 8)
    for at in range(G):
        @pl.when(g == at)
        def _(at=at):
            full = (8 * 2 + 3) * 8 * LT + 2 * 16 + 8
            if at > 0:
                less = sum(bottom_summed(c, at - 1) for c in range(2))
                wait_rows(ss.at[S_U], full - less * 2 * 8 * LT)
            if at < G - 1:
                less = sum(top_summed(c, at + 1) for c in range(2))
                wait_rows(ss.at[S_D], full - less * 2 * 8 * LT)
            if at in (0, G - 1):
                c = 0 if at == 0 else 1
                wait_rows(ss.at[S_F], 2 * LT * sum(flow_rows(c, d)[1] for d in dests[at]))
            wait_rows(ss.at[S_FW], (2 if at in (0, G - 1) else 1) * 2 * 8 * LT)
    for c in range(2):
        mine = jnp.logical_and(is_owner, c == owner_cap)

        @pl.when(jnp.logical_not(mine))
        def _(c=c):
            wait_rows(ss.at[S_RS + c], LT * IR + 16)

    @pl.when(is_owner)
    def _():
        wait_rows(ss.at[S_RH], LT * 8 + 16)
    wait_rows(ss.at[S_1], 8 * len(peers1))
    wait_rows(ss.at[S_2], 8 * len(peers2))
    for dy, dx, cond in nbrs:
        k = 3 * (1 - dy) + (1 - dx)
        @pl.when(cond)
        def _(dy=dy, dx=dx, k=k):
            dev = (g + dy, t + dx)
            for src, dst, s, r in block_pairs(dy, 1 - dx, 0 if dy < 0 else 1):
                pltpu.make_async_remote_copy(
                    src_ref=src, dst_ref=dst, send_sem=ss.at[s + k], recv_sem=rs.at[r + k],
                    device_id=dev, device_id_type=MESH).wait_send()
    phase(None)


def shards(T, *args):
    ice = (2, NT, IH, 128)
    ocean = (NT, OH, 128)
    vm = lambda *s: pltpu.VMEM(s, F32)
    scratch = [
        vm(2, *ice), vm(*ice), vm(2, *ice), vm(*ice), vm(*ice), vm(*ice),
        vm(2, 2, 8, 8, 128), vm(2, 2, 8, 8, 128), vm(2, 3, 4, 8, 128), vm(2, 3, 4, 8, 128),
        vm(2, G, 2, 8, 128), vm(2, 2, 2, 8, 128), vm(2, 2, 2, 8, 128), vm(2, 2, 2, 8, 128),
        vm(2, 8, 128), vm(2, 8, 128), vm(2, 2, OR, 128), vm(2, LT, 8, 128),
        *[vm(*ocean) for _ in range(13)],
        pltpu.VMEM((3, 2, 8, 64), jnp.int32), pltpu.VMEM((3, 32, 64), jnp.int32),
        pltpu.VMEM((2, 8, 64), jnp.int32), pltpu.VMEM((2, 3, 8, 64), jnp.int32),
        vm(2, LT, IR, 128), vm(2, 2, 8, 128),
        vm(G, LT, IR, 128), vm(G, 2, 8, 128), vm(LT, 8, 128), vm(2, 8, 128),
        vm(8, 8, 128), vm(T // 2, 8, 128), vm(6, 8, 128), vm(DUMMY, 128),
        pltpu.SemaphoreType.DMA((N_R,)), pltpu.SemaphoreType.DMA((N_S,)), pltpu.SemaphoreType.DMA((N_L,)),
    ]
    hbm = pl.BlockSpec(memory_space=pltpu.HBM)
    vmem = pl.BlockSpec(memory_space=pltpu.VMEM)
    worked = pl.pallas_call(
        functools.partial(kernel, T),
        out_shape=(vm(2, *ice), vm(3, *ice), vm(LT, OR, 128)),
        in_specs=[hbm] * 10,
        out_specs=(vmem, vmem, vmem),
        scratch_shapes=scratch,
        compiler_params=pltpu.CompilerParams(
            collective_id=0, has_side_effects=True, vmem_limit_bytes=60 * 1024 * 1024),
    )(*args)
    return pl.pallas_call(
        deliver,
        out_shape=(
            jax.ShapeDtypeStruct((OR, 128 * LT), F32),
            jax.ShapeDtypeStruct((2, 2, IR, 128 * LT), F32),
            jax.ShapeDtypeStruct((3, 2, IR, 128 * LT), F32),
        ),
        in_specs=[vmem] * 3,
        out_specs=(hbm, hbm, hbm),
        scratch_shapes=[pltpu.SemaphoreType.DMA((3, LT))],
        compiler_params=pltpu.CompilerParams(vmem_limit_bytes=1024 * 1024),
    )(*worked)


def deliver(V, S, OUT, o_ssh, o_vel, o_str, sem):
    copies = []
    for j in range(LT):
        to = pl.ds(128 * j, 128)
        copies += [
            pltpu.make_async_copy(S.at[:, :, j, pl.ds(16, IR), :], o_str.at[:, :, :, to], sem.at[0, j]),
            pltpu.make_async_copy(V.at[:, :, j, pl.ds(16, IR), :], o_vel.at[:, :, :, to], sem.at[1, j]),
            pltpu.make_async_copy(OUT.at[j], o_ssh.at[:, to], sem.at[2, j]),
        ]
    for c in copies:
        c.start()
    for c in copies:
        c.wait()


def solution(mesh):
    return jax.shard_map(
        functools.partial(shards, mesh.shape["tile"]),
        mesh=mesh,
        in_specs=(
            P("grp", "tile"),
            P("grp", "tile"),
            P("grp", "tile"),
            P(None, "grp", "tile"),
            P("grp", "tile"),
            P(None, "grp", "tile"),
            P(None, "grp", "tile"),
            P(None, None, "grp", "tile"),
            P(None, None, "grp", "tile"),
            P(None, None, "grp", "tile"),
        ),
        out_specs=(P("grp", "tile"), P(None, None, "grp", "tile"), P(None, None, "grp", "tile")),
        check_vma=False,
    )
```

```python
import functools

import jax
import jax.numpy as jnp
from jax import lax
from jax.experimental import pallas as pl
from jax.experimental.pallas import tpu as pltpu
from jax.sharding import PartitionSpec as P

BS = 8
NSUB = 8
DAMP = 0.05
RELAX = 0.2
STRENGTH = 0.5
DRAG = 1.0
STEP = 0.5
G = 4
LT = 4
NT = LT + 1
IR = 64
OR = 256
IH = IR + 40
OH = OR + 40
F32 = jnp.float32
MESH = pl.DeviceIdType.MESH
DUMMY = 4096

R_PL, R_PR, R_FU, R_FD, R_IL, R_IR, R_OL, R_OR = 41, 43, 45, 47, 4, 5, 6, 7
R_IU, R_ID, R_F = 8, 10, 12
R_OU, R_OD, R_RS, R_RH, R_1, R_2 = 14, 15, 16, 20, 21, 22
R_BI, R_BO = 23, 32
N_R = 49
S_FL, S_FR, S_L, S_R, S_U, S_D, S_F, S_RS, S_1, S_2 = 0, 1, 2, 3, 4, 5, 6, 7, 9, 10
S_RH, S_FW = 11, 30
S_BI, S_BO = 12, 21
N_S = 31
L_BLK, L_ICE, L_FL, L_OC, L_OUT, L_OUTS, L_ED = 0, 1, 2, 3, 4, 5, 6
N_L = 7


def east(tiles, lane):
    turned = [pltpu.roll(x, 127, 1) for x in tiles]
    return [jnp.where(lane == 127, turned[(j + 1) % NT], turned[j]) for j in range(NT)]


def west(tiles, lane):
    turned = [pltpu.roll(x, 1, 1) for x in tiles]
    return [jnp.where(lane == 0, turned[(j - 1) % NT], turned[j]) for j in range(NT)]


class Phases:
    def __init__(self):
        self.open = None

    def __call__(self, name):
        if self.open is not None:
            self.open.__exit__(None, None, None)
        self.open = None
        if name:
            self.open = jax.named_scope(name)
            self.open.__enter__()


def kernel(
    T,
    base, depth, ssh, cur, land, thick, iblk, ivel, istr, wind,
    V, S, OUT,
    W, TH, FL, CV, C1, C2,
    PI, LI, PC, LC, PF, LF, PH, LH, PHO, LHO, CE, FE,
    B, D, X, Z, Y0, Y1, Y2, H, WID, DG, WET, V1, V2,
    BI, BO, PB, LB, SPB, XB, RSP, RX, RH, RXH, L1, L2, MOM, DUM,
    rs, ss, ls, far,
):
    g = lax.axis_index("grp")
    t = lax.axis_index("tile")
    has_l, has_r, has_u, has_d = t > 0, t < T - 1, g > 0, g < G - 1
    lane = lax.broadcasted_iota(jnp.int32, (8, 128), 1)
    sub = lax.broadcasted_iota(jnp.int32, (8, 128), 0)
    zero = jnp.zeros((8, 128), F32)
    first_cap = g // 2
    owner_cap = jnp.where(g == 0, 0, 1)
    is_owner = jnp.logical_or(g == 0, g == G - 1)

    def wait_rows(sem, rows):
        pltpu.make_async_copy(DUM.at[pl.ds(0, rows)], DUM.at[pl.ds(0, rows)], sem).wait()

    def send(src, dst, s, r, dev):
        pltpu.make_async_remote_copy(
            src_ref=src, dst_ref=dst, send_sem=ss.at[s], recv_sem=rs.at[r],
            device_id=dev, device_id_type=MESH,
        ).start()

    def local(src, dst, s):
        pltpu.make_async_copy(src, dst, ls.at[s]).start()

    def cols(j):
        return pl.ds(128 * j, 128)

    nbrs = []
    for dy in (-1, 0, 1):
        for dx in (-1, 0, 1):
            if dy == 0 and dx == 0:
                continue
            cond = None
            for need, there in ((dy < 0, has_u), (dy > 0, has_d), (dx < 0, has_l), (dx > 0, has_r)):
                if need:
                    cond = there if cond is None else jnp.logical_and(cond, there)
            nbrs.append((dy, dx, cond))

    def top_summed(c, d):
        return (c == 0 and d in (1, 2)) or (c == 1 and d == 1)

    def bottom_summed(c, d):
        return (c == 1 and d in (1, 2)) or (c == 0 and d == 2)

    def top_is_summed(c):
        return jnp.logical_or(g == 1, jnp.logical_and(g == 2, c == 0))

    def bottom_is_summed(c):
        return jnp.logical_or(g == 2, jnp.logical_and(g == 1, c == 1))

    phase = Phases()
    phase("signal")
    barrier = pltpu.get_barrier_semaphore()
    core = lax.rem(t, 2)
    M2 = T // 2
    mine2 = t // 2
    peers1 = []
    for dg in range(G):
        for dc in range(2):
            if dg or dc:
                peers1.append((lax.rem(g + dg, G), t - core + lax.rem(core + dc, 2)))
    peers2 = [(g, 2 * lax.rem(mine2 + k, M2) + core) for k in range(1, M2)]
    for dg in range(G):
        for dx, cond in ((-1, has_l), (0, None), (1, has_r)):
            dev = (lax.rem(g + dg, G), t + dx)
            if cond is not None:
                @pl.when(cond)
                def _(dev=dev):
                    pl.semaphore_signal(barrier, inc=1, device_id=dev, device_id_type=MESH)
            elif dg:
                pl.semaphore_signal(barrier, inc=1, device_id=dev, device_id_type=MESH)

    def tell(n):
        for dt in (-(2 << n), 2 << n):
            @pl.when(jnp.logical_and(t + dt >= 0, t + dt < T))
            def _(dt=dt):
                pl.semaphore_signal(far.at[n], inc=1, device_id=(g, t + dt), device_id_type=MESH)

    def hear(n):
        d = 2 << n
        before = jnp.minimum(jnp.maximum(t - d + 1, 0), 1)
        after = jnp.minimum(jnp.maximum(T - t - d, 0), 1)
        pl.semaphore_wait(far.at[n], before + after)

    phase("loads")
    local(iblk, BI.at[1], L_BLK)
    local(land, BO.at[1], L_BLK)
    for j in range(LT):
        local(ivel.at[:, :, :, cols(j)], V.at[:, :, j, pl.ds(16, IR), :], L_ICE)
        local(istr.at[:, :, :, cols(j)], S.at[:, :, j, pl.ds(16, IR), :], L_ICE)
        local(wind.at[:, :, :, cols(j)], W.at[:, :, j, pl.ds(16, IR), :], L_ICE)
        local(thick.at[:, :, cols(j)], TH.at[:, j, pl.ds(16, IR), :], L_ICE)
        local(base.at[:, cols(j)], B.at[j, pl.ds(16, OR), :], L_OC)
        local(depth.at[:, cols(j)], D.at[j, pl.ds(16, OR), :], L_OC)
        local(ssh.at[:, cols(j)], X.at[j, pl.ds(16, OR), :], L_OC)

    @pl.when(is_owner)
    def _():
        local(cur.at[:, :, cols(0)], CE.at[0], L_ED)
        local(cur.at[:, :, cols(LT - 1)], CE.at[1], L_ED)

    pltpu.make_async_copy(iblk, BI.at[1], ls.at[L_BLK]).wait()
    pltpu.make_async_copy(land, BO.at[1], ls.at[L_BLK]).wait()
    line = lax.broadcasted_iota(jnp.int32, (8, 64), 0)
    for e, i, o in ((0, 0, 0), (1, 7, 7)):
        ends = [BI[1, 0][i:i + 1], BI[1, 1][i:i + 1], BO[1, 24 * e:24 * e + 8][o:o + 1]]
        ends = [jnp.broadcast_to(x, (8, 64)) for x in ends]
        PB[e] = jnp.where(line == 0, ends[0], jnp.where(line == 1, ends[1], ends[2]))

    phase("barrier")
    wide = 1 + jnp.minimum(t, 1) + jnp.minimum(T - 1 - t, 1)
    pl.semaphore_wait(barrier, G * wide - 1)

    phase("sends")
    left, right, up, down = (g, t - 1), (g, t + 1), (g - 1, t), (g + 1, t)
    for dy, dx, cond in nbrs:
        k = 3 * (1 - dy) + (1 - dx)
        @pl.when(cond)
        def _(dy=dy, dx=dx, k=k):
            dev = (g + dy, t + dx)
            if dy == 0:
                send(iblk, BI.at[1 - dx], S_BI + k, R_BI + k, dev)
                send(land, BO.at[1 - dx], S_BO + k, R_BO + k, dev)
            else:
                e = 0 if dy < 0 else 1
                send(PB.at[e], LB.at[1 - e, 1 - dx], S_BI + k, R_BI + k, dev)

    def flow_rows(c, d):
        lo = IR * d if d == 0 or top_summed(c, d) else IR * d - 8
        hi = IR * d + IR if d == G - 1 or bottom_summed(c, d) else IR * d + IR + 8
        return lo, hi - lo, 16 + lo - IR * d

    dests = {0: (1, 3, 2), G - 1: (2, 0, 1)}

    def send_flow(c, d):
        lo, n, at = flow_rows(c, d)
        for j in range(LT):
            send(cur.at[:, pl.ds(lo, n), cols(j)], FL.at[:, c, j, pl.ds(at, n), :],
                 S_F, R_F + c, (d, t))

    def halo_ice(dev, c, src, dst, s, r):
        there = dev[0]
        if s == S_D:
            summed = jnp.logical_or(there == 1, jnp.logical_and(there == 2, c == 0))
        else:
            summed = jnp.logical_or(there == 2, jnp.logical_and(there == 1, c == 1))

        @pl.when(jnp.logical_not(summed))
        def _():
            for j in range(LT):
                send(wind.at[:, c, pl.ds(src, 8), cols(j)], W.at[:, c, j, pl.ds(dst, 8), :], s, r, dev)
        for j in range(LT):
            send(ivel.at[:, c, pl.ds(src, 8), cols(j)], V.at[:, c, j, pl.ds(dst, 8), :], s, r, dev)
            send(istr.at[:, c, pl.ds(src, 8), cols(j)], S.at[:, c, j, pl.ds(dst, 8), :], s, r, dev)
            send(thick.at[c, pl.ds(src, 8), cols(j)], TH.at[c, j, pl.ds(dst, 8), :], s, r, dev)

    def halo_turn(turn):
        for dev, cond, src, dst, s, r in (
            (up, has_u, 0, IR + 16, S_U, R_ID),
            (down, has_d, IR - 8, 8, S_D, R_IU),
        ):
            @pl.when(cond)
            def _(dev=dev, src=src, dst=dst, s=s, r=r):
                there = dev[0] // 2
                c = there if turn == 0 else 1 - there
                halo_ice(dev, c, src, dst, s, r + c)

    for own, c in ((0, 0), (G - 1, 1)):
        @pl.when(g == own)
        def _(own=own, c=c):
            send_flow(c, dests[own][0])
            send_flow(c, dests[own][1])
            lo, n, at = flow_rows(c, own)
            for j in range(LT):
                local(cur.at[:, pl.ds(lo, n), cols(j)], FL.at[:, c, j, pl.ds(at, n), :], L_FL)
    halo_turn(0)

    phase("zeros")
    for cond, row, orow, by in ((g == 0, 8, 8, 0), (g == G - 1, IR + 16, OR + 16, 1)):
        @pl.when(cond)
        def _(row=row, orow=orow, by=by):
            for c in range(2):
                for j in range(NT):
                    for k in range(3):
                        S[k, c, j, pl.ds(row, 8), :] = zero
                    for k in range(2):
                        V[k, c, j, pl.ds(row, 8), :] = zero
                        W[k, c, j, pl.ds(row, 8), :] = zero
                        FL[k, c, j, pl.ds(row, 8), :] = zero
                    TH[c, j, pl.ds(row, 8), :] = zero
            for j in range(NT):
                B[j, pl.ds(orow, 8), :] = zero
                D[j, pl.ds(orow, 8), :] = zero
                X[j, pl.ds(orow, 8), :] = zero
            for x in range(3):
                LB[by, x] = jnp.zeros((8, 64), jnp.int32)

    for d in (1, 2):
        @pl.when(g == d)
        def _(d=d):
            for c in range(2):
                for here, row in ((top_summed(c, d), 8), (bottom_summed(c, d), IR + 16)):
                    if here:
                        for k in range(2):
                            for j in range(LT):
                                FL[k, c, j, pl.ds(row, 8), :] = zero

    for cond, side, bx in ((t == 0, 0, 0), (t == T - 1, 1, 2)):
        @pl.when(cond)
        def _(side=side, bx=bx):
            for c in range(2):
                for k in range(8):
                    LI[side, c, k] = zero
                for v in range(2):
                    LF[side, c, v] = zero
            for k in range(3):
                for v in range(4):
                    LC[side, k, v] = zero
            for y in range(2):
                LB[y, bx] = jnp.zeros((8, 64), jnp.int32)
                BI[bx, y] = jnp.zeros((8, 64), jnp.int32)
            BO[bx] = jnp.zeros((32, 64), jnp.int32)

    phase("pack")
    slot_of = lane // 16

    def put(pack, e, at, x):
        moved = pltpu.roll(x, 16 * at, 1) if at else x
        return jnp.where(slot_of == (at - e) % 8, moved, pack)

    def take(from_right, from_left, at):
        both = jnp.where(slot_of == at, from_right, from_left)
        return pltpu.roll(both, 128 - 16 * at, 1) if at else both

    thin_of, thin_before = lane // 12, lax.rem(lane + 12, 128) // 12

    def put_thin(pack, e, at, x):
        moved = pltpu.roll(x, 12 * at, 1) if at else x
        return jnp.where((thin_before if e else thin_of) == at, moved, pack)

    def take_thin(from_right, from_left, at):
        both = jnp.where(thin_of == at, from_right, from_left)
        return pltpu.roll(both, 128 - 12 * at, 1) if at else both

    wait_rows(ls.at[L_ICE], 8 * 2 * IR * LT)

    def ice_get(k, c, j, r):
        if k < 2:
            return V[k, c, j, pl.ds(r, 8), :]
        if k < 5:
            return S[k - 2, c, j, pl.ds(r, 8), :]
        return W[k - 5, c, j, pl.ds(r, 8), :] if k < 7 else TH[c, j, pl.ds(r, 8), :]

    def ice_set(k, c, j, r, x):
        if k < 2:
            V[k, c, j, pl.ds(r, 8), :] = x
        elif k < 5:
            S[k - 2, c, j, pl.ds(r, 8), :] = x
        elif k < 7:
            W[k - 5, c, j, pl.ds(r, 8), :] = x
        else:
            TH[c, j, pl.ds(r, 8), :] = x

    for e, j in ((0, 0), (1, LT - 1)):
        for c in range(2):
            for k in range(8):
                pack = zero
                for i in range(IR // 8):
                    pack = put(pack, e, i, ice_get(k, c, j, 16 + 8 * i))
                PI[e, c, k] = pack

    for own in (0, G - 1):
        @pl.when(g == own)
        def _(own=own):
            wait_rows(ls.at[L_ED], 2 * 2 * OR)
            for e in range(2):
                for d in range(G):
                    for k in range(2):
                        pack = zero
                        for s in range(10):
                            q = 8 * d - 1 + s
                            if 0 <= q < OR // 8:
                                pack = put_thin(pack, e, s, CE[e, k, pl.ds(8 * q, 8), :])
                        PF[e, d, k] = pack

    wait_rows(ls.at[L_OC], 3 * OR * LT)
    for e, j in ((0, 0), (1, LT - 1)):
        for k, ref in enumerate((B, D, X)):
            for v in range(4):
                pack = zero
                for i in range(8):
                    pack = put(pack, e, i, ref[j, pl.ds(16 + 64 * v + 8 * i, 8), :])
                PC[e, k, v] = pack

    for e, dev, cond, s, ri, ro in ((0, left, has_l, S_L, R_IR, R_OR), (1, right, has_r, S_R, R_IL, R_OL)):
        @pl.when(cond)
        def _(e=e, dev=dev, s=s, ri=ri, ro=ro):
            send(PI.at[e], LI.at[1 - e], s, ri, dev)
            send(PC.at[e], LC.at[1 - e], s, ro, dev)

    for own, c in ((0, 0), (G - 1, 1)):
        @pl.when(g == own)
        def _(own=own, c=c):
            for e, dx, cond, s, r in ((0, -1, has_l, S_FL, R_PR), (1, 1, has_r, S_FR, R_PL)):
                @pl.when(cond)
                def _(e=e, dx=dx, s=s, r=r):
                    for dg in range(G):
                        d = dg if own == 0 else G - 1 - dg
                        dev = (g + dg if own == 0 else g - dg, t + dx)
                        send(PF.at[e, d], LF.at[1 - e, c], s, r + c, dev)

    phase("mergeice")
    @pl.when(has_l)
    def _():
        wait_rows(rs.at[R_IL], 2 * 8 * 8)

    @pl.when(has_r)
    def _():
        wait_rows(rs.at[R_IR], 2 * 8 * 8)

    tell(0)
    quarter = lane // 32
    for c in range(2):
        ends = [[zero, zero], [zero, zero]]
        for k in range(8):
            for i in range(IR // 8):
                x = take(LI[1, c, k], LI[0, c, k], i)
                ice_set(k, c, LT, 16 + 8 * i, x)
                for e, at in ((0, 0), (1, IR // 8 - 1)):
                    if i == at:
                        moved = pltpu.roll(x, (32 * (k % 4) + 16) % 128, 1)
                        ends[e][k // 4] = jnp.where(quarter == k % 4, moved, ends[e][k // 4])
        for e in range(2):
            for v in range(2):
                PH[e, c, v] = ends[e][v]
    for e, dev, cond, s, r in ((0, up, has_u, S_U, R_ID), (1, down, has_d, S_D, R_IU)):
        @pl.when(cond)
        def _(e=e, dev=dev, s=s, r=r):
            for c in range(2):
                send(PH.at[e, c], LH.at[1 - e, c], s, r + c, dev)

    for own, c, row, to, dev, r in (
        (0, 0, IR + 8, 8, down, R_FU), (G - 1, 1, 16, IR + 16, up, R_FD + 1)):
        @pl.when(g == own)
        def _(c=c, row=row, to=to, dev=dev, r=r):
            wait_rows(ls.at[L_FL], 2 * (IR + 8) * LT)
            for k in range(2):
                for j in range(LT):
                    FE[k, j] = W[k, c, j, pl.ds(row, 8), :] + FL[k, c, j, pl.ds(row, 8), :] * DRAG
            for j in range(LT):
                send(FE.at[:, j], W.at[:, c, j, pl.ds(to, 8), :], S_FW, r, dev)

    for own, c in ((0, 0), (G - 1, 1)):
        @pl.when(g == own)
        def _(own=own, c=c):
            send_flow(c, dests[own][2])
    halo_turn(1)
    def ocean_ends():
        for dev, cond, at, to, s, r in (
            (up, has_u, 0, OR + 16, S_U, R_OD),
            (down, has_d, OR - 8, 8, S_D, R_OU),
        ):
            @pl.when(cond)
            def _(dev=dev, at=at, to=to, s=s, r=r):
                for j in range(LT):
                    send(base.at[pl.ds(at, 8), cols(j)], B.at[j, pl.ds(to, 8), :], s, r, dev)
                    send(depth.at[pl.ds(at, 8), cols(j)], D.at[j, pl.ds(to, 8), :], s, r, dev)
                    send(ssh.at[pl.ds(at, 8), cols(j)], X.at[j, pl.ds(to, 8), :], s, r, dev)

    phase("mergeoc")
    @pl.when(has_l)
    def _():
        wait_rows(rs.at[R_OL], 3 * 4 * 8)

    @pl.when(has_r)
    def _():
        wait_rows(rs.at[R_OR], 3 * 4 * 8)

    ends = [zero, zero]
    for k, ref in enumerate((B, D, X)):
        for q in range(OR // 8):
            x = take(LC[1, k, q // 8], LC[0, k, q // 8], q % 8)
            ref[LT, pl.ds(16 + 8 * q, 8), :] = x
            for e, at in ((0, 0), (1, OR // 8 - 1)):
                if q == at:
                    moved = pltpu.roll(x, 32 * k + 16, 1)
                    ends[e] = jnp.where(quarter == k, moved, ends[e])
    for e, dev, cond, s, r in ((0, up, has_u, S_U, R_OD), (1, down, has_d, S_D, R_OU)):
        PHO[e] = ends[e]
        @pl.when(cond)
        def _(e=e, dev=dev, s=s, r=r):
            send(PHO.at[e], LHO.at[1 - e], s, r, dev)

    phase("masks")
    def block_pairs(dy, x, e):
        if dy == 0:
            return [(iblk, BI.at[x], S_BI, R_BI), (land, BO.at[x], S_BO, R_BO)]
        return [(PB.at[e], LB.at[1 - e, x], S_BI, R_BI)]

    for dy, dx, cond in nbrs:
        k = 3 * (1 + dy) + (1 + dx)
        @pl.when(cond)
        def _(dy=dy, dx=dx, k=k):
            dev = (g + dy, t + dx)
            pairs = block_pairs(dy, 1 + dx, 1 if dy < 0 else 0)
            for src, dst, s, r in pairs:
                pltpu.make_async_remote_copy(
                    src_ref=src, dst_ref=dst, send_sem=ss.at[s + k], recv_sem=rs.at[r + k],
                    device_id=dev, device_id_type=MESH).wait_recv()

    def selection(width, first, start):
        block = lax.broadcasted_iota(jnp.int32, (64, width), 0)
        at = lax.broadcasted_iota(jnp.int32, (64, width), 1)
        hit = block == at // BS + first
        if start is not None:
            hit = jnp.logical_and(hit, (at < 64) if start == 0 else (at >= 64))
        return hit.astype(F32)

    sel_c = selection(128 * LT, 0, None)
    sel_r = selection(128, 0, 0)
    sel_l = selection(128, 48, 1)

    def spread_rows(refs):
        lft, mid, rgt = (ref.astype(F32) for ref in refs)
        wide = jnp.dot(mid, sel_c, preferred_element_type=F32)
        last = jnp.dot(rgt, sel_r, preferred_element_type=F32) + jnp.dot(
            lft, sel_l, preferred_element_type=F32)
        return wide, last

    def paint(ref, row, parts, b):
        wide, last = parts
        for j in range(LT):
            ref[j, pl.ds(row, 8), :] = jnp.broadcast_to(wide[b:b + 1, 128 * j:128 * j + 128], (8, 128))
        ref[LT, pl.ds(row, 8), :] = jnp.broadcast_to(last[b:b + 1, :], (8, 128))

    ends = [spread_rows([LB[y, x] for x in range(3)]) for y in range(2)]
    for c in range(2):
        cov = CV.at[c]
        paint(cov, 8, ends[0], c)
        mid = spread_rows([BI[x, c] for x in range(3)])
        for b in range(8):
            paint(cov, 16 + 8 * b, mid, b)
        paint(cov, IR + 16, ends[1], c)
    paint(WET, 8, ends[0], 2)
    for q in range(4):
        mid = spread_rows([BO[x, 8 * q:8 * q + 8] for x in range(3)])
        for b in range(8):
            paint(WET, 16 + 64 * q + 8 * b, mid, b)
    paint(WET, OR + 16, ends[1], 2)

    hear(0)
    tell(1)

    def static(c, r):
        rr = pl.ds(r, 8)
        for j in range(NT):
            cov = CV[c, j, rr, :]
            thc = TH[c, j, rr, :] * cov
            scale = cov / (thc + (1.0 + STEP * DRAG))
            C1[c, j, rr, :] = scale * (thc + 1.0)
            C2[c, j, rr, :] = scale * STEP
            TH[c, j, rr, :] = thc * (RELAX * STRENGTH / (1.0 + RELAX))

    for c in range(2):
        def own_static(i, carry, c=c):
            static(c, pl.multiple_of(8 * i + 16, 8))
            return carry
        lax.fori_loop(0, IR // 8, own_static, 0)

    def pass_on(c, row, to, dev, r):
        for j in range(LT):
            send(W.at[:, c, j, pl.ds(row, 8), :], W.at[:, c, j, pl.ds(to, 8), :], S_FW, r + c, dev)

    def cap(c, turn):
        phase = Phases()
        phase("capwait")

        for e, cond, r, row, rf, summed in (
            (0, has_u, R_IU, 8, R_FU, top_is_summed(c)),
            (1, has_d, R_ID, IR + 16, R_FD, bottom_is_summed(c)),
        ):
            @pl.when(cond)
            def _(e=e, r=r, row=row, rf=rf, summed=summed):
                @pl.when(summed)
                def _():
                    wait_rows(rs.at[rf + c], 2 * 8 * LT)
                    wait_rows(rs.at[r + c], 6 * 8 * LT + 16)

                @pl.when(jnp.logical_not(summed))
                def _():
                    wait_rows(rs.at[r + c], 8 * 8 * LT + 16)
                for k in range(8):
                    x = pltpu.roll(LH[e, c, k // 4], (128 - 32 * (k % 4) - 16) % 128, 1)
                    ice_set(k, c, LT, row, x)

        @pl.when(has_l)
        def _():
            wait_rows(rs.at[R_PL + c], 16)

        @pl.when(has_r)
        def _():
            wait_rows(rs.at[R_PR + c], 16)

        for k in range(2):
            for s in range(10):
                FL[k, c, LT, pl.ds(8 + 8 * s, 8), :] = take_thin(LF[1, c, k], LF[0, c, k], s)

        mine = jnp.logical_and(is_owner, c == owner_cap)
        at_end = jnp.logical_or(jnp.logical_and(c == 0, g == G - 1), jnp.logical_and(c == 1, g == 0))

        @pl.when(jnp.logical_not(mine))
        def _():
            both = jnp.logical_and(top_is_summed(c), bottom_is_summed(c))

            @pl.when(both)
            def _():
                wait_rows(rs.at[R_F + c], 2 * IR * LT)

            @pl.when(jnp.logical_not(both))
            def _():
                wait_rows(rs.at[R_F + c], 2 * (IR + 8) * LT)

        phase("prepare")
        @pl.when(turn == 0)
        def _():
            hear(1)
            tell(2)
        static(c, 8)
        static(c, IR + 16)

        def prepare(i, carry):
            r = pl.ds(pl.multiple_of(8 * i + 8, 8), 8)
            for j in range(NT):
                for k in range(2):
                    W[k, c, j, r, :] = W[k, c, j, r, :] + FL[k, c, j, r, :] * DRAG
            return carry
        lax.fori_loop(0, IR // 8 + 2, prepare, 0)

        @pl.when(jnp.logical_and(c == 0, g == 1))
        def _():
            pass_on(0, IR + 8, 8, down, R_FU)

        @pl.when(jnp.logical_and(c == 0, g == G - 1))
        def _():
            pass_on(0, 16, IR + 16, up, R_FD)

        @pl.when(jnp.logical_and(c == 1, g == 0))
        def _():
            pass_on(1, IR + 8, 8, down, R_FU)

        @pl.when(jnp.logical_and(c == 1, g == 2))
        def _():
            pass_on(1, 16, IR + 16, up, R_FD)

        phase("subcycles")
        @pl.when(turn == 1)
        def _():
            ocean_ends()

        keep = 1.0 / (1.0 + RELAX)

        def group(r):
            rr = pl.ds(r, 8)
            u = [V[0, c, j, rr, :] for j in range(NT)]
            v = [V[1, c, j, rr, :] for j in range(NT)]
            ue, ve = east(u, lane), east(v, lane)
            s0, s1, s2 = [], [], []
            for j in range(NT):
                dux = V[0, c, j, pl.ds(r + 1, 8), :] - u[j]
                dvx = V[1, c, j, pl.ds(r + 1, 8), :] - v[j]
                duy, dvy = ue[j] - u[j], ve[j] - v[j]
                ed, et, es = dux + dvy, dux - dvy, duy + dvx
                inv = lax.rsqrt(ed * ed + et * et + es * es + 1.0)
                a = TH[c, j, rr, :]
                ai = a * inv
                s0.append(S[0, c, j, rr, :] * keep + (ed * ai - a))
                s1.append(S[1, c, j, rr, :] * keep + et * ai)
                s2.append(S[2, c, j, rr, :] * keep + es * ai)
                S[0, c, j, rr, :] = s0[j]
                S[1, c, j, rr, :] = s1[j]
                S[2, c, j, rr, :] = s2[j]

        def push(r):
            rr, above = pl.ds(r, 8), pl.ds(r - 1, 8)
            s0 = [S[0, c, j, rr, :] for j in range(NT)]
            s1 = [S[1, c, j, rr, :] for j in range(NT)]
            s2 = [S[2, c, j, rr, :] for j in range(NT)]
            dif = [s0[j] - s1[j] for j in range(NT)]
            dw, sw = west(dif, lane), west(s2, lane)
            for j in range(NT):
                tot_up = S[0, c, j, above, :] + S[1, c, j, above, :]
                f0 = 0.5 * ((s0[j] + s1[j]) - tot_up) + (s2[j] - sw[j])
                f1 = 0.5 * (dif[j] - dw[j]) + (s2[j] - S[2, c, j, above, :])
                c1, c2 = C1[c, j, rr, :], C2[c, j, rr, :]
                V[0, c, j, rr, :] = c1 * V[0, c, j, rr, :] + c2 * (f0 + W[0, c, j, rr, :])
                V[1, c, j, rr, :] = c1 * V[1, c, j, rr, :] + c2 * (f1 + W[1, c, j, rr, :])

        def subcycle(n, carry):
            for i in range(IR // 8 + 2):
                group(8 + 8 * i)
            for i in range(IR // 8 + 2):
                push(8 + 8 * i)
            return carry
        lax.fori_loop(0, NSUB, subcycle, 0)

        phase("diverge")
        @pl.when(turn == 0)
        def _():
            hear(2)
            tell(3)
        prev = [zero] * NT
        pack = zero
        for i in range(IR // 8):
            rr = pl.ds(16 + 8 * i, 8)
            p0, p1 = [], []
            for j in range(NT):
                cov = CV[c, j, rr, :] * DRAG
                p0.append(cov * (V[0, c, j, rr, :] - FL[0, c, j, rr, :]))
                p1.append(cov * (V[1, c, j, rr, :] - FL[1, c, j, rr, :]))
            pw = west(p1, lane)
            for j in range(NT):
                turned = pltpu.roll(p0[j], 1, 0)
                above = jnp.where(sub == 0, prev[j], turned)
                prev[j] = turned
                sp = (p0[j] - above) + (p1[j] - pw[j])
                if j < LT:
                    SPB[c, j, pl.ds(8 * i, 8), :] = sp
                else:
                    pack = jnp.where(lane // 16 == i, pltpu.roll(sp, 16 * i + 8, 1), pack)
        XB[c, 0] = pack
        extra = zero
        for j in range(NT):
            extra = jnp.where(sub == j, -jnp.broadcast_to(prev[j][0:1, :], (8, 128)), extra)
        XB[c, 1] = extra

        @pl.when(mine)
        def _():
            for j in range(LT):
                for i in range(IR // 8):
                    RSP[g, j, pl.ds(8 * i, 8), :] = SPB[c, j, pl.ds(8 * i, 8), :]
            RX[g, 0] = XB[c, 0]
            RX[g, 1] = XB[c, 1]

        @pl.when(jnp.logical_not(mine))
        def _():
            dev = (c * (G - 1), t)
            send(SPB.at[c], RSP.at[g], S_RS + c, R_RS + g, dev)
            send(XB.at[c], RX.at[g], S_RS + c, R_RS + g, dev)

        @pl.when(at_end)
        def _():
            at = jnp.where(c == 0, IR - 8, 0)
            dev = (1 + c, t)
            send(SPB.at[c, :, pl.ds(pl.multiple_of(at, 8), 8), :], RH, S_RH, R_RH, dev)
            send(XB.at[c], RXH, S_RH, R_RH, dev)
        phase(None)

    def caps(turn, carry):
        cap(jnp.where(turn == 0, first_cap, 1 - first_cap), turn)
        return carry

    def ocean_rows(body, carry, unroll=4):
        def step(i, cc):
            for m in range(unroll):
                cc = body(pl.multiple_of(8 * (unroll * i + m) + 16, 8), cc)
            return cc
        return lax.fori_loop(0, OR // 8 // unroll, step, carry)

    def shifted_sum(ref, r):
        rr = pl.ds(r, 8)
        mid = [ref[j, rr, :] for j in range(NT)]
        e, w = east(mid, lane), west(mid, lane)
        return mid, [
            (ref[j, pl.ds(r + 1, 8), :] + ref[j, pl.ds(r - 1, 8), :]) + (e[j] + w[j])
            for j in range(NT)
        ]

    def ocean_prepare():
        phase = Phases()
        phase("oceanwait")

        for e, cond, r, row in ((0, has_u, R_OU, 8), (1, has_d, R_OD, OR + 16)):
            @pl.when(cond)
            def _(e=e, r=r, row=row):
                wait_rows(rs.at[r], 24 * LT + 8)
                for k, ref in enumerate((B, D, X)):
                    ref[LT, pl.ds(row, 8), :] = pltpu.roll(LHO[e], 128 - 32 * k - 16, 1)

        phase("oceanprep")
        def first(r, carry):
            rr = pl.ds(r, 8)
            for j in range(NT):
                gg = D[j, rr, :] * WET[j, rr, :]
                D[j, rr, :] = gg
                Y0[j, rr, :] = gg * X[j, rr, :]
            return carry

        def second(r, carry):
            rr = pl.ds(r, 8)
            gs, gn = shifted_sum(D, r)
            _, xn = shifted_sum(Y0, r)
            for j in range(NT):
                diag = gs[j] * gn[j] + DAMP
                inv = 1.0 / diag
                wid = WET[j, rr, :] * inv
                h = gs[j] * inv
                DG[j, rr, :] = diag
                WID[j, rr, :] = wid
                H[j, rr, :] = h
                Z[j, rr, :] = wid * B[j, rr, :] + h * xn[j] - X[j, rr, :]
            return carry
        for body in (first, second):
            body(8, 0)
            ocean_rows(body, 0)
            body(OR + 16, 0)
        phase(None)

    lax.fori_loop(0, 2, caps, 0)
    ocean_prepare()

    phase("arrive")
    late_block = {0: 2, G - 1: 1}

    def add_block(d, more_from):
        for i in range(IR // 8):
            rr = pl.ds(16 + IR * d + 8 * i, 8)
            for j in range(NT):
                if j < LT:
                    sp = RSP[d, j, pl.ds(8 * i, 8), :]
                else:
                    sp = pltpu.roll(RX[d, 0], 128 - (16 * i + 8), 1)
                if i == 0 and more_from is not None:
                    sp = sp + below_block(more_from, j)
                Z[j, rr, :] = Z[j, rr, :] + WID[j, rr, :] * sp

    def below_block(d, j):
        return jnp.where(sub == 0, jnp.broadcast_to(RX[d, 1][j:j + 1, :], (8, 128)), 0.0)

    def add_below(d):
        rr = pl.ds(16 + IR * (d + 1), 8)
        for j in range(NT):
            Z[j, rr, :] = Z[j, rr, :] + WID[j, rr, :] * below_block(d, j)

    for own, last_in in late_block.items():
        @pl.when(g == own)
        def _(own=own, last_in=last_in):
            rest = [d for d in range(G) if d != last_in]
            for d in rest:
                if d != own:
                    wait_rows(rs.at[R_RS + d], LT * IR + 16)
            for d in rest:
                add_block(d, d - 1 if d - 1 in rest else None)
            if own == 0:
                add_below(G - 1)

    @pl.when(jnp.logical_not(is_owner))
    def _():
        wait_rows(rs.at[R_RH], LT * 8 + 16)

        @pl.when(g == 1)
        def _():
            rr = pl.ds(16, 8)
            for j in range(NT):
                more = jnp.broadcast_to(RXH[1][j:j + 1, :], (8, 128))
                Z[j, rr, :] = Z[j, rr, :] + WID[j, rr, :] * jnp.where(sub == 0, more, 0.0)
        for at, row, i in ((1, 8, 7), (2, OR + 16, 0)):
            @pl.when(g == at)
            def _(row=row, i=i):
                rr = pl.ds(row, 8)
                for j in range(NT):
                    sp = RH[j] if j < LT else pltpu.roll(RXH[0], 128 - (16 * i + 8), 1)
                    Z[j, rr, :] = Z[j, rr, :] + WID[j, rr, :] * sp

    phase("krylov")
    def krylov0(r, acc):
        rr = pl.ds(r, 8)
        for j in range(NT):
            z = Z[j, rr, :]
            Y0[j, rr, :] = D[j, rr, :] * z
            if j < LT and acc is not None:
                acc = (acc[0] + DG[j, rr, :] * z * z,)
        return acc

    def krylov(src, dst, vec, r, acc):
        rr = pl.ds(r, 8)
        y, n = shifted_sum(src, r)
        for j in range(NT):
            v = H[j, rr, :] * n[j]
            out = D[j, rr, :] * v
            vec[j, rr, :] = v
            dst[j, rr, :] = out
            if j < LT and acc is not None:
                acc = (acc[0] + y[j] * n[j], acc[1] + out * n[j])
        return acc

    def krylov3(r, acc):
        if acc is None:
            return None
        y, n = shifted_sum(Y2, r)
        for j in range(LT):
            acc = (acc[0] + y[j] * n[j],)
        return acc

    sweeps = (
        (krylov0, (0,)),
        (functools.partial(krylov, Y0, Y1, V1), (1, 2)),
        (functools.partial(krylov, Y1, Y2, V2), (3, 4)),
        (krylov3, (5,)),
    )
    start = jnp.where(g == 0, 13, jnp.where(g == G - 1, 5, 17))
    end = jnp.where(g == 0, 29, jnp.where(g == G - 1, 21, 17))

    def row_of(group):
        return pl.multiple_of(8 * group + 8, 8)

    for body, into in sweeps:
        body(8, None)
        body(OR + 16, None)
        body(row_of(start), None)
        body(row_of(end - 1), None)

        def some(i, acc, first, count, body=body):
            for m in range(count):
                acc = body(row_of(first + count * i + m), acc)
            return acc

        @pl.when(is_owner)
        def _(some=some, into=into):
            acc = (zero,) * len(into)
            acc = lax.fori_loop(0, (start - 1) // 4, functools.partial(some, first=1, count=4), acc)
            acc = lax.fori_loop(0, (33 - end) // 4, functools.partial(some, first=end, count=4), acc)
            for k, m in zip(into, acc):
                MOM[k] = m

        @pl.when(jnp.logical_not(is_owner))
        def _(some=some, into=into):
            acc = lax.fori_loop(
                0, 2, functools.partial(some, first=1, count=16), (zero,) * len(into))
            for k, m in zip(into, acc):
                MOM[k] = m

    phase("late")
    for own, last_in in late_block.items():
        @pl.when(g == own)
        def _(own=own, last_in=last_in):
            wait_rows(rs.at[R_RS + last_in], LT * IR + 16)
            add_block(last_in, last_in - 1)
            add_below(last_in)

    phase("krylate")

    @pl.when(is_owner)
    def _():
        for body, into in sweeps:
            acc = (zero,) * len(into)
            for m in range(16):
                acc = body(row_of(start + m), acc)
            for k, m in zip(into, acc):
                MOM[k] = MOM[k] + m

    moments = [MOM[k] for k in range(6)]
    phase("red1")
    tile = zero
    for k, m in enumerate(moments):
        tile = jnp.where(sub == k, jnp.sum(m, axis=0, keepdims=True), tile)
    slot1 = 2 * g + core
    L1[slot1] = tile
    for dev in peers1:
        send(L1.at[slot1], L1.at[slot1], S_1, R_1, dev)
    wait_rows(rs.at[R_1], 8 * len(peers1))
    tile = L1[0]
    for k in range(1, 8):
        tile = tile + L1[k]
    phase("red2")
    hear(3)
    L2[mine2] = tile
    for dev in peers2:
        send(L2.at[mine2], L2.at[mine2], S_2, R_2, dev)
    wait_rows(rs.at[R_2], 8 * len(peers2))
    tile = L2[0]
    for k in range(1, M2):
        tile = tile + L2[k]
    phase("coef")
    total = jnp.sum(tile, axis=1, keepdims=True)
    mu = [total[k:k + 1, :] for k in range(6)]
    nu = [mu[k] - mu[k + 1] for k in range(5)]

    a0 = mu[0] / nu[0]
    z10, z11 = 1.0 - a0, a0
    rz1 = z11 * (z10 * mu[1] + z11 * mu[2])
    b0 = rz1 / mu[0]
    p10, p11 = z10 + b0, z11
    a1 = rz1 / (p11 * (p10 * nu[1] + p11 * nu[2]))
    z20, z21, z22 = z10 - a1 * p10, z11 - a1 * (p11 - p10), a1 * p11
    rz2 = z22 * (z20 * mu[2] + z21 * mu[3] + z22 * mu[4])
    b1 = rz2 / rz1
    p20, p21, p22 = z20 + b1 * p10, z21 + b1 * p11, z22
    a2 = rz2 / (p22 * (p20 * nu[2] + p21 * nu[3] + p22 * nu[4]))
    k0 = jnp.broadcast_to(a0 + a1 * p10 + a2 * p20, (8, 128))
    k1 = jnp.broadcast_to(a1 * p11 + a2 * p21, (8, 128))
    k2 = jnp.broadcast_to(a2 * p22, (8, 128))

    phase("finish")
    def finish(r, carry):
        rr = pl.ds(r, 8)
        for j in range(LT):
            OUT[j, pl.ds(pl.multiple_of(r - 16, 8), 8), :] = X[j, rr, :] + (
                k0 * Z[j, rr, :] + (k1 * V1[j, rr, :] + k2 * V2[j, rr, :]))
        return carry
    ocean_rows(finish, 0)
    phase("sentwait")
    for s, cond in ((S_FL, jnp.logical_and(is_owner, has_l)), (S_FR, jnp.logical_and(is_owner, has_r))):
        @pl.when(cond)
        def _(s=s):
            wait_rows(ss.at[s], G * 16)
    for s, cond in ((S_L, has_l), (S_R, has_r)):
        @pl.when(cond)
        def _(s=s):
            wait_rows(ss.at[s], 2 * 8 * 8 + 3 * 4 * 8)
    for at in range(G):
        @pl.when(g == at)
        def _(at=at):
            full = (8 * 2 + 3) * 8 * LT + 2 * 16 + 8
            if at > 0:
                less = sum(bottom_summed(c, at - 1) for c in range(2))
                wait_rows(ss.at[S_U], full - less * 2 * 8 * LT)
            if at < G - 1:
                less = sum(top_summed(c, at + 1) for c in range(2))
                wait_rows(ss.at[S_D], full - less * 2 * 8 * LT)
            if at in (0, G - 1):
                c = 0 if at == 0 else 1
                wait_rows(ss.at[S_F], 2 * LT * sum(flow_rows(c, d)[1] for d in dests[at]))
            wait_rows(ss.at[S_FW], (2 if at in (0, G - 1) else 1) * 2 * 8 * LT)
    for c in range(2):
        mine = jnp.logical_and(is_owner, c == owner_cap)

        @pl.when(jnp.logical_not(mine))
        def _(c=c):
            wait_rows(ss.at[S_RS + c], LT * IR + 16)

    @pl.when(is_owner)
    def _():
        wait_rows(ss.at[S_RH], LT * 8 + 16)
    wait_rows(ss.at[S_1], 8 * len(peers1))
    wait_rows(ss.at[S_2], 8 * len(peers2))
    for dy, dx, cond in nbrs:
        k = 3 * (1 - dy) + (1 - dx)
        @pl.when(cond)
        def _(dy=dy, dx=dx, k=k):
            dev = (g + dy, t + dx)
            for src, dst, s, r in block_pairs(dy, 1 - dx, 0 if dy < 0 else 1):
                pltpu.make_async_remote_copy(
                    src_ref=src, dst_ref=dst, send_sem=ss.at[s + k], recv_sem=rs.at[r + k],
                    device_id=dev, device_id_type=MESH).wait_send()
    phase(None)


def shards(T, *args):
    ice = (2, NT, IH, 128)
    ocean = (NT, OH, 128)
    vm = lambda *s: pltpu.VMEM(s, F32)
    scratch = [
        vm(2, *ice), vm(*ice), vm(2, *ice), vm(*ice), vm(*ice), vm(*ice),
        vm(2, 2, 8, 8, 128), vm(2, 2, 8, 8, 128), vm(2, 3, 4, 8, 128), vm(2, 3, 4, 8, 128),
        vm(2, G, 2, 8, 128), vm(2, 2, 2, 8, 128), vm(2, 2, 2, 8, 128), vm(2, 2, 2, 8, 128),
        vm(2, 8, 128), vm(2, 8, 128), vm(2, 2, OR, 128), vm(2, LT, 8, 128),
        *[vm(*ocean) for _ in range(13)],
        pltpu.VMEM((3, 2, 8, 64), jnp.int32), pltpu.VMEM((3, 32, 64), jnp.int32),
        pltpu.VMEM((2, 8, 64), jnp.int32), pltpu.VMEM((2, 3, 8, 64), jnp.int32),
        vm(2, LT, IR, 128), vm(2, 2, 8, 128),
        vm(G, LT, IR, 128), vm(G, 2, 8, 128), vm(LT, 8, 128), vm(2, 8, 128),
        vm(8, 8, 128), vm(T // 2, 8, 128), vm(6, 8, 128), vm(DUMMY, 128),
        pltpu.SemaphoreType.DMA((N_R,)), pltpu.SemaphoreType.DMA((N_S,)), pltpu.SemaphoreType.DMA((N_L,)),
        pltpu.SemaphoreType.REGULAR((4,)),
    ]
    hbm = pl.BlockSpec(memory_space=pltpu.HBM)
    vmem = pl.BlockSpec(memory_space=pltpu.VMEM)
    worked = pl.pallas_call(
        functools.partial(kernel, T),
        out_shape=(vm(2, *ice), vm(3, *ice), vm(LT, OR, 128)),
        in_specs=[hbm] * 10,
        out_specs=(vmem, vmem, vmem),
        scratch_shapes=scratch,
        compiler_params=pltpu.CompilerParams(
            collective_id=0, has_side_effects=True, vmem_limit_bytes=60 * 1024 * 1024),
    )(*args)
    return pl.pallas_call(
        deliver,
        out_shape=(
            jax.ShapeDtypeStruct((OR, 128 * LT), F32),
            jax.ShapeDtypeStruct((2, 2, IR, 128 * LT), F32),
            jax.ShapeDtypeStruct((3, 2, IR, 128 * LT), F32),
        ),
        in_specs=[vmem] * 3,
        out_specs=(hbm, hbm, hbm),
        scratch_shapes=[pltpu.SemaphoreType.DMA((3, LT))],
        compiler_params=pltpu.CompilerParams(vmem_limit_bytes=1024 * 1024),
    )(*worked)


def deliver(V, S, OUT, o_ssh, o_vel, o_str, sem):
    copies = []
    for j in range(LT):
        to = pl.ds(128 * j, 128)
        copies += [
            pltpu.make_async_copy(S.at[:, :, j, pl.ds(16, IR), :], o_str.at[:, :, :, to], sem.at[0, j]),
            pltpu.make_async_copy(V.at[:, :, j, pl.ds(16, IR), :], o_vel.at[:, :, :, to], sem.at[1, j]),
            pltpu.make_async_copy(OUT.at[j], o_ssh.at[:, to], sem.at[2, j]),
        ]
    for c in copies:
        c.start()
    for c in copies:
        c.wait()


def solution(mesh):
    return jax.shard_map(
        functools.partial(shards, mesh.shape["tile"]),
        mesh=mesh,
        in_specs=(
            P("grp", "tile"),
            P("grp", "tile"),
            P("grp", "tile"),
            P(None, "grp", "tile"),
            P("grp", "tile"),
            P(None, "grp", "tile"),
            P(None, "grp", "tile"),
            P(None, None, "grp", "tile"),
            P(None, None, "grp", "tile"),
            P(None, None, "grp", "tile"),
        ),
        out_specs=(P("grp", "tile"), P(None, None, "grp", "tile"), P(None, None, "grp", "tile")),
        check_vma=False,
    )
```

```python
import functools

import jax
import jax.numpy as jnp
from jax import lax
from jax.experimental import pallas as pl
from jax.experimental.pallas import tpu as pltpu
from jax.sharding import PartitionSpec as P

BS = 8
NSUB = 8
DAMP = 0.05
RELAX = 0.2
STRENGTH = 0.5
DRAG = 1.0
STEP = 0.5
G = 4
LT = 4
NT = LT + 1
IR = 64
OR = 256
IH = IR + 40
OH = OR + 40
F32 = jnp.float32
MESH = pl.DeviceIdType.MESH
DUMMY = 4096

R_PL, R_PR, R_FU, R_FD, R_IL, R_IR, R_OL, R_OR = 41, 43, 45, 47, 4, 5, 6, 7
R_IU, R_ID, R_F = 8, 10, 12
R_OU, R_OD, R_RS, R_RH, R_1, R_2 = 14, 15, 16, 20, 21, 22
R_BI, R_BO = 23, 32
N_R = 49
S_FL, S_FR, S_L, S_R, S_U, S_D, S_F, S_RS, S_1, S_2 = 0, 1, 2, 3, 4, 5, 6, 7, 9, 10
S_RH, S_FW = 11, 30
S_BI, S_BO = 12, 21
N_S = 31
L_BLK, L_ICE, L_FL, L_OC, L_OUT, L_OUTS, L_ED = 0, 1, 2, 3, 4, 5, 6
N_L = 7


def east(tiles, lane):
    turned = [pltpu.roll(x, 127, 1) for x in tiles]
    return [jnp.where(lane == 127, turned[(j + 1) % NT], turned[j]) for j in range(NT)]


def west(tiles, lane):
    turned = [pltpu.roll(x, 1, 1) for x in tiles]
    return [jnp.where(lane == 0, turned[(j - 1) % NT], turned[j]) for j in range(NT)]


class Phases:
    def __init__(self):
        self.open = None

    def __call__(self, name):
        if self.open is not None:
            self.open.__exit__(None, None, None)
        self.open = None
        if name:
            self.open = jax.named_scope(name)
            self.open.__enter__()


def kernel(
    T,
    base, depth, ssh, cur, land, thick, iblk, ivel, istr, wind,
    V, S, OUT,
    W, TH, FL, CV, C1, C2,
    PI, LI, PC, LC, PF, LF, PH, LH, PHO, LHO, CE, FE,
    B, D, X, Z, Y0, Y1, Y2, H, WID, DG, WET, V1, V2,
    BI, BO, PB, LB, SPB, XB, RSP, RX, RH, RXH, L1, L2, MOM, DUM,
    rs, ss, ls,
):
    g = lax.axis_index("grp")
    t = lax.axis_index("tile")
    has_l, has_r, has_u, has_d = t > 0, t < T - 1, g > 0, g < G - 1
    lane = lax.broadcasted_iota(jnp.int32, (8, 128), 1)
    sub = lax.broadcasted_iota(jnp.int32, (8, 128), 0)
    zero = jnp.zeros((8, 128), F32)
    first_cap = g // 2
    owner_cap = jnp.where(g == 0, 0, 1)
    is_owner = jnp.logical_or(g == 0, g == G - 1)

    def wait_rows(sem, rows):
        pltpu.make_async_copy(DUM.at[pl.ds(0, rows)], DUM.at[pl.ds(0, rows)], sem).wait()

    def send(src, dst, s, r, dev):
        pltpu.make_async_remote_copy(
            src_ref=src, dst_ref=dst, send_sem=ss.at[s], recv_sem=rs.at[r],
            device_id=dev, device_id_type=MESH,
        ).start()

    def local(src, dst, s):
        pltpu.make_async_copy(src, dst, ls.at[s]).start()

    def cols(j):
        return pl.ds(128 * j, 128)

    nbrs = []
    for dy in (-1, 0, 1):
        for dx in (-1, 0, 1):
            if dy == 0 and dx == 0:
                continue
            cond = None
            for need, there in ((dy < 0, has_u), (dy > 0, has_d), (dx < 0, has_l), (dx > 0, has_r)):
                if need:
                    cond = there if cond is None else jnp.logical_and(cond, there)
            nbrs.append((dy, dx, cond))

    def top_summed(c, d):
        return (c == 0 and d in (1, 2)) or (c == 1 and d == 1)

    def bottom_summed(c, d):
        return (c == 1 and d in (1, 2)) or (c == 0 and d == 2)

    def top_is_summed(c):
        return jnp.logical_or(g == 1, jnp.logical_and(g == 2, c == 0))

    def bottom_is_summed(c):
        return jnp.logical_or(g == 2, jnp.logical_and(g == 1, c == 1))

    phase = Phases()
    phase("signal")
    barrier = pltpu.get_barrier_semaphore()
    core = lax.rem(t, 2)
    M2 = T // 2
    mine2 = t // 2
    peers1 = []
    for dg in range(G):
        for dc in range(2):
            if dg or dc:
                peers1.append((lax.rem(g + dg, G), t - core + lax.rem(core + dc, 2)))
    peers2 = [(g, 2 * lax.rem(mine2 + k, M2) + core) for k in range(1, M2)]
    for dg in range(G):
        for dx, cond in ((-1, has_l), (0, None), (1, has_r)):
            dev = (lax.rem(g + dg, G), t + dx)
            if cond is not None:
                @pl.when(cond)
                def _(dev=dev):
                    pl.semaphore_signal(barrier, inc=1, device_id=dev, device_id_type=MESH)
            elif dg:
                pl.semaphore_signal(barrier, inc=1, device_id=dev, device_id_type=MESH)
    for dev in peers2:
        pl.semaphore_signal(barrier, inc=1, device_id=dev, device_id_type=MESH)

    phase("loads")
    local(iblk, BI.at[1], L_BLK)
    local(land, BO.at[1], L_BLK)
    for j in range(LT):
        local(ivel.at[:, :, :, cols(j)], V.at[:, :, j, pl.ds(16, IR), :], L_ICE)
        local(istr.at[:, :, :, cols(j)], S.at[:, :, j, pl.ds(16, IR), :], L_ICE)
        local(wind.at[:, :, :, cols(j)], W.at[:, :, j, pl.ds(16, IR), :], L_ICE)
        local(thick.at[:, :, cols(j)], TH.at[:, j, pl.ds(16, IR), :], L_ICE)
        local(base.at[:, cols(j)], B.at[j, pl.ds(16, OR), :], L_OC)
        local(depth.at[:, cols(j)], D.at[j, pl.ds(16, OR), :], L_OC)
        local(ssh.at[:, cols(j)], X.at[j, pl.ds(16, OR), :], L_OC)

    @pl.when(is_owner)
    def _():
        local(cur.at[:, :, cols(0)], CE.at[0], L_ED)
        local(cur.at[:, :, cols(LT - 1)], CE.at[1], L_ED)

    pltpu.make_async_copy(iblk, BI.at[1], ls.at[L_BLK]).wait()
    pltpu.make_async_copy(land, BO.at[1], ls.at[L_BLK]).wait()
    line = lax.broadcasted_iota(jnp.int32, (8, 64), 0)
    for e, i, o in ((0, 0, 0), (1, 7, 7)):
        ends = [BI[1, 0][i:i + 1], BI[1, 1][i:i + 1], BO[1, 24 * e:24 * e + 8][o:o + 1]]
        ends = [jnp.broadcast_to(x, (8, 64)) for x in ends]
        PB[e] = jnp.where(line == 0, ends[0], jnp.where(line == 1, ends[1], ends[2]))

    phase("barrier")
    wide = 1 + jnp.minimum(t, 1) + jnp.minimum(T - 1 - t, 1)
    pl.semaphore_wait(barrier, G * wide - 1 + len(peers2))

    phase("sends")
    left, right, up, down = (g, t - 1), (g, t + 1), (g - 1, t), (g + 1, t)
    for dy, dx, cond in nbrs:
        k = 3 * (1 - dy) + (1 - dx)
        @pl.when(cond)
        def _(dy=dy, dx=dx, k=k):
            dev = (g + dy, t + dx)
            if dy == 0:
                send(iblk, BI.at[1 - dx], S_BI + k, R_BI + k, dev)
                send(land, BO.at[1 - dx], S_BO + k, R_BO + k, dev)
            else:
                e = 0 if dy < 0 else 1
                send(PB.at[e], LB.at[1 - e, 1 - dx], S_BI + k, R_BI + k, dev)

    def flow_rows(c, d):
        lo = IR * d if d == 0 or top_summed(c, d) else IR * d - 8
        hi = IR * d + IR if d == G - 1 or bottom_summed(c, d) else IR * d + IR + 8
        return lo, hi - lo, 16 + lo - IR * d

    dests = {0: (1, 3, 2), G - 1: (2, 0, 1)}

    def send_flow(c, d):
        lo, n, at = flow_rows(c, d)
        for j in range(LT):
            send(cur.at[:, pl.ds(lo, n), cols(j)], FL.at[:, c, j, pl.ds(at, n), :],
                 S_F, R_F + c, (d, t))

    def halo_ice(dev, c, src, dst, s, r):
        there = dev[0]
        if s == S_D:
            summed = jnp.logical_or(there == 1, jnp.logical_and(there == 2, c == 0))
        else:
            summed = jnp.logical_or(there == 2, jnp.logical_and(there == 1, c == 1))

        @pl.when(jnp.logical_not(summed))
        def _():
            for j in range(LT):
                send(wind.at[:, c, pl.ds(src, 8), cols(j)], W.at[:, c, j, pl.ds(dst, 8), :], s, r, dev)
        for j in range(LT):
            send(ivel.at[:, c, pl.ds(src, 8), cols(j)], V.at[:, c, j, pl.ds(dst, 8), :], s, r, dev)
            send(istr.at[:, c, pl.ds(src, 8), cols(j)], S.at[:, c, j, pl.ds(dst, 8), :], s, r, dev)
            send(thick.at[c, pl.ds(src, 8), cols(j)], TH.at[c, j, pl.ds(dst, 8), :], s, r, dev)

    def halo_turn(turn):
        for dev, cond, src, dst, s, r in (
            (up, has_u, 0, IR + 16, S_U, R_ID),
            (down, has_d, IR - 8, 8, S_D, R_IU),
        ):
            @pl.when(cond)
            def _(dev=dev, src=src, dst=dst, s=s, r=r):
                there = dev[0] // 2
                c = there if turn == 0 else 1 - there
                halo_ice(dev, c, src, dst, s, r + c)

    for own, c in ((0, 0), (G - 1, 1)):
        @pl.when(g == own)
        def _(own=own, c=c):
            send_flow(c, dests[own][0])
            send_flow(c, dests[own][1])
            lo, n, at = flow_rows(c, own)
            for j in range(LT):
                local(cur.at[:, pl.ds(lo, n), cols(j)], FL.at[:, c, j, pl.ds(at, n), :], L_FL)
    halo_turn(0)

    phase("zeros")
    for cond, row, orow, by in ((g == 0, 8, 8, 0), (g == G - 1, IR + 16, OR + 16, 1)):
        @pl.when(cond)
        def _(row=row, orow=orow, by=by):
            for c in range(2):
                for j in range(NT):
                    for k in range(3):
                        S[k, c, j, pl.ds(row, 8), :] = zero
                    for k in range(2):
                        V[k, c, j, pl.ds(row, 8), :] = zero
                        W[k, c, j, pl.ds(row, 8), :] = zero
                        FL[k, c, j, pl.ds(row, 8), :] = zero
                    TH[c, j, pl.ds(row, 8), :] = zero
            for j in range(NT):
                B[j, pl.ds(orow, 8), :] = zero
                D[j, pl.ds(orow, 8), :] = zero
                X[j, pl.ds(orow, 8), :] = zero
            for x in range(3):
                LB[by, x] = jnp.zeros((8, 64), jnp.int32)

    for d in (1, 2):
        @pl.when(g == d)
        def _(d=d):
            for c in range(2):
                for here, row in ((top_summed(c, d), 8), (bottom_summed(c, d), IR + 16)):
                    if here:
                        for k in range(2):
                            for j in range(LT):
                                FL[k, c, j, pl.ds(row, 8), :] = zero

    for cond, side, bx in ((t == 0, 0, 0), (t == T - 1, 1, 2)):
        @pl.when(cond)
        def _(side=side, bx=bx):
            for c in range(2):
                for k in range(8):
                    LI[side, c, k] = zero
                for v in range(2):
                    LF[side, c, v] = zero
            for k in range(3):
                for v in range(4):
                    LC[side, k, v] = zero
            for y in range(2):
                LB[y, bx] = jnp.zeros((8, 64), jnp.int32)
                BI[bx, y] = jnp.zeros((8, 64), jnp.int32)
            BO[bx] = jnp.zeros((32, 64), jnp.int32)

    phase("pack")
    slot_of = lane // 16

    def put(pack, e, at, x):
        moved = pltpu.roll(x, 16 * at, 1) if at else x
        return jnp.where(slot_of == (at - e) % 8, moved, pack)

    def take(from_right, from_left, at):
        both = jnp.where(slot_of == at, from_right, from_left)
        return pltpu.roll(both, 128 - 16 * at, 1) if at else both

    thin_of, thin_before = lane // 12, lax.rem(lane + 12, 128) // 12

    def put_thin(pack, e, at, x):
        moved = pltpu.roll(x, 12 * at, 1) if at else x
        return jnp.where((thin_before if e else thin_of) == at, moved, pack)

    def take_thin(from_right, from_left, at):
        both = jnp.where(thin_of == at, from_right, from_left)
        return pltpu.roll(both, 128 - 12 * at, 1) if at else both

    wait_rows(ls.at[L_ICE], 8 * 2 * IR * LT)

    def ice_get(k, c, j, r):
        if k < 2:
            return V[k, c, j, pl.ds(r, 8), :]
        if k < 5:
            return S[k - 2, c, j, pl.ds(r, 8), :]
        return W[k - 5, c, j, pl.ds(r, 8), :] if k < 7 else TH[c, j, pl.ds(r, 8), :]

    def ice_set(k, c, j, r, x):
        if k < 2:
            V[k, c, j, pl.ds(r, 8), :] = x
        elif k < 5:
            S[k - 2, c, j, pl.ds(r, 8), :] = x
        elif k < 7:
            W[k - 5, c, j, pl.ds(r, 8), :] = x
        else:
            TH[c, j, pl.ds(r, 8), :] = x

    for e, j in ((0, 0), (1, LT - 1)):
        for c in range(2):
            for k in range(8):
                pack = zero
                for i in range(IR // 8):
                    pack = put(pack, e, i, ice_get(k, c, j, 16 + 8 * i))
                PI[e, c, k] = pack

    for own in (0, G - 1):
        @pl.when(g == own)
        def _(own=own):
            wait_rows(ls.at[L_ED], 2 * 2 * OR)
            for e in range(2):
                for d in range(G):
                    for k in range(2):
                        pack = zero
                        for s in range(10):
                            q = 8 * d - 1 + s
                            if 0 <= q < OR // 8:
                                pack = put_thin(pack, e, s, CE[e, k, pl.ds(8 * q, 8), :])
                        PF[e, d, k] = pack

    wait_rows(ls.at[L_OC], 3 * OR * LT)
    for e, j in ((0, 0), (1, LT - 1)):
        for k, ref in enumerate((B, D, X)):
            for v in range(4):
                pack = zero
                for i in range(8):
                    pack = put(pack, e, i, ref[j, pl.ds(16 + 64 * v + 8 * i, 8), :])
                PC[e, k, v] = pack

    for e, dev, cond, s, ri, ro in ((0, left, has_l, S_L, R_IR, R_OR), (1, right, has_r, S_R, R_IL, R_OL)):
        @pl.when(cond)
        def _(e=e, dev=dev, s=s, ri=ri, ro=ro):
            send(PI.at[e], LI.at[1 - e], s, ri, dev)
            send(PC.at[e], LC.at[1 - e], s, ro, dev)

    for own, c in ((0, 0), (G - 1, 1)):
        @pl.when(g == own)
        def _(own=own, c=c):
            for e, dx, cond, s, r in ((0, -1, has_l, S_FL, R_PR), (1, 1, has_r, S_FR, R_PL)):
                @pl.when(cond)
                def _(e=e, dx=dx, s=s, r=r):
                    for dg in range(G):
                        d = dg if own == 0 else G - 1 - dg
                        dev = (g + dg if own == 0 else g - dg, t + dx)
                        send(PF.at[e, d], LF.at[1 - e, c], s, r + c, dev)

    phase("mergeice")
    @pl.when(has_l)
    def _():
        wait_rows(rs.at[R_IL], 2 * 8 * 8)

    @pl.when(has_r)
    def _():
        wait_rows(rs.at[R_IR], 2 * 8 * 8)

    quarter = lane // 32
    for c in range(2):
        ends = [[zero, zero], [zero, zero]]
        for k in range(8):
            for i in range(IR // 8):
                x = take(LI[1, c, k], LI[0, c, k], i)
                ice_set(k, c, LT, 16 + 8 * i, x)
                for e, at in ((0, 0), (1, IR // 8 - 1)):
                    if i == at:
                        moved = pltpu.roll(x, (32 * (k % 4) + 16) % 128, 1)
                        ends[e][k // 4] = jnp.where(quarter == k % 4, moved, ends[e][k // 4])
        for e in range(2):
            for v in range(2):
                PH[e, c, v] = ends[e][v]
    for e, dev, cond, s, r in ((0, up, has_u, S_U, R_ID), (1, down, has_d, S_D, R_IU)):
        @pl.when(cond)
        def _(e=e, dev=dev, s=s, r=r):
            for c in range(2):
                send(PH.at[e, c], LH.at[1 - e, c], s, r + c, dev)

    for own, c, row, to, dev, r in (
        (0, 0, IR + 8, 8, down, R_FU), (G - 1, 1, 16, IR + 16, up, R_FD + 1)):
        @pl.when(g == own)
        def _(c=c, row=row, to=to, dev=dev, r=r):
            wait_rows(ls.at[L_FL], 2 * (IR + 8) * LT)
            for k in range(2):
                for j in range(LT):
                    FE[k, j] = W[k, c, j, pl.ds(row, 8), :] + FL[k, c, j, pl.ds(row, 8), :] * DRAG
            for j in range(LT):
                send(FE.at[:, j], W.at[:, c, j, pl.ds(to, 8), :], S_FW, r, dev)

    for own, c in ((0, 0), (G - 1, 1)):
        @pl.when(g == own)
        def _(own=own, c=c):
            send_flow(c, dests[own][2])
    halo_turn(1)
    def ocean_ends():
        for dev, cond, at, to, s, r in (
            (up, has_u, 0, OR + 16, S_U, R_OD),
            (down, has_d, OR - 8, 8, S_D, R_OU),
        ):
            @pl.when(cond)
            def _(dev=dev, at=at, to=to, s=s, r=r):
                for j in range(LT):
                    send(base.at[pl.ds(at, 8), cols(j)], B.at[j, pl.ds(to, 8), :], s, r, dev)
                    send(depth.at[pl.ds(at, 8), cols(j)], D.at[j, pl.ds(to, 8), :], s, r, dev)
                    send(ssh.at[pl.ds(at, 8), cols(j)], X.at[j, pl.ds(to, 8), :], s, r, dev)

    phase("mergeoc")
    @pl.when(has_l)
    def _():
        wait_rows(rs.at[R_OL], 3 * 4 * 8)

    @pl.when(has_r)
    def _():
        wait_rows(rs.at[R_OR], 3 * 4 * 8)

    ends = [zero, zero]
    for k, ref in enumerate((B, D, X)):
        for q in range(OR // 8):
            x = take(LC[1, k, q // 8], LC[0, k, q // 8], q % 8)
            ref[LT, pl.ds(16 + 8 * q, 8), :] = x
            for e, at in ((0, 0), (1, OR // 8 - 1)):
                if q == at:
                    moved = pltpu.roll(x, 32 * k + 16, 1)
                    ends[e] = jnp.where(quarter == k, moved, ends[e])
    for e, dev, cond, s, r in ((0, up, has_u, S_U, R_OD), (1, down, has_d, S_D, R_OU)):
        PHO[e] = ends[e]
        @pl.when(cond)
        def _(e=e, dev=dev, s=s, r=r):
            send(PHO.at[e], LHO.at[1 - e], s, r, dev)

    phase("masks")
    def block_pairs(dy, x, e):
        if dy == 0:
            return [(iblk, BI.at[x], S_BI, R_BI), (land, BO.at[x], S_BO, R_BO)]
        return [(PB.at[e], LB.at[1 - e, x], S_BI, R_BI)]

    for dy, dx, cond in nbrs:
        k = 3 * (1 + dy) + (1 + dx)
        @pl.when(cond)
        def _(dy=dy, dx=dx, k=k):
            dev = (g + dy, t + dx)
            pairs = block_pairs(dy, 1 + dx, 1 if dy < 0 else 0)
            for src, dst, s, r in pairs:
                pltpu.make_async_remote_copy(
                    src_ref=src, dst_ref=dst, send_sem=ss.at[s + k], recv_sem=rs.at[r + k],
                    device_id=dev, device_id_type=MESH).wait_recv()

    def selection(width, first, start):
        block = lax.broadcasted_iota(jnp.int32, (64, width), 0)
        at = lax.broadcasted_iota(jnp.int32, (64, width), 1)
        hit = block == at // BS + first
        if start is not None:
            hit = jnp.logical_and(hit, (at < 64) if start == 0 else (at >= 64))
        return hit.astype(F32)

    sel_c = selection(128 * LT, 0, None)
    sel_r = selection(128, 0, 0)
    sel_l = selection(128, 48, 1)

    def spread_rows(refs):
        lft, mid, rgt = (ref.astype(F32) for ref in refs)
        wide = jnp.dot(mid, sel_c, preferred_element_type=F32)
        last = jnp.dot(rgt, sel_r, preferred_element_type=F32) + jnp.dot(
            lft, sel_l, preferred_element_type=F32)
        return wide, last

    def paint(ref, row, parts, b):
        wide, last = parts
        for j in range(LT):
            ref[j, pl.ds(row, 8), :] = jnp.broadcast_to(wide[b:b + 1, 128 * j:128 * j + 128], (8, 128))
        ref[LT, pl.ds(row, 8), :] = jnp.broadcast_to(last[b:b + 1, :], (8, 128))

    ends = [spread_rows([LB[y, x] for x in range(3)]) for y in range(2)]
    for c in range(2):
        cov = CV.at[c]
        paint(cov, 8, ends[0], c)
        mid = spread_rows([BI[x, c] for x in range(3)])
        for b in range(8):
            paint(cov, 16 + 8 * b, mid, b)
        paint(cov, IR + 16, ends[1], c)
    paint(WET, 8, ends[0], 2)
    for q in range(4):
        mid = spread_rows([BO[x, 8 * q:8 * q + 8] for x in range(3)])
        for b in range(8):
            paint(WET, 16 + 64 * q + 8 * b, mid, b)
    paint(WET, OR + 16, ends[1], 2)

    def static(c, r):
        rr = pl.ds(r, 8)
        for j in range(NT):
            cov = CV[c, j, rr, :]
            thc = TH[c, j, rr, :] * cov
            scale = cov / (thc + (1.0 + STEP * DRAG))
            C1[c, j, rr, :] = scale * (thc + 1.0)
            C2[c, j, rr, :] = scale * STEP
            TH[c, j, rr, :] = thc * (RELAX * STRENGTH / (1.0 + RELAX))

    for c in range(2):
        def own_static(i, carry, c=c):
            static(c, pl.multiple_of(8 * i + 16, 8))
            return carry
        lax.fori_loop(0, IR // 8, own_static, 0)

    def pass_on(c, row, to, dev, r):
        for j in range(LT):
            send(W.at[:, c, j, pl.ds(row, 8), :], W.at[:, c, j, pl.ds(to, 8), :], S_FW, r + c, dev)

    def cap(c, turn):
        phase = Phases()
        phase("capwait")

        for e, cond, r, row, rf, summed in (
            (0, has_u, R_IU, 8, R_FU, top_is_summed(c)),
            (1, has_d, R_ID, IR + 16, R_FD, bottom_is_summed(c)),
        ):
            @pl.when(cond)
            def _(e=e, r=r, row=row, rf=rf, summed=summed):
                @pl.when(summed)
                def _():
                    wait_rows(rs.at[rf + c], 2 * 8 * LT)
                    wait_rows(rs.at[r + c], 6 * 8 * LT + 16)

                @pl.when(jnp.logical_not(summed))
                def _():
                    wait_rows(rs.at[r + c], 8 * 8 * LT + 16)
                for k in range(8):
                    x = pltpu.roll(LH[e, c, k // 4], (128 - 32 * (k % 4) - 16) % 128, 1)
                    ice_set(k, c, LT, row, x)

        @pl.when(has_l)
        def _():
            wait_rows(rs.at[R_PL + c], 16)

        @pl.when(has_r)
        def _():
            wait_rows(rs.at[R_PR + c], 16)

        for k in range(2):
            for s in range(10):
                FL[k, c, LT, pl.ds(8 + 8 * s, 8), :] = take_thin(LF[1, c, k], LF[0, c, k], s)

        mine = jnp.logical_and(is_owner, c == owner_cap)
        at_end = jnp.logical_or(jnp.logical_and(c == 0, g == G - 1), jnp.logical_and(c == 1, g == 0))

        @pl.when(jnp.logical_not(mine))
        def _():
            both = jnp.logical_and(top_is_summed(c), bottom_is_summed(c))

            @pl.when(both)
            def _():
                wait_rows(rs.at[R_F + c], 2 * IR * LT)

            @pl.when(jnp.logical_not(both))
            def _():
                wait_rows(rs.at[R_F + c], 2 * (IR + 8) * LT)

        phase("prepare")
        static(c, 8)
        static(c, IR + 16)

        def prepare(i, carry):
            r = pl.ds(pl.multiple_of(8 * i + 8, 8), 8)
            for j in range(NT):
                for k in range(2):
                    W[k, c, j, r, :] = W[k, c, j, r, :] + FL[k, c, j, r, :] * DRAG
            return carry
        lax.fori_loop(0, IR // 8 + 2, prepare, 0)

        @pl.when(jnp.logical_and(c == 0, g == 1))
        def _():
            pass_on(0, IR + 8, 8, down, R_FU)

        @pl.when(jnp.logical_and(c == 0, g == G - 1))
        def _():
            pass_on(0, 16, IR + 16, up, R_FD)

        @pl.when(jnp.logical_and(c == 1, g == 0))
        def _():
            pass_on(1, IR + 8, 8, down, R_FU)

        @pl.when(jnp.logical_and(c == 1, g == 2))
        def _():
            pass_on(1, 16, IR + 16, up, R_FD)

        phase("subcycles")
        @pl.when(turn == 1)
        def _():
            ocean_ends()

        keep = 1.0 / (1.0 + RELAX)

        def group(r):
            rr = pl.ds(r, 8)
            u = [V[0, c, j, rr, :] for j in range(NT)]
            v = [V[1, c, j, rr, :] for j in range(NT)]
            ue, ve = east(u, lane), east(v, lane)
            s0, s1, s2 = [], [], []
            for j in range(NT):
                dux = V[0, c, j, pl.ds(r + 1, 8), :] - u[j]
                dvx = V[1, c, j, pl.ds(r + 1, 8), :] - v[j]
                duy, dvy = ue[j] - u[j], ve[j] - v[j]
                ed, et, es = dux + dvy, dux - dvy, duy + dvx
                inv = lax.rsqrt(ed * ed + et * et + es * es + 1.0)
                a = TH[c, j, rr, :]
                ai = a * inv
                s0.append(S[0, c, j, rr, :] * keep + (ed * ai - a))
                s1.append(S[1, c, j, rr, :] * keep + et * ai)
                s2.append(S[2, c, j, rr, :] * keep + es * ai)
                S[0, c, j, rr, :] = s0[j]
                S[1, c, j, rr, :] = s1[j]
                S[2, c, j, rr, :] = s2[j]

        def push(r):
            rr, above = pl.ds(r, 8), pl.ds(r - 1, 8)
            s0 = [S[0, c, j, rr, :] for j in range(NT)]
            s1 = [S[1, c, j, rr, :] for j in range(NT)]
            s2 = [S[2, c, j, rr, :] for j in range(NT)]
            dif = [s0[j] - s1[j] for j in range(NT)]
            dw, sw = west(dif, lane), west(s2, lane)
            for j in range(NT):
                tot_up = S[0, c, j, above, :] + S[1, c, j, above, :]
                f0 = 0.5 * ((s0[j] + s1[j]) - tot_up) + (s2[j] - sw[j])
                f1 = 0.5 * (dif[j] - dw[j]) + (s2[j] - S[2, c, j, above, :])
                c1, c2 = C1[c, j, rr, :], C2[c, j, rr, :]
                V[0, c, j, rr, :] = c1 * V[0, c, j, rr, :] + c2 * (f0 + W[0, c, j, rr, :])
                V[1, c, j, rr, :] = c1 * V[1, c, j, rr, :] + c2 * (f1 + W[1, c, j, rr, :])

        def subcycle(n, carry):
            for i in range(IR // 8 + 2):
                group(8 + 8 * i)
            for i in range(IR // 8 + 2):
                push(8 + 8 * i)
            return carry
        lax.fori_loop(0, NSUB, subcycle, 0)

        phase("diverge")
        prev = [zero] * NT
        pack = zero
        for i in range(IR // 8):
            rr = pl.ds(16 + 8 * i, 8)
            p0, p1 = [], []
            for j in range(NT):
                cov = CV[c, j, rr, :] * DRAG
                p0.append(cov * (V[0, c, j, rr, :] - FL[0, c, j, rr, :]))
                p1.append(cov * (V[1, c, j, rr, :] - FL[1, c, j, rr, :]))
            pw = west(p1, lane)
            for j in range(NT):
                turned = pltpu.roll(p0[j], 1, 0)
                above = jnp.where(sub == 0, prev[j], turned)
                prev[j] = turned
                sp = (p0[j] - above) + (p1[j] - pw[j])
                if j < LT:
                    SPB[c, j, pl.ds(8 * i, 8), :] = sp
                else:
                    pack = jnp.where(lane // 16 == i, pltpu.roll(sp, 16 * i + 8, 1), pack)
        XB[c, 0] = pack
        extra = zero
        for j in range(NT):
            extra = jnp.where(sub == j, -jnp.broadcast_to(prev[j][0:1, :], (8, 128)), extra)
        XB[c, 1] = extra

        @pl.when(mine)
        def _():
            for j in range(LT):
                for i in range(IR // 8):
                    RSP[g, j, pl.ds(8 * i, 8), :] = SPB[c, j, pl.ds(8 * i, 8), :]
            RX[g, 0] = XB[c, 0]
            RX[g, 1] = XB[c, 1]

        @pl.when(jnp.logical_not(mine))
        def _():
            dev = (c * (G - 1), t)
            send(SPB.at[c], RSP.at[g], S_RS + c, R_RS + g, dev)
            send(XB.at[c], RX.at[g], S_RS + c, R_RS + g, dev)

        @pl.when(at_end)
        def _():
            at = jnp.where(c == 0, IR - 8, 0)
            dev = (1 + c, t)
            send(SPB.at[c, :, pl.ds(pl.multiple_of(at, 8), 8), :], RH, S_RH, R_RH, dev)
            send(XB.at[c], RXH, S_RH, R_RH, dev)
        phase(None)

    def caps(turn, carry):
        cap(jnp.where(turn == 0, first_cap, 1 - first_cap), turn)
        return carry

    def ocean_rows(body, carry, unroll=4):
        def step(i, cc):
            for m in range(unroll):
                cc = body(pl.multiple_of(8 * (unroll * i + m) + 16, 8), cc)
            return cc
        return lax.fori_loop(0, OR // 8 // unroll, step, carry)

    def shifted_sum(ref, r):
        rr = pl.ds(r, 8)
        mid = [ref[j, rr, :] for j in range(NT)]
        e, w = east(mid, lane), west(mid, lane)
        return mid, [
            (ref[j, pl.ds(r + 1, 8), :] + ref[j, pl.ds(r - 1, 8), :]) + (e[j] + w[j])
            for j in range(NT)
        ]

    def ocean_prepare():
        phase = Phases()
        phase("oceanwait")

        for e, cond, r, row in ((0, has_u, R_OU, 8), (1, has_d, R_OD, OR + 16)):
            @pl.when(cond)
            def _(e=e, r=r, row=row):
                wait_rows(rs.at[r], 24 * LT + 8)
                for k, ref in enumerate((B, D, X)):
                    ref[LT, pl.ds(row, 8), :] = pltpu.roll(LHO[e], 128 - 32 * k - 16, 1)

        phase("oceanprep")
        def first(r, carry):
            rr = pl.ds(r, 8)
            for j in range(NT):
                gg = D[j, rr, :] * WET[j, rr, :]
                D[j, rr, :] = gg
                Y0[j, rr, :] = gg * X[j, rr, :]
            return carry

        def second(r, carry):
            rr = pl.ds(r, 8)
            gs, gn = shifted_sum(D, r)
            _, xn = shifted_sum(Y0, r)
            for j in range(NT):
                diag = gs[j] * gn[j] + DAMP
                inv = 1.0 / diag
                wid = WET[j, rr, :] * inv
                h = gs[j] * inv
                DG[j, rr, :] = diag
                WID[j, rr, :] = wid
                H[j, rr, :] = h
                Z[j, rr, :] = wid * B[j, rr, :] + h * xn[j] - X[j, rr, :]
            return carry
        for body in (first, second):
            body(8, 0)
            ocean_rows(body, 0)
            body(OR + 16, 0)
        phase(None)

    lax.fori_loop(0, 2, caps, 0)
    ocean_prepare()

    phase("arrive")
    late_block = {0: 2, G - 1: 1}

    def add_block(d, more_from):
        for i in range(IR // 8):
            rr = pl.ds(16 + IR * d + 8 * i, 8)
            for j in range(NT):
                if j < LT:
                    sp = RSP[d, j, pl.ds(8 * i, 8), :]
                else:
                    sp = pltpu.roll(RX[d, 0], 128 - (16 * i + 8), 1)
                if i == 0 and more_from is not None:
                    sp = sp + below_block(more_from, j)
                Z[j, rr, :] = Z[j, rr, :] + WID[j, rr, :] * sp

    def below_block(d, j):
        return jnp.where(sub == 0, jnp.broadcast_to(RX[d, 1][j:j + 1, :], (8, 128)), 0.0)

    def add_below(d):
        rr = pl.ds(16 + IR * (d + 1), 8)
        for j in range(NT):
            Z[j, rr, :] = Z[j, rr, :] + WID[j, rr, :] * below_block(d, j)

    for own, last_in in late_block.items():
        @pl.when(g == own)
        def _(own=own, last_in=last_in):
            rest = [d for d in range(G) if d != last_in]
            for d in rest:
                if d != own:
                    wait_rows(rs.at[R_RS + d], LT * IR + 16)
            for d in rest:
                add_block(d, d - 1 if d - 1 in rest else None)
            if own == 0:
                add_below(G - 1)

    @pl.when(jnp.logical_not(is_owner))
    def _():
        wait_rows(rs.at[R_RH], LT * 8 + 16)

        @pl.when(g == 1)
        def _():
            rr = pl.ds(16, 8)
            for j in range(NT):
                more = jnp.broadcast_to(RXH[1][j:j + 1, :], (8, 128))
                Z[j, rr, :] = Z[j, rr, :] + WID[j, rr, :] * jnp.where(sub == 0, more, 0.0)
        for at, row, i in ((1, 8, 7), (2, OR + 16, 0)):
            @pl.when(g == at)
            def _(row=row, i=i):
                rr = pl.ds(row, 8)
                for j in range(NT):
                    sp = RH[j] if j < LT else pltpu.roll(RXH[0], 128 - (16 * i + 8), 1)
                    Z[j, rr, :] = Z[j, rr, :] + WID[j, rr, :] * sp

    phase("krylov")
    def krylov0(r, acc):
        rr = pl.ds(r, 8)
        for j in range(NT):
            z = Z[j, rr, :]
            Y0[j, rr, :] = D[j, rr, :] * z
            if j < LT and acc is not None:
                acc = (acc[0] + DG[j, rr, :] * z * z,)
        return acc

    def krylov(src, dst, vec, r, acc):
        rr = pl.ds(r, 8)
        y, n = shifted_sum(src, r)
        for j in range(NT):
            v = H[j, rr, :] * n[j]
            out = D[j, rr, :] * v
            vec[j, rr, :] = v
            dst[j, rr, :] = out
            if j < LT and acc is not None:
                acc = (acc[0] + y[j] * n[j], acc[1] + out * n[j])
        return acc

    def krylov3(r, acc):
        if acc is None:
            return None
        y, n = shifted_sum(Y2, r)
        for j in range(LT):
            acc = (acc[0] + y[j] * n[j],)
        return acc

    sweeps = (
        (krylov0, (0,)),
        (functools.partial(krylov, Y0, Y1, V1), (1, 2)),
        (functools.partial(krylov, Y1, Y2, V2), (3, 4)),
        (krylov3, (5,)),
    )
    start = jnp.where(g == 0, 15, jnp.where(g == G - 1, 7, 17))
    end = jnp.where(g == 0, 27, jnp.where(g == G - 1, 19, 17))

    def row_of(group):
        return pl.multiple_of(8 * group + 8, 8)

    for body, into in sweeps:
        body(8, None)
        body(OR + 16, None)
        body(row_of(start), None)
        body(row_of(end - 1), None)

        def some(i, acc, first, count, body=body):
            for m in range(count):
                acc = body(row_of(first + count * i + m), acc)
            return acc

        @pl.when(is_owner)
        def _(some=some, into=into):
            acc = (zero,) * len(into)
            acc = lax.fori_loop(0, (start - 1) // 2, functools.partial(some, first=1, count=2), acc)
            acc = lax.fori_loop(0, (33 - end) // 2, functools.partial(some, first=end, count=2), acc)
            for k, m in zip(into, acc):
                MOM[k] = m

        @pl.when(jnp.logical_not(is_owner))
        def _(some=some, into=into):
            acc = lax.fori_loop(
                0, 2, functools.partial(some, first=1, count=16), (zero,) * len(into))
            for k, m in zip(into, acc):
                MOM[k] = m

    phase("late")
    for own, last_in in late_block.items():
        @pl.when(g == own)
        def _(own=own, last_in=last_in):
            wait_rows(rs.at[R_RS + last_in], LT * IR + 16)
            add_block(last_in, last_in - 1)
            add_below(last_in)

    phase("krylate")

    @pl.when(is_owner)
    def _():
        for body, into in sweeps:
            acc = (zero,) * len(into)
            for m in range(12):
                acc = body(row_of(start + m), acc)
            for k, m in zip(into, acc):
                MOM[k] = MOM[k] + m

    moments = [MOM[k] for k in range(6)]
    phase("red1")
    tile = zero
    for k, m in enumerate(moments):
        tile = jnp.where(sub == k, jnp.sum(m, axis=0, keepdims=True), tile)
    slot1 = 2 * g + core
    L1[slot1] = tile
    for dev in peers1:
        send(L1.at[slot1], L1.at[slot1], S_1, R_1, dev)
    wait_rows(rs.at[R_1], 8 * len(peers1))
    tile = L1[0]
    for k in range(1, 8):
        tile = tile + L1[k]
    phase("red2")
    L2[mine2] = tile
    for dev in peers2:
        send(L2.at[mine2], L2.at[mine2], S_2, R_2, dev)
    wait_rows(rs.at[R_2], 8 * len(peers2))
    tile = L2[0]
    for k in range(1, M2):
        tile = tile + L2[k]
    phase("coef")
    total = jnp.sum(tile, axis=1, keepdims=True)
    mu = [total[k:k + 1, :] for k in range(6)]
    nu = [mu[k] - mu[k + 1] for k in range(5)]

    a0 = mu[0] / nu[0]
    z10, z11 = 1.0 - a0, a0
    rz1 = z11 * (z10 * mu[1] + z11 * mu[2])
    b0 = rz1 / mu[0]
    p10, p11 = z10 + b0, z11
    a1 = rz1 / (p11 * (p10 * nu[1] + p11 * nu[2]))
    z20, z21, z22 = z10 - a1 * p10, z11 - a1 * (p11 - p10), a1 * p11
    rz2 = z22 * (z20 * mu[2] + z21 * mu[3] + z22 * mu[4])
    b1 = rz2 / rz1
    p20, p21, p22 = z20 + b1 * p10, z21 + b1 * p11, z22
    a2 = rz2 / (p22 * (p20 * nu[2] + p21 * nu[3] + p22 * nu[4]))
    k0 = jnp.broadcast_to(a0 + a1 * p10 + a2 * p20, (8, 128))
    k1 = jnp.broadcast_to(a1 * p11 + a2 * p21, (8, 128))
    k2 = jnp.broadcast_to(a2 * p22, (8, 128))

    phase("finish")
    def finish(r, carry):
        rr = pl.ds(r, 8)
        for j in range(LT):
            OUT[j, pl.ds(pl.multiple_of(r - 16, 8), 8), :] = X[j, rr, :] + (
                k0 * Z[j, rr, :] + (k1 * V1[j, rr, :] + k2 * V2[j, rr, :]))
        return carry
    ocean_rows(finish, 0)
    phase("sentwait")
    for s, cond in ((S_FL, jnp.logical_and(is_owner, has_l)), (S_FR, jnp.logical_and(is_owner, has_r))):
        @pl.when(cond)
        def _(s=s):
            wait_rows(ss.at[s], G * 16)
    for s, cond in ((S_L, has_l), (S_R, has_r)):
        @pl.when(cond)
        def _(s=s):
            wait_rows(ss.at[s], 2 * 8 * 8 + 3 * 4 * 8)
    for at in range(G):
        @pl.when(g == at)
        def _(at=at):
            full = (8 * 2 + 3) * 8 * LT + 2 * 16 + 8
            if at > 0:
                less = sum(bottom_summed(c, at - 1) for c in range(2))
                wait_rows(ss.at[S_U], full - less * 2 * 8 * LT)
            if at < G - 1:
                less = sum(top_summed(c, at + 1) for c in range(2))
                wait_rows(ss.at[S_D], full - less * 2 * 8 * LT)
            if at in (0, G - 1):
                c = 0 if at == 0 else 1
                wait_rows(ss.at[S_F], 2 * LT * sum(flow_rows(c, d)[1] for d in dests[at]))
            wait_rows(ss.at[S_FW], (2 if at in (0, G - 1) else 1) * 2 * 8 * LT)
    for c in range(2):
        mine = jnp.logical_and(is_owner, c == owner_cap)

        @pl.when(jnp.logical_not(mine))
        def _(c=c):
            wait_rows(ss.at[S_RS + c], LT * IR + 16)

    @pl.when(is_owner)
    def _():
        wait_rows(ss.at[S_RH], LT * 8 + 16)
    wait_rows(ss.at[S_1], 8 * len(peers1))
    wait_rows(ss.at[S_2], 8 * len(peers2))
    for dy, dx, cond in nbrs:
        k = 3 * (1 - dy) + (1 - dx)
        @pl.when(cond)
        def _(dy=dy, dx=dx, k=k):
            dev = (g + dy, t + dx)
            for src, dst, s, r in block_pairs(dy, 1 - dx, 0 if dy < 0 else 1):
                pltpu.make_async_remote_copy(
                    src_ref=src, dst_ref=dst, send_sem=ss.at[s + k], recv_sem=rs.at[r + k],
                    device_id=dev, device_id_type=MESH).wait_send()
    phase(None)


def shards(T, *args):
    ice = (2, NT, IH, 128)
    ocean = (NT, OH, 128)
    vm = lambda *s: pltpu.VMEM(s, F32)
    scratch = [
        vm(2, *ice), vm(*ice), vm(2, *ice), vm(*ice), vm(*ice), vm(*ice),
        vm(2, 2, 8, 8, 128), vm(2, 2, 8, 8, 128), vm(2, 3, 4, 8, 128), vm(2, 3, 4, 8, 128),
        vm(2, G, 2, 8, 128), vm(2, 2, 2, 8, 128), vm(2, 2, 2, 8, 128), vm(2, 2, 2, 8, 128),
        vm(2, 8, 128), vm(2, 8, 128), vm(2, 2, OR, 128), vm(2, LT, 8, 128),
        *[vm(*ocean) for _ in range(13)],
        pltpu.VMEM((3, 2, 8, 64), jnp.int32), pltpu.VMEM((3, 32, 64), jnp.int32),
        pltpu.VMEM((2, 8, 64), jnp.int32), pltpu.VMEM((2, 3, 8, 64), jnp.int32),
        vm(2, LT, IR, 128), vm(2, 2, 8, 128),
        vm(G, LT, IR, 128), vm(G, 2, 8, 128), vm(LT, 8, 128), vm(2, 8, 128),
        vm(8, 8, 128), vm(T // 2, 8, 128), vm(6, 8, 128), vm(DUMMY, 128),
        pltpu.SemaphoreType.DMA((N_R,)), pltpu.SemaphoreType.DMA((N_S,)), pltpu.SemaphoreType.DMA((N_L,)),
    ]
    hbm = pl.BlockSpec(memory_space=pltpu.HBM)
    vmem = pl.BlockSpec(memory_space=pltpu.VMEM)
    worked = pl.pallas_call(
        functools.partial(kernel, T),
        out_shape=(vm(2, *ice), vm(3, *ice), vm(LT, OR, 128)),
        in_specs=[hbm] * 10,
        out_specs=(vmem, vmem, vmem),
        scratch_shapes=scratch,
        compiler_params=pltpu.CompilerParams(
            collective_id=0, has_side_effects=True, vmem_limit_bytes=60 * 1024 * 1024),
    )(*args)
    return pl.pallas_call(
        deliver,
        out_shape=(
            jax.ShapeDtypeStruct((OR, 128 * LT), F32),
            jax.ShapeDtypeStruct((2, 2, IR, 128 * LT), F32),
            jax.ShapeDtypeStruct((3, 2, IR, 128 * LT), F32),
        ),
        in_specs=[vmem] * 3,
        out_specs=(hbm, hbm, hbm),
        scratch_shapes=[pltpu.SemaphoreType.DMA((3, LT))],
        compiler_params=pltpu.CompilerParams(vmem_limit_bytes=1024 * 1024),
    )(*worked)


def deliver(V, S, OUT, o_ssh, o_vel, o_str, sem):
    copies = []
    for j in range(LT):
        to = pl.ds(128 * j, 128)
        copies += [
            pltpu.make_async_copy(S.at[:, :, j, pl.ds(16, IR), :], o_str.at[:, :, :, to], sem.at[0, j]),
            pltpu.make_async_copy(V.at[:, :, j, pl.ds(16, IR), :], o_vel.at[:, :, :, to], sem.at[1, j]),
            pltpu.make_async_copy(OUT.at[j], o_ssh.at[:, to], sem.at[2, j]),
        ]
    for c in copies:
        c.start()
    for c in copies:
        c.wait()


def solution(mesh):
    return jax.shard_map(
        functools.partial(shards, mesh.shape["tile"]),
        mesh=mesh,
        in_specs=(
            P("grp", "tile"),
            P("grp", "tile"),
            P("grp", "tile"),
            P(None, "grp", "tile"),
            P("grp", "tile"),
            P(None, "grp", "tile"),
            P(None, "grp", "tile"),
            P(None, None, "grp", "tile"),
            P(None, None, "grp", "tile"),
            P(None, None, "grp", "tile"),
        ),
        out_specs=(P("grp", "tile"), P(None, None, "grp", "tile"), P(None, None, "grp", "tile")),
        check_vma=False,
    )
```
